128 devices in a mesh: rows: 32 (over z, y, core), vecs: 4 (over x).
Axes of the slice: x: 4, y: 4, z: 4, core: 2. Of those that a mesh axis runs over, the one named last changes fastest.
Arguments:
- basis: bfloat16 [100, 2097152], P('vecs', 'rows'), may hold values from -6 to 6
- coefficients: bfloat16 [100, 40], replicated, may hold values from -0.625 to 0.625
- eigen_values: float32 [40], P('vecs'), may hold values from -3 to 1
- stiffness: float32 [2097152], P('rows'), may hold values from 6.5 to 10
- damping: float32 [2097152], P('rows'), may hold values from 0.2 to 2
- mass: float32 [2097152], P('rows'), may hold values from 0.5 to 2
- link_count: int32 [32], P('rows'), may hold values from 1024 to 4096, as said below
- lower_cells: int32 [32, 4096], P('rows'), may hold values from 0 to 4095
- upper_cells: int32 [32, 4096], P('rows'), may hold values from 0 to 4095
Outputs:
- eigvecs: bfloat16 [40, 2097152], P('vecs', 'rows')
- residuals: bfloat16 [40, 2097152], P('vecs', 'rows')
- relative_norms: float32 [40], P('vecs')
The draws below stay inside these ranges and needn't reach their ends.
Inputs may be any that keep to these rules, and one draw needn't show every extreme that they name: Interface s joins subdomain s to subdomain (s + 1) mod 32; only its first link_count[s] slots are used, the others are to be ignored. Some interface uses all 4096 slots in every draw. `lower_cells`: slots beyond link_count[s] hold values that are not used. `upper_cells`: slots beyond link_count[s] hold values that are not used.
All inputs are finite; a program needn't handle non-finite values.
Results may differ from the reference program's by a relative error of at most 0.0037.
The reference program's roundings to bfloat16 on the way count: a program that leaves them out, or rounds other values in their place, can miss the bound.
Values may be sent and summed in bfloat16 or wider, within the bound.
A program may use at most 320 MiB of HBM per device.

```python
import math
import jax
import jax.numpy as jnp
from jax import lax

RANK = 100
NV = 40
WID = 64
ZD = 16
HMAX = 4096
NSUB = 32
NROWS = 2097152
N_ROWS = 32


def draw_link_count(key, part):
    first_key, second_key = jax.random.split(jax.random.fold_in(key, 17))
    counts = jax.random.randint(first_key, (NSUB,), HMAX // 4, HMAX + 1)
    chosen = jax.random.randint(second_key, (), 0, NSUB)
    return jnp.where(jnp.arange(NSUB) == chosen, HMAX, counts).astype(jnp.int32)


def place_ends(array, key, least, largest):
    shape = array.shape
    place = [jax.random.randint(jax.random.fold_in(key, axis), (), 0, shape[axis]) for axis in range(len(shape))]
    array = array.at[tuple(place)].set(least)
    longest = shape.index(max(shape))
    place[longest] = (place[longest] + 1) % shape[longest]
    return array.at[tuple(place)].set(largest)


def block_levels(rng, dims, cuts, smallest, top_value):
    gain, own = 1.0, jax.random.fold_in(rng, 6)
    for dim, blocks in cuts:
        steps = jnp.exp(jax.random.uniform(jax.random.fold_in(own, dim), (blocks,), jnp.float32, smallest / len(cuts), top_value / len(cuts)))
        gain = gain * jnp.repeat(steps, dims[dim] // blocks).reshape([-1 if axis == dim else 1 for axis in range(len(dims))])
    return gain


def scatter_about(stream_key, dims, deviation, reach, cuts=(), held_as=jnp.bfloat16):
    result = deviation * jax.random.normal(stream_key, dims, jnp.float32)
    if cuts:
        result = result * block_levels(stream_key, dims, cuts, -0.22, 0.18)
    return jnp.clip(result, -reach, reach).astype(held_as)


def setup_inputs(seed: int = 0) -> dict:
    keys = jax.random.split(jax.random.key(seed), 10)
    basis = scatter_about(keys[0], (RANK, NROWS), 1.0, 6.0, ((0, 4), (1, 32)))
    coefficients = scatter_about(keys[1], (RANK, NV), RANK ** -0.5, 0.625)
    eigen_values = jnp.clip(-3.0 + 4.0 * jax.random.uniform(keys[2], (NV,), jnp.float32) ** block_levels(keys[2], (NV,), ((0, 4),), -0.2, 0.2), -3.0, 1.0)
    stiffness = jnp.clip(6.5 + 3.5 * jax.random.uniform(keys[3], (NROWS,), jnp.float32) ** block_levels(keys[3], (NROWS,), ((0, 32),), -0.2, 0.2), 6.5, 10.0)
    damping = jnp.clip(0.2 + 1.8 * jax.random.uniform(keys[4], (NROWS,), jnp.float32) ** block_levels(keys[4], (NROWS,), ((0, 32),), -0.2, 0.2), 0.2, 2.0)
    mass = jnp.clip(jnp.exp(math.log(2.0) - 1.3862944 * jax.random.uniform(keys[5], (NROWS,), jnp.float32) ** block_levels(keys[5], (NROWS,), ((0, 32),), -0.2, 0.2)), 0.5, 2.0)
    link_count = draw_link_count(jax.random.fold_in(keys[9], 71), 0)
    lower_cells = place_ends(jax.random.randint(keys[7], (NSUB, HMAX), 0, WID * WID), jax.random.fold_in(keys[7], 1), 0, (WID * WID) - 1).astype(jnp.int32)
    upper_cells = place_ends(jax.random.randint(keys[8], (NSUB, HMAX), 0, WID * WID), jax.random.fold_in(keys[8], 1), 0, (WID * WID) - 1).astype(jnp.int32)
    return {"basis": basis, "coefficients": coefficients, "eigen_values": eigen_values, "stiffness": stiffness, "damping": damping, "mass": mass, "link_count": link_count, "lower_cells": lower_cells, "upper_cells": upper_cells}


def neighbours(values, width_cells):
    depth_pad = jnp.pad(values, ((0, 0), (1, 1), (0, 0)))
    total = depth_pad[:, 2:] + depth_pad[:, :-2]
    across = jnp.pad(values, ((0, 0), (0, 0), (width_cells, width_cells)))
    total = total + across[:, :, 2 * width_cells:] + across[:, :, :-2 * width_cells]
    column = jnp.arange(values.shape[2]) % width_cells
    shifted = jnp.pad(values, ((0, 0), (0, 0), (1, 1)))
    total = total + jnp.where(column < width_cells - 1, shifted[:, :, 2:], 0.0)
    total = total + jnp.where(column > 0, shifted[:, :, :-2], 0.0)
    return total

def reference(basis, coefficients, eigen_values, stiffness, damping, mass, link_count, lower_cells, upper_cells):
    eigvecs = jnp.dot(coefficients.T, basis, preferred_element_type=jnp.float32).astype(jnp.bfloat16)
    vectors = eigvecs.astype(jnp.float32)
    plane_cells = WID * WID
    rows_local = ZD * plane_cells
    subdomains = N_ROWS
    neighbour_sum = neighbours(vectors.reshape(NV * subdomains, ZD, plane_cells), WID).reshape(NV, subdomains * rows_local)
    index_sub = jnp.arange(subdomains, dtype=jnp.int32)[:, None]
    lower_rows = (index_sub * rows_local + (ZD - 1) * plane_cells + lower_cells).reshape(-1).astype(jnp.int32)
    upper_rows = ((index_sub + 1) % subdomains * rows_local + upper_cells).reshape(-1).astype(jnp.int32)
    slot_used = (jnp.arange(HMAX, dtype=jnp.int32)[None, :] < link_count[:, None]).astype(jnp.float32).reshape(-1)
    link_sum = jnp.zeros_like(vectors)
    link_sum = link_sum.at[:, lower_rows].add(vectors[:, upper_rows] * slot_used)
    link_sum = link_sum.at[:, upper_rows].add(vectors[:, lower_rows] * slot_used)
    eigen_col = eigen_values[:, None]
    diagonal = eigen_col * eigen_col * mass[None, :] + eigen_col * damping[None, :] + stiffness[None, :]
    coupling = eigen_col * eigen_col * 0.1 + eigen_col * 0.3 + 1.0
    residual_full = diagonal * vectors - coupling * (neighbour_sum + link_sum)
    vector_sq = lax.optimization_barrier(jnp.sum(vectors * vectors, axis=1))
    residual_sq = lax.optimization_barrier(jnp.sum(residual_full * residual_full, axis=1))
    relative_norms = jnp.sqrt(residual_sq) / jnp.sqrt(vector_sq + 1.0)
    return (eigvecs, residual_full.astype(jnp.bfloat16), relative_norms)
```

```python
import functools

import jax
import jax.numpy as jnp
from jax import lax
from jax.experimental import pallas as pl
from jax.experimental.pallas import tpu as pltpu
from jax.sharding import PartitionSpec as P

WID = 64
PLANE = WID * WID
SPAN = 1024
SLOTS = 512
LOW = 256


def link_plane(part_a, part_b, gather_ref, scatter_ref, count, link_a, link_b):
    high = PLANE // LOW
    whole = jnp.concatenate(
        [part_a[...].astype(jnp.float32), part_b[...].astype(jnp.float32), jnp.zeros((6, PLANE), jnp.float32)], axis=0
    ).astype(jnp.bfloat16)
    table = jnp.concatenate([whole[:, LOW * h : LOW * (h + 1)] for h in range(high)], axis=0)
    cell = lax.broadcasted_iota(jnp.int32, (LOW, SLOTS), 0)
    slot = lax.broadcasted_iota(jnp.int32, (1, SLOTS), 1)

    def step(t, total):
        at = pl.multiple_of(t * SLOTS, SLOTS)
        source = gather_ref[:, pl.ds(at, SLOTS)]
        target = scatter_ref[:, pl.ds(at, SLOTS)]
        pick = jnp.where(cell == (source & (LOW - 1)), 1.0, 0.0).astype(jnp.bfloat16)
        rows = jnp.dot(table, pick, preferred_element_type=jnp.float32)
        source_high = source >> 8
        value = jnp.zeros((16, SLOTS), jnp.float32)
        for h in range(high):
            value = value + jnp.where(source_high == h, rows[16 * h : 16 * h + 16], 0.0)
        target_high = jnp.where(slot + at < count, target >> 8, -1)
        spread = jnp.concatenate(
            [jnp.where(target_high == h, value, 0.0).astype(jnp.bfloat16) for h in range(high)], axis=0
        )
        place = jnp.where(cell == (target & (LOW - 1)), 1.0, 0.0).astype(jnp.bfloat16)
        return total + lax.dot_general(
            spread, place, (((1,), (1,)), ((), ())), preferred_element_type=jnp.float32
        )

    total = lax.fori_loop(0, PLANE // SLOTS, step, jnp.zeros((16 * high, LOW), jnp.float32))
    for h in range(high):
        link_a[:, LOW * h : LOW * (h + 1)] = total[16 * h : 16 * h + 8]
        link_b[:, LOW * h : LOW * (h + 1)] = total[16 * h + 8 : 16 * h + 10]


def residual_span(ref, out_rows, diag_refs, lam, coupling, z, c, before, after, link, eig_ref, res_ref, sums):
    rows = ref.shape[0]
    base = z * PLANE + c * SPAN
    if not isinstance(base, int):
        base = pl.multiple_of(base, SPAN)

    def load(at, width):
        if not isinstance(at, int):
            at = pl.multiple_of(at, 128)
        return ref[:, pl.ds(at, width)].astype(jnp.float32)

    raw = ref[:, pl.ds(base, SPAN)]
    value = raw.astype(jnp.float32)
    edge = jnp.zeros((rows, 128), jnp.float32)
    left = load(base - 128, 128) if c > 0 else edge
    right = load(base + SPAN, 128) if c < PLANE // SPAN - 1 else edge
    wide = jnp.concatenate([left, value, right], axis=1)
    span = SPAN + 256
    total = pltpu.roll(wide, WID, 1)[:, 128 : 128 + SPAN] + pltpu.roll(wide, span - WID, 1)[:, 128 : 128 + SPAN]
    column = lax.broadcasted_iota(jnp.int32, (1, SPAN), 1) & (WID - 1)
    total = total + jnp.where(column > 0, pltpu.roll(value, 1, 1), 0.0)
    total = total + jnp.where(column < WID - 1, pltpu.roll(value, SPAN - 1, 1), 0.0)
    if before:
        total = total + load(base - PLANE, SPAN)
    if after:
        total = total + load(base + PLANE, SPAN)
    if link is not None:
        total = total + link[:, c * SPAN : (c + 1) * SPAN]
    mass, damping, stiffness = (r[:, pl.ds(base, SPAN)] for r in diag_refs)
    residual = (lam * lam * mass + lam * damping + stiffness) * value - coupling * total
    eig_ref[out_rows, pl.ds(base, SPAN)] = raw
    res_ref[out_rows, pl.ds(base, SPAN)] = residual.astype(jnp.bfloat16)
    vector_sq, residual_sq = sums
    for k in range(SPAN // 128):
        part = slice(128 * k, 128 * (k + 1))
        vector_sq = vector_sq + value[:, part] * value[:, part]
        residual_sq = residual_sq + residual[:, part] * residual[:, part]
    return vector_sq, residual_sq


def residual_all(ea, eb, diag_refs, eigen, links, eig_ref, res_ref, sums_ref):
    depth = ea.shape[1] // PLANE
    for ref, out_rows, link in ((ea, slice(0, 8), 0), (eb, slice(8, 10), 1)):
        lam = eigen[out_rows, :]
        coupling = lam * lam * 0.1 + lam * 0.3 + 1.0
        rows = ref.shape[0]

        def plane(z, sums, before, after, link_ref):
            for c in range(PLANE // SPAN):
                sums = residual_span(
                    ref, out_rows, diag_refs, lam, coupling, z, c, before, after, link_ref, eig_ref, res_ref, sums
                )
            return sums

        zero = jnp.zeros((rows, 128), jnp.float32)
        sums = plane(0, (zero, zero), False, True, links[0][link])
        sums = lax.fori_loop(1, depth - 1, lambda z, s: plane(z, s, True, True, None), sums)
        sums = plane(depth - 1, sums, True, False, links[1][link])
        sums_ref[0, out_rows, :] = sums[0]
        sums_ref[1, out_rows, :] = sums[1]


def finish_kernel(
    ea, eb, above_a, above_b, below_a, below_b, lower, upper, down_lower, down_upper, counts,
    mass, damping, stiffness, eigen, eig_ref, res_ref, sums_ref, first_a, first_b, last_a, last_b,
):
    link_plane(below_a, below_b, down_lower, down_upper, counts[1], first_a, first_b)
    link_plane(above_a, above_b, upper, lower, counts[0], last_a, last_b)
    residual_all(
        ea, eb, (mass, damping, stiffness), eigen, ((first_a, first_b), (last_a, last_b)), eig_ref, res_ref, sums_ref
    )


def finish(*operands):
    rows = operands[0].shape[1]
    vmem = pl.BlockSpec(memory_space=pltpu.VMEM)
    specs = [vmem] * 10 + [pl.BlockSpec(memory_space=pltpu.SMEM)] + [vmem] * 4
    plane = lambda r: pltpu.VMEM((r, PLANE), jnp.float32)
    return pl.pallas_call(
        finish_kernel,
        out_shape=(
            jax.ShapeDtypeStruct((10, rows), jnp.bfloat16),
            jax.ShapeDtypeStruct((10, rows), jnp.bfloat16),
            jax.ShapeDtypeStruct((2, 10, 128), jnp.float32),
        ),
        in_specs=specs,
        out_specs=(vmem, vmem, vmem),
        scratch_shapes=[plane(8), plane(2), plane(8), plane(2)],
        compiler_params=pltpu.CompilerParams(vmem_limit_bytes=40 * 2**20),
        name="finish",
    )(*operands)


def from_behind(value, axis, steps):
    count = lax.axis_size(axis)
    pairs = [(source, (source + steps) % count) for source in range(count)]
    return lax.ppermute(value, axis, pairs)


def on_device(basis, coefficients, eigen_values, stiffness, damping, mass, link_count, lower_cells, upper_cells):
    rows_local = basis.shape[1]
    quarter = lax.all_to_all(basis, "vecs", split_axis=1, concat_axis=0, tiled=True)
    quarter_vecs = jnp.dot(coefficients.T, quarter, preferred_element_type=jnp.float32).astype(jnp.bfloat16)
    eigvecs = lax.all_to_all(quarter_vecs, "vecs", split_axis=0, concat_axis=1, tiled=True)
    lists = jnp.concatenate([lower_cells, upper_cells, jnp.broadcast_to(link_count[:, None], (1, 128))], axis=1)
    down = from_behind(lists, "rows", 1)
    slots = lower_cells.shape[1]
    down_lower, down_upper, down_count = down[:, :slots], down[:, slots : 2 * slots], down[0, 2 * slots :][:1]
    ea, eb = eigvecs[:8], eigvecs[8:]
    below = from_behind(eigvecs[:, rows_local - PLANE :], "rows", 1)
    above = from_behind(eigvecs[:, :PLANE], "rows", -1)
    wide = lambda a: a.reshape(1, rows_local)
    eig, res, sums = finish(
        ea, eb, above[:8], above[8:], below[:8], below[8:], lower_cells, upper_cells, down_lower, down_upper,
        jnp.concatenate([link_count, down_count]), wide(mass), wide(damping), wide(stiffness), eigen_values[:, None],
    )
    local = jnp.sum(sums, axis=2).reshape(1, 20)
    devices = lax.axis_size("rows")
    totals = lax.all_to_all(jnp.broadcast_to(local[None], (devices, 1, 20)), "rows", 0, 0, tiled=True).sum(axis=0)
    totals = totals.reshape(2, 10)
    norms = jnp.sqrt(totals[1]) / jnp.sqrt(totals[0] + 1.0)
    return eig, res, norms


def solution(mesh):
    placed = (
        P("vecs", "rows"), P(), P("vecs"), P("rows"), P("rows"), P("rows"), P("rows"), P("rows", None), P("rows", None),
    )
    return jax.shard_map(
        on_device,
        mesh=mesh,
        in_specs=placed,
        out_specs=(P("vecs", "rows"), P("vecs", "rows"), P("vecs")),
        check_vma=False,
    )
```

```python
import functools

import jax
import jax.numpy as jnp
from jax import lax
from jax.experimental import pallas as pl
from jax.experimental.pallas import tpu as pltpu
from jax.sharding import PartitionSpec as P

WID = 64
PLANE = WID * WID
SPAN = 1024
SLOTS = 512
LOW = 256


def link_plane(part_a, part_b, gather_ref, scatter_ref, link_a, link_b):
    high = PLANE // LOW
    whole = jnp.concatenate(
        [part_a[...].astype(jnp.float32), part_b[...].astype(jnp.float32), jnp.zeros((6, PLANE), jnp.float32)], axis=0
    ).astype(jnp.bfloat16)
    table = jnp.concatenate([whole[:, LOW * h : LOW * (h + 1)] for h in range(high)], axis=0)
    cell = lax.broadcasted_iota(jnp.int32, (LOW, SLOTS), 0)

    def step(t, total):
        at = pl.multiple_of(t * SLOTS, SLOTS)
        source = gather_ref[:, pl.ds(at, SLOTS)]
        target = scatter_ref[:, pl.ds(at, SLOTS)]
        pick = jnp.where(cell == (source & (LOW - 1)), 1.0, 0.0).astype(jnp.bfloat16)
        rows = jnp.dot(table, pick, preferred_element_type=jnp.float32)
        source_high = source >> 8
        value = jnp.zeros((16, SLOTS), jnp.float32)
        for h in range(high):
            value = value + jnp.where(source_high == h, rows[16 * h : 16 * h + 16], 0.0)
        target_high = target >> 8
        spread = jnp.concatenate(
            [jnp.where(target_high == h, value, 0.0).astype(jnp.bfloat16) for h in range(high)], axis=0
        )
        place = jnp.where(cell == (target & (LOW - 1)), 1.0, 0.0).astype(jnp.bfloat16)
        return total + lax.dot_general(
            spread, place, (((1,), (1,)), ((), ())), preferred_element_type=jnp.float32
        )

    total = lax.fori_loop(0, PLANE // SLOTS, step, jnp.zeros((16 * high, LOW), jnp.float32))
    for h in range(high):
        link_a[:, LOW * h : LOW * (h + 1)] = total[16 * h : 16 * h + 8]
        link_b[:, LOW * h : LOW * (h + 1)] = total[16 * h + 8 : 16 * h + 10]


def residual_span(ref, out_rows, diag_refs, lam, coupling, z, c, before, after, link, eig_ref, res_ref, sums):
    rows = ref.shape[0]
    base = z * PLANE + c * SPAN
    if not isinstance(base, int):
        base = pl.multiple_of(base, SPAN)

    def load(at, width):
        if not isinstance(at, int):
            at = pl.multiple_of(at, 128)
        return ref[:, pl.ds(at, width)].astype(jnp.float32)

    raw = ref[:, pl.ds(base, SPAN)]
    value = raw.astype(jnp.float32)
    edge = jnp.zeros((rows, 128), jnp.float32)
    left = load(base - 128, 128) if c > 0 else edge
    right = load(base + SPAN, 128) if c < PLANE // SPAN - 1 else edge
    wide = jnp.concatenate([left, value, right], axis=1)
    span = SPAN + 256
    total = pltpu.roll(wide, WID, 1)[:, 128 : 128 + SPAN] + pltpu.roll(wide, span - WID, 1)[:, 128 : 128 + SPAN]
    column = lax.broadcasted_iota(jnp.int32, (1, SPAN), 1) & (WID - 1)
    total = total + jnp.where(column > 0, pltpu.roll(value, 1, 1), 0.0)
    total = total + jnp.where(column < WID - 1, pltpu.roll(value, SPAN - 1, 1), 0.0)
    if before:
        total = total + load(base - PLANE, SPAN)
    if after:
        total = total + load(base + PLANE, SPAN)
    if link is not None:
        total = total + link[:, c * SPAN : (c + 1) * SPAN]
    mass, damping, stiffness = (r[:, pl.ds(base, SPAN)] for r in diag_refs)
    residual = (lam * lam * mass + lam * damping + stiffness) * value - coupling * total
    eig_ref[out_rows, pl.ds(base, SPAN)] = raw
    res_ref[out_rows, pl.ds(base, SPAN)] = residual.astype(jnp.bfloat16)
    vector_sq, residual_sq = sums
    for k in range(SPAN // 128):
        part = slice(128 * k, 128 * (k + 1))
        vector_sq = vector_sq + value[:, part] * value[:, part]
        residual_sq = residual_sq + residual[:, part] * residual[:, part]
    return vector_sq, residual_sq


def residual_all(ea, eb, diag_refs, eigen, links, eig_ref, res_ref, sums_ref):
    depth = ea.shape[1] // PLANE
    for ref, out_rows, link in ((ea, slice(0, 8), 0), (eb, slice(8, 10), 1)):
        lam = eigen[out_rows, :]
        coupling = lam * lam * 0.1 + lam * 0.3 + 1.0
        rows = ref.shape[0]

        def plane(z, sums, before, after, link_ref):
            for c in range(PLANE // SPAN):
                sums = residual_span(
                    ref, out_rows, diag_refs, lam, coupling, z, c, before, after, link_ref, eig_ref, res_ref, sums
                )
            return sums

        zero = jnp.zeros((rows, 128), jnp.float32)
        sums = plane(0, (zero, zero), False, True, links[0][link])
        sums = lax.fori_loop(1, depth - 1, lambda z, s: plane(z, s, True, True, None), sums)
        sums = plane(depth - 1, sums, True, False, links[1][link])
        sums_ref[0, out_rows, :] = sums[0]
        sums_ref[1, out_rows, :] = sums[1]


def finish_kernel(
    ea, eb, above_a, above_b, below_a, below_b, lower, upper, down_lower, down_upper,
    mass, damping, stiffness, eigen, eig_ref, res_ref, sums_ref, first_a, first_b, last_a, last_b,
):
    link_plane(below_a, below_b, down_lower, down_upper, first_a, first_b)
    link_plane(above_a, above_b, upper, lower, last_a, last_b)
    residual_all(
        ea, eb, (mass, damping, stiffness), eigen, ((first_a, first_b), (last_a, last_b)), eig_ref, res_ref, sums_ref
    )


def finish(*operands):
    rows = operands[0].shape[1]
    vmem = pl.BlockSpec(memory_space=pltpu.VMEM)
    specs = [vmem] * 14
    plane = lambda r: pltpu.VMEM((r, PLANE), jnp.float32)
    return pl.pallas_call(
        finish_kernel,
        out_shape=(
            jax.ShapeDtypeStruct((10, rows), jnp.bfloat16),
            jax.ShapeDtypeStruct((10, rows), jnp.bfloat16),
            jax.ShapeDtypeStruct((2, 10, 128), jnp.float32),
        ),
        in_specs=specs,
        out_specs=(vmem, vmem, vmem),
        scratch_shapes=[plane(8), plane(2), plane(8), plane(2)],
        compiler_params=pltpu.CompilerParams(vmem_limit_bytes=40 * 2**20),
        name="finish",
    )(*operands)


MESH = pl.DeviceIdType.MESH
PIECE = 2048
CHUNK = 4 * PIECE
HALF = PIECE // 2
ORDER = (0, 7, 1, 2, 3, 4, 5, 6)
AHEAD = 3


def exchange_kernel(
    basis, extra, coefs, lists, ea, eb, above_a, above_b, below_a, below_b, down_lists,
    ra, rb, sa, sb, own_sem, own_extra_sem, basis_sem, extra_sem, vec_a_sem, vec_b_sem, plane_sem,
):
    me, sub = lax.axis_index("vecs"), lax.axis_index("rows")
    subs = lax.axis_size("rows")
    following, previous = lax.rem(sub + 1, subs), lax.rem(sub + subs - 1, subs)
    ahead = [lax.rem(me + d, 4) for d in (1, 2, 3)]
    behind = [lax.rem(me + 4 - d, 4) for d in (1, 2, 3)]
    order = (0, 2, 1)

    barrier = pltpu.get_barrier_semaphore()
    for peer in ahead:
        pl.semaphore_signal(barrier, inc=1, device_id={"vecs": peer}, device_id_type=MESH)
    for peer in (following, previous):
        pl.semaphore_signal(barrier, inc=1, device_id={"rows": peer}, device_id_type=MESH)
    pl.semaphore_wait(barrier, 5)

    def remote(source, target, sems, at, peer):
        return pltpu.make_async_remote_copy(
            src_ref=source, dst_ref=target, send_sem=sems.at[(0, *at)], recv_sem=sems.at[(1, *at)],
            device_id=peer, device_id_type=MESH,
        )

    def columns(c, q):
        return pl.ds(pl.multiple_of(c * CHUNK + q * PIECE, PIECE), PIECE)

    def send_basis(c):
        for d in order:
            peer = ahead[d]
            for g in range(3):
                remote(
                    basis.at[pl.ds(8 * g, 8), columns(c, peer)], ra.at[c, g, me], basis_sem, (c, d, g), {"vecs": peer}
                ).start()
            remote(extra.at[c, peer], rb.at[c, me], extra_sem, (c, d), {"vecs": peer}).start()

    def own_copies(c):
        for g in range(3):
            yield pltpu.make_async_copy(
                basis.at[pl.ds(8 * g, 8), columns(c, me)], ra.at[c, g, me], own_sem.at[c, g]
            )
        yield pltpu.make_async_copy(extra.at[c, me], rb.at[c, me], own_extra_sem.at[c])

    def basis_arrivals(c):
        for d in order:
            for g in range(3):
                block = ra.at[c, g, behind[d]]
                yield remote(block, block, basis_sem, (c, d, g), {"vecs": ahead[d]})
            block = rb.at[c, behind[d]]
            yield remote(block, block, extra_sem, (c, d), {"vecs": ahead[d]})

    def vec_copies(c):
        for d in order:
            peer = ahead[d]
            yield remote(sa.at[c, peer], ea.at[:, columns(c, me)], vec_a_sem, (c, d), {"vecs": peer})
            yield remote(sb.at[c, peer], eb.at[:, columns(c, me)], vec_b_sem, (c, d), {"vecs": peer})

    def vec_arrivals(c):
        for d in order:
            block = ea.at[:, columns(c, behind[d])]
            yield remote(block, block, vec_a_sem, (c, d), {"vecs": ahead[d]})
            block = eb.at[:, columns(c, behind[d])]
            yield remote(block, block, vec_b_sem, (c, d), {"vecs": ahead[d]})

    rows_local = basis.shape[1]
    plane_copies = {
        ORDER[0]: (
            remote(ea.at[:, pl.ds(0, PLANE)], above_a, plane_sem, (0,), {"rows": previous}),
            remote(eb.at[:, pl.ds(0, PLANE)], above_b, plane_sem, (1,), {"rows": previous}),
        ),
        ORDER[1]: (
            remote(ea.at[:, pl.ds(rows_local - PLANE, PLANE)], below_a, plane_sem, (2,), {"rows": following}),
            remote(eb.at[:, pl.ds(rows_local - PLANE, PLANE)], below_b, plane_sem, (3,), {"rows": following}),
        ),
    }
    list_copy = remote(lists, down_lists, plane_sem, (4,), {"rows": following})

    for c in ORDER[:AHEAD]:
        send_basis(c)
    list_copy.start()
    for c in ORDER:
        for copy in own_copies(c):
            copy.start()

    def product(c):
        for h in range(2):
            at = pl.ds(h * HALF, HALF)
            parts = [ra[c, g, :, :, at].reshape(32, HALF) for g in range(3)]
            odd = jnp.concatenate(
                [rb[c, q].astype(jnp.float32) for q in range(4)] + [jnp.zeros((24, HALF), jnp.float32)], axis=0
            )
            whole = jnp.concatenate([*parts, odd.astype(jnp.bfloat16)], axis=0)
            out = jnp.dot(coefs[h], whole, preferred_element_type=jnp.float32)
            for p in range(4):
                sa[c, p, :, at] = out[8 * p : 8 * p + 8].astype(jnp.bfloat16)
                sb[c, p, :, at] = out[32 + 2 * p : 34 + 2 * p].astype(jnp.bfloat16)
        ea[:, columns(c, me)] = sa[c, me]
        eb[:, columns(c, me)] = sb[c, me]

    def arrived(c):
        for copy in vec_arrivals(c):
            copy.wait_recv()
        for copy in plane_copies.get(c, ()):
            copy.start()

    for i, c in enumerate(ORDER):
        for copy in own_copies(c):
            copy.wait()
        for copy in basis_arrivals(c):
            copy.wait_recv()
        product(c)
        for copy in vec_copies(c):
            copy.start()
        if i + AHEAD < len(ORDER):
            send_basis(ORDER[i + AHEAD])
        if i >= 2:
            arrived(ORDER[i - 2])
    arrived(ORDER[-2])
    arrived(ORDER[-1])
    for copies in plane_copies.values():
        for copy in copies:
            copy.wait()
    list_copy.wait()
    for c in ORDER:
        for copy in basis_arrivals(c):
            copy.wait_send()
        for copy in vec_copies(c):
            copy.wait_send()


def exchange(basis, extra, coefs, lists):
    rows = basis.shape[1]
    chunks = rows // CHUNK
    vmem = pl.BlockSpec(memory_space=pltpu.VMEM)
    hbm = pl.BlockSpec(memory_space=pl.ANY)
    bf16 = lambda *shape: jax.ShapeDtypeStruct(shape, jnp.bfloat16)
    dma = pltpu.SemaphoreType.DMA
    return pl.pallas_call(
        exchange_kernel,
        out_shape=(
            bf16(8, rows), bf16(2, rows), bf16(8, PLANE), bf16(2, PLANE), bf16(8, PLANE), bf16(2, PLANE),
            jax.ShapeDtypeStruct(lists.shape, jnp.int32),
        ),
        in_specs=[hbm, vmem, vmem, vmem],
        out_specs=(vmem,) * 7,
        scratch_shapes=[
            pltpu.VMEM((chunks, 3, 4, 8, PIECE), jnp.bfloat16),
            pltpu.VMEM((chunks, 4, 2, HALF), jnp.bfloat16),
            pltpu.VMEM((chunks, 4, 8, PIECE), jnp.bfloat16),
            pltpu.VMEM((chunks, 4, 2, PIECE), jnp.bfloat16),
            dma((chunks, 3)), dma((chunks,)), dma((2, chunks, 3, 3)), dma((2, chunks, 3)),
            dma((2, chunks, 3)), dma((2, chunks, 3)), dma((2, 5)),
        ],
        compiler_params=pltpu.CompilerParams(
            collective_id=0, has_side_effects=True, vmem_limit_bytes=48 * 2**20
        ),
        name="exchange",
    )(basis, extra, coefs, lists)


def spread_coefficients(coefficients):
    by_vec = coefficients.T.reshape(4, 10, 4, 25)
    ordered = jnp.concatenate([by_vec[:, :8].reshape(32, 4, 25), by_vec[:, 8:].reshape(8, 4, 25)], axis=0)
    main = ordered[:, :, :24].reshape(40, 4, 3, 8).transpose(0, 2, 1, 3).reshape(40, 96)
    odd = ordered[:, :, 24]
    none = jnp.zeros_like(odd)
    pad = jnp.zeros((40, 24), coefficients.dtype)
    halves = [jnp.stack([odd, none], axis=2), jnp.stack([none, odd], axis=2)]
    return jnp.stack([jnp.concatenate([main, half.reshape(40, 8), pad], axis=1) for half in halves])


def on_device(basis, coefficients, eigen_values, stiffness, damping, mass, link_count, lower_cells, upper_cells):
    rows_local = basis.shape[1]
    extra = basis[24].reshape(rows_local // CHUNK, 4, 2, HALF)
    used = jnp.arange(lower_cells.shape[1], dtype=jnp.int32)[None, :] < link_count[0]
    lists = jnp.where(used, jnp.concatenate([lower_cells, upper_cells], axis=0), -1)
    ea, eb, above_a, above_b, below_a, below_b, down = exchange(
        basis, extra, spread_coefficients(coefficients), lists
    )
    wide = lambda a: a.reshape(1, rows_local)
    eig, res, sums = finish(
        ea, eb, above_a, above_b, below_a, below_b, lists[:1], lists[1:], down[:1], down[1:],
        wide(mass), wide(damping), wide(stiffness), eigen_values[:, None],
    )
    local = jnp.sum(sums, axis=2).reshape(1, 20)
    devices = lax.axis_size("rows")
    totals = lax.all_to_all(jnp.broadcast_to(local[None], (devices, 1, 20)), "rows", 0, 0, tiled=True).sum(axis=0)
    totals = totals.reshape(2, 10)
    norms = jnp.sqrt(totals[1]) / jnp.sqrt(totals[0] + 1.0)
    return eig, res, norms


def solution(mesh):
    placed = (
        P("vecs", "rows"), P(), P("vecs"), P("rows"), P("rows"), P("rows"), P("rows"), P("rows", None), P("rows", None),
    )
    return jax.shard_map(
        on_device,
        mesh=mesh,
        in_specs=placed,
        out_specs=(P("vecs", "rows"), P("vecs", "rows"), P("vecs")),
        check_vma=False,
    )
```

```python
import functools

import jax
import jax.numpy as jnp
from jax import lax
from jax.experimental import pallas as pl
from jax.experimental.pallas import tpu as pltpu
from jax.sharding import PartitionSpec as P

WID = 64
PLANE = WID * WID
SPAN = 1024
SLOTS = 512
LOW = 256


def link_plane(part_a, part_b, lists, gather, scatter, link_a, link_b):
    high = PLANE // LOW
    whole = jnp.concatenate(
        [part_a[...].astype(jnp.float32), part_b[...].astype(jnp.float32), jnp.zeros((6, PLANE), jnp.float32)], axis=0
    ).astype(jnp.bfloat16)
    table = jnp.concatenate([whole[:, LOW * h : LOW * (h + 1)] for h in range(high)], axis=0)
    cell = lax.broadcasted_iota(jnp.int32, (LOW, SLOTS), 0)

    def step(t, total):
        at = pl.multiple_of(t * SLOTS, SLOTS)
        source = lists[gather : gather + 1, pl.ds(at, SLOTS)]
        target = lists[scatter : scatter + 1, pl.ds(at, SLOTS)]
        pick = jnp.where(cell == (source & (LOW - 1)), 1.0, 0.0).astype(jnp.bfloat16)
        rows = jnp.dot(table, pick, preferred_element_type=jnp.float32)
        source_high = source >> 8
        value = jnp.zeros((16, SLOTS), jnp.float32)
        for h in range(high):
            value = value + jnp.where(source_high == h, rows[16 * h : 16 * h + 16], 0.0)
        target_high = target >> 8
        spread = jnp.concatenate(
            [jnp.where(target_high == h, value, 0.0).astype(jnp.bfloat16) for h in range(high)], axis=0
        )
        place = jnp.where(cell == (target & (LOW - 1)), 1.0, 0.0).astype(jnp.bfloat16)
        return total + lax.dot_general(
            spread, place, (((1,), (1,)), ((), ())), preferred_element_type=jnp.float32
        )

    total = lax.fori_loop(0, PLANE // SLOTS, step, jnp.zeros((16 * high, LOW), jnp.float32))
    for h in range(high):
        link_a[:, LOW * h : LOW * (h + 1)] = total[16 * h : 16 * h + 8]
        link_b[:, LOW * h : LOW * (h + 1)] = total[16 * h + 8 : 16 * h + 10]


def residual_spans(vecs, outs, diag_refs, eigen, first, planes, links, sums):
    eig_ref, res_ref = outs
    depth = eig_ref.shape[1] // PLANE
    spans = PLANE // SPAN
    column = lax.broadcasted_iota(jnp.int32, (1, SPAN), 1) & (WID - 1)
    groups = ((vecs[0], slice(0, 8)), (vecs[1], slice(8, 10)))
    factors = []
    for _, part in groups:
        lam = eigen[part]
        factors.append((lam, lam * lam, lam * lam * 0.1 + lam * 0.3 + 1.0))

    def step(i, totals):
        c = i % spans
        base = pl.multiple_of(first * PLANE + i * SPAN, SPAN)
        here = pl.ds(base, SPAN)
        before = pl.ds(pl.multiple_of(jnp.where(c > 0, base - 128, base), 128), 128)
        after = pl.ds(pl.multiple_of(jnp.where(c < spans - 1, base + SPAN, base), 128), 128)
        mass, damping, stiffness = (r[:, here] for r in diag_refs)
        done = []
        for k, (ref, part) in enumerate(groups):
            lam, square, coupling = factors[k]
            raw = ref[:, here]
            value = raw.astype(jnp.float32)
            left = jnp.where(c > 0, ref[:, before].astype(jnp.float32), 0.0)
            right = jnp.where(c < spans - 1, ref[:, after].astype(jnp.float32), 0.0)
            wide = jnp.concatenate([left, value, right], axis=1)
            span = SPAN + 256
            total = pltpu.roll(wide, WID, 1)[:, 128 : 128 + SPAN] + pltpu.roll(wide, span - WID, 1)[:, 128 : 128 + SPAN]
            total = total + jnp.where(column > 0, pltpu.roll(value, 1, 1), 0.0)
            total = total + jnp.where(column < WID - 1, pltpu.roll(value, SPAN - 1, 1), 0.0)
            if not (links is not None and first == 0):
                total = total + ref[:, pl.ds(pl.multiple_of(base - PLANE, SPAN), SPAN)].astype(jnp.float32)
            if not (links is not None and first == depth - 1):
                total = total + ref[:, pl.ds(pl.multiple_of(base + PLANE, SPAN), SPAN)].astype(jnp.float32)
            if links is not None:
                total = total + links[k][:, pl.ds(pl.multiple_of(i * SPAN, SPAN), SPAN)]
            residual = (square * mass + lam * damping + stiffness) * value - coupling * total
            eig_ref[part, here] = raw
            res_ref[part, here] = residual.astype(jnp.bfloat16)
            vector_sq, residual_sq = totals[2 * k], totals[2 * k + 1]
            for t in range(SPAN // 128):
                lanes = slice(128 * t, 128 * (t + 1))
                vector_sq = vector_sq + value[:, lanes] * value[:, lanes]
                residual_sq = residual_sq + residual[:, lanes] * residual[:, lanes]
            done += [vector_sq, residual_sq]
        return tuple(done)

    totals = lax.fori_loop(0, planes * spans, step, tuple(ref[...] for ref in sums))
    for ref, total in zip(sums, totals):
        ref[...] = total


def column_of(row):
    n = row.shape[1]
    same = lax.broadcasted_iota(jnp.int32, (n, n), 0) == lax.broadcasted_iota(jnp.int32, (n, n), 1)
    return jnp.sum(jnp.where(same, row, 0.0), axis=1, keepdims=True)


def spread_coefficients(coefficients, coefs):
    out = lax.broadcasted_iota(jnp.int32, (40, 40), 0)
    vec = lax.broadcasted_iota(jnp.int32, (40, 40), 1)
    rest = out - 32
    wanted = jnp.where(out < 32, 10 * (out >> 3) + (out & 7), 10 * (rest >> 1) + 8 + (rest & 1))
    rows = jnp.where(vec == wanted, 1.0, 0.0).astype(jnp.bfloat16)
    ordered = jnp.dot(rows, coefficients[...], preferred_element_type=jnp.float32).astype(jnp.bfloat16)
    rank = lax.broadcasted_iota(jnp.int32, (100, 128), 0)
    at = lax.broadcasted_iota(jnp.int32, (100, 128), 1)
    odd = at - 96
    for h in range(2):
        main = 25 * ((at >> 3) & 3) + 8 * (at >> 5) + (at & 7)
        other = jnp.where((odd < 8) & ((odd & 1) == h), 25 * (odd >> 1) + 24, -1)
        pick = jnp.where(rank == jnp.where(at < 96, main, other), 1.0, 0.0).astype(jnp.bfloat16)
        coefs[h] = jnp.dot(ordered, pick, preferred_element_type=jnp.float32).astype(jnp.bfloat16)


MESH = pl.DeviceIdType.MESH
PIECE = 2048
CHUNK = 4 * PIECE
HALF = PIECE // 2
ORDER = (0, 7, 1, 2, 3, 4, 5, 6)
AHEAD = 3


def whole_kernel(
    basis, coefficients, lists, mass, damping, stiffness, eigen_row, eig_ref, res_ref, norm_ref,
    odd_rows, extra, coefs, ea, eb, above_a, above_b, below_a, below_b, down_lists, ra, rb, sa, sb,
    first_a, first_b, last_a, last_b, square_a, residual_a, square_b, residual_b, squares,
    own_sem, odd_sem, basis_sem, extra_sem, vec_a_sem, vec_b_sem, plane_sem, square_sem,
):
    me, sub = lax.axis_index("vecs"), lax.axis_index("rows")
    subs = lax.axis_size("rows")
    following, previous = lax.rem(sub + 1, subs), lax.rem(sub + subs - 1, subs)
    ahead = [lax.rem(me + d, 4) for d in (1, 2, 3)]
    behind = [lax.rem(me + 4 - d, 4) for d in (1, 2, 3)]
    order = (0, 2, 1)

    barrier = pltpu.get_barrier_semaphore()
    for peer in ahead:
        pl.semaphore_signal(barrier, inc=1, device_id={"vecs": peer}, device_id_type=MESH)

    @pl.loop(1, subs)
    def _(d):
        pl.semaphore_signal(barrier, inc=1, device_id={"rows": lax.rem(sub + d, subs)}, device_id_type=MESH)

    def remote(source, target, sems, at, peer):
        return pltpu.make_async_remote_copy(
            src_ref=source, dst_ref=target, send_sem=sems.at[(0, *at)], recv_sem=sems.at[(1, *at)],
            device_id=peer, device_id_type=MESH,
        )

    def columns(c, q):
        return pl.ds(pl.multiple_of(c * CHUNK + q * PIECE, PIECE), PIECE)

    def send_basis(c):
        for d in order:
            peer = ahead[d]
            for g in range(3):
                remote(
                    basis.at[pl.ds(8 * g, 8), columns(c, peer)], ra.at[c, g, me], basis_sem, (c, d, g), {"vecs": peer}
                ).start()

    def send_extra(c):
        for d in order:
            peer = ahead[d]
            remote(extra.at[c, peer], rb.at[c, me], extra_sem, (c, d), {"vecs": peer}).start()

    def own_copies(c):
        for g in range(3):
            yield pltpu.make_async_copy(
                basis.at[pl.ds(8 * g, 8), columns(c, me)], ra.at[c, g, me], own_sem.at[c, g]
            )

    def basis_arrivals(c):
        for d in order:
            for g in range(3):
                block = ra.at[c, g, behind[d]]
                yield remote(block, block, basis_sem, (c, d, g), {"vecs": ahead[d]})
            block = rb.at[c, behind[d]]
            yield remote(block, block, extra_sem, (c, d), {"vecs": ahead[d]})

    def vec_copies(c):
        for d in order:
            peer = ahead[d]
            yield remote(sa.at[c, peer], ea.at[:, columns(c, me)], vec_a_sem, (c, d), {"vecs": peer})
            yield remote(sb.at[c, peer], eb.at[:, columns(c, me)], vec_b_sem, (c, d), {"vecs": peer})

    def vec_arrivals(c):
        for d in order:
            block = ea.at[:, columns(c, behind[d])]
            yield remote(block, block, vec_a_sem, (c, d), {"vecs": ahead[d]})
            block = eb.at[:, columns(c, behind[d])]
            yield remote(block, block, vec_b_sem, (c, d), {"vecs": ahead[d]})

    rows_local = basis.shape[1]
    plane_copies = {
        ORDER[0]: (
            remote(ea.at[:, pl.ds(0, PLANE)], above_a, plane_sem, (0,), {"rows": previous}),
            remote(eb.at[:, pl.ds(0, PLANE)], above_b, plane_sem, (1,), {"rows": previous}),
        ),
        ORDER[1]: (
            remote(ea.at[:, pl.ds(rows_local - PLANE, PLANE)], below_a, plane_sem, (2,), {"rows": following}),
            remote(eb.at[:, pl.ds(rows_local - PLANE, PLANE)], below_b, plane_sem, (3,), {"rows": following}),
        ),
    }
    list_copy = remote(lists, down_lists, plane_sem, (4,), {"rows": following})

    odd_copy = pltpu.make_async_copy(basis.at[pl.ds(24, 1), :], odd_rows, odd_sem)
    odd_copy.start()
    for c in ORDER:
        for copy in own_copies(c):
            copy.start()
    spread_coefficients(coefficients, coefs)
    pl.semaphore_wait(barrier, subs + 2)
    for c in ORDER[:AHEAD]:
        send_basis(c)
    list_copy.start()
    odd_copy.wait()
    for c in ORDER:
        for q in range(4):
            at = c * CHUNK + q * PIECE
            pair = [odd_rows[0:1, at + h * HALF : at + (h + 1) * HALF].astype(jnp.float32) for h in range(2)]
            extra[c, q] = jnp.concatenate(pair, axis=0).astype(jnp.bfloat16)
    for c in ORDER:
        rb[c, me] = extra[c, me]
    for c in ORDER[:AHEAD]:
        send_extra(c)
    sums = (square_a, residual_a, square_b, residual_b)
    for ref in sums:
        ref[...] = jnp.zeros_like(ref)
    eigen = column_of(eigen_row[...])
    diag_refs = (mass, damping, stiffness)

    def planes_done(first, planes, links=None):
        residual_spans((ea, eb), (eig_ref, res_ref), diag_refs, eigen, first, planes, links, sums)

    def product(c):
        for h in range(2):
            at = pl.ds(h * HALF, HALF)
            parts = [ra[c, g, :, :, at].reshape(32, HALF) for g in range(3)]
            odd = jnp.concatenate(
                [rb[c, q].astype(jnp.float32) for q in range(4)] + [jnp.zeros((24, HALF), jnp.float32)], axis=0
            )
            whole = jnp.concatenate([*parts, odd.astype(jnp.bfloat16)], axis=0)
            out = jnp.dot(coefs[h], whole, preferred_element_type=jnp.float32)
            for p in range(4):
                sa[c, p, :, at] = out[8 * p : 8 * p + 8].astype(jnp.bfloat16)
                sb[c, p, :, at] = out[32 + 2 * p : 34 + 2 * p].astype(jnp.bfloat16)
        ea[:, columns(c, me)] = sa[c, me]
        eb[:, columns(c, me)] = sb[c, me]

    def arrived(c):
        for copy in vec_arrivals(c):
            copy.wait_recv()
        for copy in plane_copies.get(c, ()):
            copy.start()

    def first_links():
        for copy in plane_copies[ORDER[1]]:
            copy.wait_recv()
        list_copy.wait_recv()
        link_plane(below_a, below_b, down_lists, 0, 1, first_a, first_b)

    def last_links():
        for copy in plane_copies[ORDER[0]]:
            copy.wait_recv()
        link_plane(above_a, above_b, lists, 1, 0, last_a, last_b)

    def outer_planes():
        planes_done(0, 1, (first_a, first_b))
        planes_done(rows_local // PLANE - 1, 1, (last_a, last_b))

    later = {5: first_links, 6: last_links, 7: outer_planes}
    for i, c in enumerate(ORDER):
        for copy in own_copies(c):
            copy.wait()
        for copy in basis_arrivals(c):
            copy.wait_recv()
        product(c)
        for copy in vec_copies(c):
            copy.start()
        if i + AHEAD < len(ORDER):
            send_basis(ORDER[i + AHEAD])
            send_extra(ORDER[i + AHEAD])
        if i >= 2:
            arrived(ORDER[i - 2])
            if i >= 4:
                planes_done(2 * ORDER[i - 2] - 1, 2)
        if i in later:
            later[i]()
    arrived(ORDER[-2])
    planes_done(2 * ORDER[-2] - 1, 2)
    arrived(ORDER[-1])
    planes_done(2 * ORDER[-1] - 1, 4)

    lane = lax.broadcasted_iota(jnp.int32, (1, 128), 1)
    message = jnp.zeros((1, 128), jnp.float32)
    for ref, start in ((square_a, 0), (square_b, 8), (residual_a, 16), (residual_b, 24)):
        column = jnp.sum(ref[...], axis=1, keepdims=True)
        row = lax.broadcasted_iota(jnp.int32, (ref.shape[0], 128), 0) + start
        message = message + jnp.sum(jnp.where(row == lane, column, 0.0), axis=0, keepdims=True)
    squares[sub] = message

    def square_copy(d):
        return remote(squares.at[sub], squares.at[sub], square_sem, (d,), {"rows": lax.rem(sub + d, subs)})

    @pl.loop(1, subs)
    def _(d):
        square_copy(d).start()

    for copies in plane_copies.values():
        for copy in copies:
            copy.wait_send()
    list_copy.wait_send()
    for c in ORDER:
        for copy in basis_arrivals(c):
            copy.wait_send()
        for copy in vec_copies(c):
            copy.wait_send()

    @pl.loop(1, subs)
    def _(d):
        block = squares.at[lax.rem(sub + subs - d, subs)]
        remote(block, block, square_sem, (d,), {"rows": lax.rem(sub + d, subs)}).wait_recv()

    @pl.loop(1, subs)
    def _(d):
        square_copy(d).wait_send()

    total = jnp.sum(squares[...], axis=0)
    norms = jnp.sqrt(pltpu.roll(total, 112, 1)) / jnp.sqrt(total + 1.0)
    norm_ref[...] = norms[:, :10]


def whole(basis, coefficients, lists, mass, damping, stiffness, eigen_row):
    rows = basis.shape[1]
    chunks = rows // CHUNK
    subs = lax.axis_size("rows")
    vmem = pl.BlockSpec(memory_space=pltpu.VMEM)
    f32 = lambda *shape: pltpu.VMEM(shape, jnp.float32)
    bf16 = lambda *shape: pltpu.VMEM(shape, jnp.bfloat16)
    dma = pltpu.SemaphoreType.DMA
    return pl.pallas_call(
        whole_kernel,
        out_shape=(
            jax.ShapeDtypeStruct((10, rows), jnp.bfloat16),
            jax.ShapeDtypeStruct((10, rows), jnp.bfloat16),
            jax.ShapeDtypeStruct((1, 10), jnp.float32),
        ),
        in_specs=[pl.BlockSpec(memory_space=pltpu.HBM)] + [vmem] * 6,
        out_specs=(vmem,) * 3,
        scratch_shapes=[
            bf16(1, rows), bf16(chunks, 4, 2, HALF), bf16(2, 40, 128), bf16(8, rows), bf16(2, rows),
            bf16(8, PLANE), bf16(2, PLANE), bf16(8, PLANE), bf16(2, PLANE), pltpu.VMEM(lists.shape, jnp.int32),
            bf16(chunks, 3, 4, 8, PIECE), bf16(chunks, 4, 2, HALF), bf16(chunks, 4, 8, PIECE), bf16(chunks, 4, 2, PIECE),
            f32(8, PLANE), f32(2, PLANE), f32(8, PLANE), f32(2, PLANE),
            f32(8, 128), f32(8, 128), f32(2, 128), f32(2, 128), f32(subs, 1, 128),
            dma((chunks, 3)), dma(()), dma((2, chunks, 3, 3)), dma((2, chunks, 3)),
            dma((2, chunks, 3)), dma((2, chunks, 3)), dma((2, 5)), dma((2, subs)),
        ],
        compiler_params=pltpu.CompilerParams(
            collective_id=0, has_side_effects=True, vmem_limit_bytes=48 * 2**20
        ),
        name="whole",
    )(basis, coefficients, lists, mass, damping, stiffness, eigen_row)


def on_device(basis, coefficients, eigen_values, stiffness, damping, mass, link_count, lower_cells, upper_cells):
    rows_local = basis.shape[1]
    used = jnp.arange(lower_cells.shape[1], dtype=jnp.int32)[None, :] < link_count[0]
    lists = jnp.where(used, jnp.concatenate([lower_cells, upper_cells], axis=0), -1)
    wide = lambda a: a.reshape(1, rows_local)
    eig, res, norms = whole(
        basis, coefficients.T, lists, wide(mass), wide(damping), wide(stiffness), eigen_values[None, :]
    )
    return eig, res, norms.reshape(10)


def solution(mesh):
    placed = (
        P("vecs", "rows"), P(), P("vecs"), P("rows"), P("rows"), P("rows"), P("rows"), P("rows", None), P("rows", None),
    )
    return jax.shard_map(
        on_device,
        mesh=mesh,
        in_specs=placed,
        out_specs=(P("vecs", "rows"), P("vecs", "rows"), P("vecs")),
        check_vma=False,
    )
```

```python
import functools

import jax
import jax.numpy as jnp
from jax import lax
from jax.experimental import pallas as pl
from jax.experimental.pallas import tpu as pltpu
from jax.sharding import PartitionSpec as P

WID = 64
PLANE = WID * WID
SPAN = 1024
SLOTS = 512
LOW = 256


def link_plane(part_a, part_b, lists, gather, scatter, link_a, link_b):
    high = PLANE // LOW
    whole = jnp.concatenate(
        [part_a[...].astype(jnp.float32), part_b[...].astype(jnp.float32), jnp.zeros((6, PLANE), jnp.float32)], axis=0
    ).astype(jnp.bfloat16)
    table = jnp.concatenate([whole[:, LOW * h : LOW * (h + 1)] for h in range(high)], axis=0)
    cell = lax.broadcasted_iota(jnp.int32, (LOW, SLOTS), 0)

    def step(t, total):
        at = pl.multiple_of(t * SLOTS, SLOTS)
        source = lists[gather : gather + 1, pl.ds(at, SLOTS)]
        target = lists[scatter : scatter + 1, pl.ds(at, SLOTS)]
        pick = jnp.where(cell == (source & (LOW - 1)), 1.0, 0.0).astype(jnp.bfloat16)
        rows = jnp.dot(table, pick, preferred_element_type=jnp.float32)
        source_high = source >> 8
        value = jnp.zeros((16, SLOTS), jnp.float32)
        for h in range(high):
            value = value + jnp.where(source_high == h, rows[16 * h : 16 * h + 16], 0.0)
        target_high = target >> 8
        spread = jnp.concatenate(
            [jnp.where(target_high == h, value, 0.0).astype(jnp.bfloat16) for h in range(high)], axis=0
        )
        place = jnp.where(cell == (target & (LOW - 1)), 1.0, 0.0).astype(jnp.bfloat16)
        return total + lax.dot_general(
            spread, place, (((1,), (1,)), ((), ())), preferred_element_type=jnp.float32
        )

    total = lax.fori_loop(0, PLANE // SLOTS, step, jnp.zeros((16 * high, LOW), jnp.float32))
    for h in range(high):
        link_a[:, LOW * h : LOW * (h + 1)] = total[16 * h : 16 * h + 8]
        link_b[:, LOW * h : LOW * (h + 1)] = total[16 * h + 8 : 16 * h + 10]


def residual_spans(vecs, outs, diag_refs, eigen, first, planes, links, sums):
    eig_ref, res_ref = outs
    depth = eig_ref.shape[1] // PLANE
    spans = PLANE // SPAN
    column = lax.broadcasted_iota(jnp.int32, (1, SPAN), 1) & (WID - 1)
    groups = ((vecs[0], slice(0, 8)), (vecs[1], slice(8, 10)))
    factors = []
    for _, part in groups:
        lam = eigen[part]
        factors.append((lam, lam * lam, lam * lam * 0.1 + lam * 0.3 + 1.0))

    def step(i, totals):
        c = i % spans
        base = pl.multiple_of(first * PLANE + i * SPAN, SPAN)
        here = pl.ds(base, SPAN)
        before = pl.ds(pl.multiple_of(jnp.where(c > 0, base - 128, base), 128), 128)
        after = pl.ds(pl.multiple_of(jnp.where(c < spans - 1, base + SPAN, base), 128), 128)
        mass, damping, stiffness = (r[:, here] for r in diag_refs)
        done = []
        for k, (ref, part) in enumerate(groups):
            lam, square, coupling = factors[k]
            raw = ref[:, here]
            value = raw.astype(jnp.float32)
            left = jnp.where(c > 0, ref[:, before].astype(jnp.float32), 0.0)
            right = jnp.where(c < spans - 1, ref[:, after].astype(jnp.float32), 0.0)
            wide = jnp.concatenate([left, value, right], axis=1)
            span = SPAN + 256
            total = pltpu.roll(wide, WID, 1)[:, 128 : 128 + SPAN] + pltpu.roll(wide, span - WID, 1)[:, 128 : 128 + SPAN]
            total = total + jnp.where(column > 0, pltpu.roll(value, 1, 1), 0.0)
            total = total + jnp.where(column < WID - 1, pltpu.roll(value, SPAN - 1, 1), 0.0)
            if not (links is not None and first == 0):
                total = total + ref[:, pl.ds(pl.multiple_of(base - PLANE, SPAN), SPAN)].astype(jnp.float32)
            if not (links is not None and first == depth - 1):
                total = total + ref[:, pl.ds(pl.multiple_of(base + PLANE, SPAN), SPAN)].astype(jnp.float32)
            if links is not None:
                total = total + links[k][:, pl.ds(pl.multiple_of(i * SPAN, SPAN), SPAN)]
            residual = (square * mass + lam * damping + stiffness) * value - coupling * total
            eig_ref[part, here] = raw
            res_ref[part, here] = residual.astype(jnp.bfloat16)
            vector_sq, residual_sq = totals[2 * k], totals[2 * k + 1]
            for t in range(SPAN // 128):
                lanes = slice(128 * t, 128 * (t + 1))
                vector_sq = vector_sq + value[:, lanes] * value[:, lanes]
                residual_sq = residual_sq + residual[:, lanes] * residual[:, lanes]
            done += [vector_sq, residual_sq]
        return tuple(done)

    totals = lax.fori_loop(0, planes * spans, step, tuple(ref[...] for ref in sums))
    for ref, total in zip(sums, totals):
        ref[...] = total


def column_of(row):
    n = row.shape[1]
    same = lax.broadcasted_iota(jnp.int32, (n, n), 0) == lax.broadcasted_iota(jnp.int32, (n, n), 1)
    return jnp.sum(jnp.where(same, row, 0.0), axis=1, keepdims=True)


def spread_coefficients(coefficients, coefs):
    out = lax.broadcasted_iota(jnp.int32, (40, 40), 0)
    vec = lax.broadcasted_iota(jnp.int32, (40, 40), 1)
    rest = out - 32
    wanted = jnp.where(out < 32, 10 * (out >> 3) + (out & 7), 10 * (rest >> 1) + 8 + (rest & 1))
    rows = jnp.where(vec == wanted, 1.0, 0.0).astype(jnp.bfloat16)
    ordered = jnp.dot(rows, coefficients[...], preferred_element_type=jnp.float32).astype(jnp.bfloat16)
    rank = lax.broadcasted_iota(jnp.int32, (100, 128), 0)
    at = lax.broadcasted_iota(jnp.int32, (100, 128), 1)
    odd = at - 96
    for h in range(2):
        main = 25 * ((at >> 3) & 3) + 8 * (at >> 5) + (at & 7)
        other = jnp.where((odd < 8) & ((odd & 1) == h), 25 * (odd >> 1) + 24, -1)
        pick = jnp.where(rank == jnp.where(at < 96, main, other), 1.0, 0.0).astype(jnp.bfloat16)
        coefs[h] = jnp.dot(ordered, pick, preferred_element_type=jnp.float32).astype(jnp.bfloat16)


MESH = pl.DeviceIdType.MESH
PIECE = 2048
CHUNK = 4 * PIECE
HALF = PIECE // 2
ORDER = (0, 7, 1, 2, 3, 4, 5, 6)
AHEAD = 3


def whole_kernel(
    count, basis, coefficients_in, lower_in, upper_in, mass_in, damping_in, stiffness_in, eigen_in,
    eig_out, res_out, norm_ref, eig_ref, res_ref, coefficients, lower, upper, mass, damping, stiffness, eigen_row, lists,
    odd_rows, extra, coefs, ea, eb, above_a, above_b, below_a, below_b, down_lists, ra, rb, sa, sb,
    first_a, first_b, last_a, last_b, square_a, residual_a, square_b, residual_b, squares,
    output_sem, input_sem, own_sem, odd_sem, basis_sem, extra_sem, vec_a_sem, vec_b_sem, plane_sem, square_sem,
):
    me, sub = lax.axis_index("vecs"), lax.axis_index("rows")
    subs = lax.axis_size("rows")
    following, previous = lax.rem(sub + 1, subs), lax.rem(sub + subs - 1, subs)
    ahead = [lax.rem(me + d, 4) for d in (1, 2, 3)]
    behind = [lax.rem(me + 4 - d, 4) for d in (1, 2, 3)]
    order = (0, 2, 1)

    barrier = pltpu.get_barrier_semaphore()
    for peer in ahead:
        pl.semaphore_signal(barrier, inc=1, device_id={"vecs": peer}, device_id_type=MESH)

    @pl.loop(1, subs)
    def _(d):
        pl.semaphore_signal(barrier, inc=1, device_id={"rows": lax.rem(sub + d, subs)}, device_id_type=MESH)

    def remote(source, target, sems, at, peer):
        return pltpu.make_async_remote_copy(
            src_ref=source, dst_ref=target, send_sem=sems.at[(0, *at)], recv_sem=sems.at[(1, *at)],
            device_id=peer, device_id_type=MESH,
        )

    def columns(c, q):
        return pl.ds(pl.multiple_of(c * CHUNK + q * PIECE, PIECE), PIECE)

    def send_basis(c):
        for d in order:
            peer = ahead[d]
            for g in range(3):
                remote(
                    basis.at[pl.ds(8 * g, 8), columns(c, peer)], ra.at[c, g, me], basis_sem, (c, d, g), {"vecs": peer}
                ).start()

    def send_extra(c):
        for d in order:
            peer = ahead[d]
            remote(extra.at[c, peer], rb.at[c, me], extra_sem, (c, d), {"vecs": peer}).start()

    def own_copies(c):
        for g in range(3):
            yield pltpu.make_async_copy(
                basis.at[pl.ds(8 * g, 8), columns(c, me)], ra.at[c, g, me], own_sem.at[c, g]
            )

    def basis_arrivals(c):
        for d in order:
            for g in range(3):
                block = ra.at[c, g, behind[d]]
                yield remote(block, block, basis_sem, (c, d, g), {"vecs": ahead[d]})
            block = rb.at[c, behind[d]]
            yield remote(block, block, extra_sem, (c, d), {"vecs": ahead[d]})

    def vec_copies(c):
        for d in order:
            peer = ahead[d]
            yield remote(sa.at[c, peer], ea.at[:, columns(c, me)], vec_a_sem, (c, d), {"vecs": peer})
            yield remote(sb.at[c, peer], eb.at[:, columns(c, me)], vec_b_sem, (c, d), {"vecs": peer})

    def vec_arrivals(c):
        for d in order:
            block = ea.at[:, columns(c, behind[d])]
            yield remote(block, block, vec_a_sem, (c, d), {"vecs": ahead[d]})
            block = eb.at[:, columns(c, behind[d])]
            yield remote(block, block, vec_b_sem, (c, d), {"vecs": ahead[d]})

    rows_local = basis.shape[1]
    plane_copies = {
        ORDER[0]: (
            remote(ea.at[:, pl.ds(0, PLANE)], above_a, plane_sem, (0,), {"rows": previous}),
            remote(eb.at[:, pl.ds(0, PLANE)], above_b, plane_sem, (1,), {"rows": previous}),
        ),
        ORDER[1]: (
            remote(ea.at[:, pl.ds(rows_local - PLANE, PLANE)], below_a, plane_sem, (2,), {"rows": following}),
            remote(eb.at[:, pl.ds(rows_local - PLANE, PLANE)], below_b, plane_sem, (3,), {"rows": following}),
        ),
    }
    list_copy = remote(lists, down_lists, plane_sem, (4,), {"rows": following})

    inputs = [
        pltpu.make_async_copy(source, target, input_sem.at[i])
        for i, (source, target) in enumerate((
            (coefficients_in, coefficients), (lower_in, lower), (upper_in, upper), (eigen_in, eigen_row),
            (mass_in, mass), (damping_in, damping), (stiffness_in, stiffness),
        ))
    ]
    inputs[0].start()
    odd_copy = pltpu.make_async_copy(basis.at[pl.ds(24, 1), :], odd_rows, odd_sem)
    odd_copy.start()
    for c in ORDER:
        for copy in own_copies(c):
            copy.start()
    for copy in inputs[1:]:
        copy.start()
    for copy in inputs[:4]:
        copy.wait()
    spread_coefficients(coefficients, coefs)
    used = lax.broadcasted_iota(jnp.int32, (1, PLANE), 1) < count[0]
    lists[0:1, :] = jnp.where(used, lower[...], -1)
    lists[1:2, :] = jnp.where(used, upper[...], -1)
    pl.semaphore_wait(barrier, subs + 2)
    for c in ORDER[:AHEAD]:
        send_basis(c)
    odd_copy.wait()
    for c in ORDER:
        for q in range(4):
            at = c * CHUNK + q * PIECE
            pair = [odd_rows[0:1, at + h * HALF : at + (h + 1) * HALF].astype(jnp.float32) for h in range(2)]
            extra[c, q] = jnp.concatenate(pair, axis=0).astype(jnp.bfloat16)
    for c in ORDER:
        rb[c, me] = extra[c, me]
    for c in ORDER[:AHEAD]:
        send_extra(c)
    list_copy.start()
    sums = (square_a, residual_a, square_b, residual_b)
    for ref in sums:
        ref[...] = jnp.zeros_like(ref)
    eigen = column_of(eigen_row[...])
    diag_refs = (mass, damping, stiffness)
    for copy in inputs[4:]:
        copy.wait()

    output_copies = []

    def planes_done(first, planes, links=None):
        residual_spans((ea, eb), (eig_ref, res_ref), diag_refs, eigen, first, planes, links, sums)
        at = pl.ds(first * PLANE, planes * PLANE)
        for k, (held, out) in enumerate(((eig_ref, eig_out), (res_ref, res_out))):
            copy = pltpu.make_async_copy(held.at[:, at], out.at[:, at], output_sem.at[k, first])
            copy.start()
            output_copies.append(copy)

    def product(c):
        for h in range(2):
            at = pl.ds(h * HALF, HALF)
            parts = [ra[c, g, :, :, at].reshape(32, HALF) for g in range(3)]
            odd = jnp.concatenate(
                [rb[c, q].astype(jnp.float32) for q in range(4)] + [jnp.zeros((24, HALF), jnp.float32)], axis=0
            )
            whole = jnp.concatenate([*parts, odd.astype(jnp.bfloat16)], axis=0)
            out = jnp.dot(coefs[h], whole, preferred_element_type=jnp.float32)
            for p in range(4):
                sa[c, p, :, at] = out[8 * p : 8 * p + 8].astype(jnp.bfloat16)
                sb[c, p, :, at] = out[32 + 2 * p : 34 + 2 * p].astype(jnp.bfloat16)
        ea[:, columns(c, me)] = sa[c, me]
        eb[:, columns(c, me)] = sb[c, me]

    def arrived(c):
        for copy in vec_arrivals(c):
            copy.wait_recv()
        for copy in plane_copies.get(c, ()):
            copy.start()

    def first_links():
        for copy in plane_copies[ORDER[1]]:
            copy.wait_recv()
        list_copy.wait_recv()
        link_plane(below_a, below_b, down_lists, 0, 1, first_a, first_b)

    def last_links():
        for copy in plane_copies[ORDER[0]]:
            copy.wait_recv()
        link_plane(above_a, above_b, lists, 1, 0, last_a, last_b)

    def outer_planes():
        planes_done(0, 1, (first_a, first_b))
        planes_done(rows_local // PLANE - 1, 1, (last_a, last_b))

    later = {5: first_links, 6: last_links, 7: outer_planes}
    for i, c in enumerate(ORDER):
        for copy in own_copies(c):
            copy.wait()
        for copy in basis_arrivals(c):
            copy.wait_recv()
        product(c)
        for copy in vec_copies(c):
            copy.start()
        if i + AHEAD < len(ORDER):
            send_basis(ORDER[i + AHEAD])
            send_extra(ORDER[i + AHEAD])
        if i >= 2:
            arrived(ORDER[i - 2])
            if i >= 4:
                planes_done(2 * ORDER[i - 2] - 1, 2)
        if i in later:
            later[i]()
    arrived(ORDER[-2])
    planes_done(2 * ORDER[-2] - 1, 2)
    arrived(ORDER[-1])
    planes_done(2 * ORDER[-1] - 1, 4)

    lane = lax.broadcasted_iota(jnp.int32, (1, 128), 1)
    message = jnp.zeros((1, 128), jnp.float32)
    for ref, start in ((square_a, 0), (square_b, 8), (residual_a, 16), (residual_b, 24)):
        column = jnp.sum(ref[...], axis=1, keepdims=True)
        row = lax.broadcasted_iota(jnp.int32, (ref.shape[0], 128), 0) + start
        message = message + jnp.sum(jnp.where(row == lane, column, 0.0), axis=0, keepdims=True)
    squares[sub] = message

    def square_copy(d):
        return remote(squares.at[sub], squares.at[sub], square_sem, (d,), {"rows": lax.rem(sub + d, subs)})

    @pl.loop(1, subs)
    def _(d):
        square_copy(d).start()

    for copies in plane_copies.values():
        for copy in copies:
            copy.wait_send()
    list_copy.wait_send()
    for c in ORDER:
        for copy in basis_arrivals(c):
            copy.wait_send()
        for copy in vec_copies(c):
            copy.wait_send()

    @pl.loop(1, subs)
    def _(d):
        block = squares.at[lax.rem(sub + subs - d, subs)]
        remote(block, block, square_sem, (d,), {"rows": lax.rem(sub + d, subs)}).wait_recv()

    @pl.loop(1, subs)
    def _(d):
        square_copy(d).wait_send()

    for copy in output_copies:
        copy.wait()
    total = jnp.sum(squares[...], axis=0)
    norms = jnp.sqrt(pltpu.roll(total, 112, 1)) / jnp.sqrt(total + 1.0)
    norm_ref[...] = norms[:, :10]


def whole(count, *arrays):
    basis = arrays[0]
    rows = basis.shape[1]
    chunks = rows // CHUNK
    subs = lax.axis_size("rows")
    vmem = pl.BlockSpec(memory_space=pltpu.VMEM)
    f32 = lambda *shape: pltpu.VMEM(shape, jnp.float32)
    bf16 = lambda *shape: pltpu.VMEM(shape, jnp.bfloat16)
    dma = pltpu.SemaphoreType.DMA
    return pl.pallas_call(
        whole_kernel,
        out_shape=(
            jax.ShapeDtypeStruct((10, rows), jnp.bfloat16),
            jax.ShapeDtypeStruct((10, rows), jnp.bfloat16),
            jax.ShapeDtypeStruct((1, 10), jnp.float32),
        ),
        in_specs=[pl.BlockSpec(memory_space=pltpu.SMEM)] + [pl.BlockSpec(memory_space=pltpu.HBM)] * 8,
        out_specs=(pl.BlockSpec(memory_space=pltpu.HBM),) * 2 + (vmem,),
        scratch_shapes=[
            bf16(10, rows), bf16(10, rows), *[pltpu.VMEM(a.shape, a.dtype) for a in arrays[1:]], pltpu.VMEM((2, PLANE), jnp.int32),
            bf16(1, rows), bf16(chunks, 4, 2, HALF), bf16(2, 40, 128), bf16(8, rows), bf16(2, rows),
            bf16(8, PLANE), bf16(2, PLANE), bf16(8, PLANE), bf16(2, PLANE), pltpu.VMEM((2, PLANE), jnp.int32),
            bf16(chunks, 3, 4, 8, PIECE), bf16(chunks, 4, 2, HALF), bf16(chunks, 4, 8, PIECE), bf16(chunks, 4, 2, PIECE),
            f32(8, PLANE), f32(2, PLANE), f32(8, PLANE), f32(2, PLANE),
            f32(8, 128), f32(8, 128), f32(2, 128), f32(2, 128), f32(subs, 1, 128),
            dma((2, rows // PLANE)), dma((7,)), dma((chunks, 3)), dma(()), dma((2, chunks, 3, 3)), dma((2, chunks, 3)),
            dma((2, chunks, 3)), dma((2, chunks, 3)), dma((2, 5)), dma((2, subs)),
        ],
        compiler_params=pltpu.CompilerParams(
            collective_id=0, has_side_effects=True, vmem_limit_bytes=67_043_328
        ),
        name="whole",
    )(count, *arrays)


def on_device(basis, coefficients, eigen_values, stiffness, damping, mass, link_count, lower_cells, upper_cells):
    rows_local = basis.shape[1]
    wide = lambda a: a.reshape(1, rows_local)
    eig, res, norms = whole(
        link_count, basis, coefficients.T, lower_cells, upper_cells, wide(mass), wide(damping), wide(stiffness), eigen_values[None, :]
    )
    return eig, res, norms.reshape(10)


def solution(mesh):
    placed = (
        P("vecs", "rows"), P(), P("vecs"), P("rows"), P("rows"), P("rows"), P("rows"), P("rows", None), P("rows", None),
    )
    return jax.shard_map(
        on_device,
        mesh=mesh,
        in_specs=placed,
        out_specs=(P("vecs", "rows"), P("vecs", "rows"), P("vecs")),
        check_vma=False,
    )
```

```python
import functools

import jax
import jax.numpy as jnp
from jax import lax
from jax.experimental import pallas as pl
from jax.experimental.pallas import tpu as pltpu
from jax.sharding import PartitionSpec as P

WID = 64
PLANE = WID * WID
SPAN = 1024
SLOTS = 512
LOW = 256


def link_plane(part_a, part_b, lists, gather, scatter, link_a, link_b):
    high = PLANE // LOW
    whole = jnp.concatenate(
        [part_a[...].astype(jnp.float32), part_b[...].astype(jnp.float32), jnp.zeros((6, PLANE), jnp.float32)], axis=0
    ).astype(jnp.bfloat16)
    table = jnp.concatenate([whole[:, LOW * h : LOW * (h + 1)] for h in range(high)], axis=0)
    cell = lax.broadcasted_iota(jnp.int32, (LOW, SLOTS), 0)

    def step(t, total):
        at = pl.multiple_of(t * SLOTS, SLOTS)
        source = lists[gather : gather + 1, pl.ds(at, SLOTS)]
        target = lists[scatter : scatter + 1, pl.ds(at, SLOTS)]
        pick = jnp.where(cell == (source & (LOW - 1)), 1.0, 0.0).astype(jnp.bfloat16)
        rows = jnp.dot(table, pick, preferred_element_type=jnp.float32)
        source_high = source >> 8
        value = jnp.zeros((16, SLOTS), jnp.float32)
        for h in range(high):
            value = value + jnp.where(source_high == h, rows[16 * h : 16 * h + 16], 0.0)
        target_high = target >> 8
        spread = jnp.concatenate(
            [jnp.where(target_high == h, value, 0.0).astype(jnp.bfloat16) for h in range(high)], axis=0
        )
        place = jnp.where(cell == (target & (LOW - 1)), 1.0, 0.0).astype(jnp.bfloat16)
        return total + lax.dot_general(
            spread, place, (((1,), (1,)), ((), ())), preferred_element_type=jnp.float32
        )

    total = lax.fori_loop(0, PLANE // SLOTS, step, jnp.zeros((16 * high, LOW), jnp.float32))
    for h in range(high):
        link_a[:, LOW * h : LOW * (h + 1)] = total[16 * h : 16 * h + 8]
        link_b[:, LOW * h : LOW * (h + 1)] = total[16 * h + 8 : 16 * h + 10]


def residual_spans(vecs, outs, diag_refs, eigen, first, planes, links, sums):
    eig_ref, res_ref = outs
    depth = eig_ref.shape[1] // PLANE
    spans = PLANE // SPAN
    column = lax.broadcasted_iota(jnp.int32, (1, SPAN), 1) & (WID - 1)
    groups = ((vecs[0], slice(0, 8)), (vecs[1], slice(8, 10)))
    factors = []
    for _, part in groups:
        lam = eigen[part]
        factors.append((lam, lam * lam, lam * lam * 0.1 + lam * 0.3 + 1.0))

    def step(i, totals):
        c = i % spans
        base = pl.multiple_of(first * PLANE + i * SPAN, SPAN)
        here = pl.ds(base, SPAN)
        before = pl.ds(pl.multiple_of(jnp.where(c > 0, base - 128, base), 128), 128)
        after = pl.ds(pl.multiple_of(jnp.where(c < spans - 1, base + SPAN, base), 128), 128)
        mass, damping, stiffness = (r[:, here] for r in diag_refs)
        done = []
        for k, (ref, part) in enumerate(groups):
            lam, square, coupling = factors[k]
            raw = ref[:, here]
            value = raw.astype(jnp.float32)
            left = jnp.where(c > 0, ref[:, before].astype(jnp.float32), 0.0)
            right = jnp.where(c < spans - 1, ref[:, after].astype(jnp.float32), 0.0)
            wide = jnp.concatenate([left, value, right], axis=1)
            span = SPAN + 256
            total = pltpu.roll(wide, WID, 1)[:, 128 : 128 + SPAN] + pltpu.roll(wide, span - WID, 1)[:, 128 : 128 + SPAN]
            total = total + jnp.where(column > 0, pltpu.roll(value, 1, 1), 0.0)
            total = total + jnp.where(column < WID - 1, pltpu.roll(value, SPAN - 1, 1), 0.0)
            if not (links is not None and first == 0):
                total = total + ref[:, pl.ds(pl.multiple_of(base - PLANE, SPAN), SPAN)].astype(jnp.float32)
            if not (links is not None and first == depth - 1):
                total = total + ref[:, pl.ds(pl.multiple_of(base + PLANE, SPAN), SPAN)].astype(jnp.float32)
            if links is not None:
                total = total + links[k][:, pl.ds(pl.multiple_of(i * SPAN, SPAN), SPAN)]
            residual = (square * mass + lam * damping + stiffness) * value - coupling * total
            eig_ref[part, here] = raw
            res_ref[part, here] = residual.astype(jnp.bfloat16)
            vector_sq, residual_sq = totals[2 * k], totals[2 * k + 1]
            for t in range(SPAN // 128):
                lanes = slice(128 * t, 128 * (t + 1))
                vector_sq = vector_sq + value[:, lanes] * value[:, lanes]
                residual_sq = residual_sq + residual[:, lanes] * residual[:, lanes]
            done += [vector_sq, residual_sq]
        return tuple(done)

    totals = lax.fori_loop(0, planes * spans, step, tuple(ref[...] for ref in sums))
    for ref, total in zip(sums, totals):
        ref[...] = total


def column_of(row):
    n = row.shape[1]
    same = lax.broadcasted_iota(jnp.int32, (n, n), 0) == lax.broadcasted_iota(jnp.int32, (n, n), 1)
    return jnp.sum(jnp.where(same, row, 0.0), axis=1, keepdims=True)


def spread_coefficients(coefficients, coefs):
    out = lax.broadcasted_iota(jnp.int32, (40, 40), 0)
    vec = lax.broadcasted_iota(jnp.int32, (40, 40), 1)
    rest = out - 32
    wanted = jnp.where(out < 32, 10 * (out >> 3) + (out & 7), 10 * (rest >> 1) + 8 + (rest & 1))
    rows = jnp.where(vec == wanted, 1.0, 0.0).astype(jnp.bfloat16)
    ordered = jnp.dot(rows, coefficients[...], preferred_element_type=jnp.float32).astype(jnp.bfloat16)
    rank = lax.broadcasted_iota(jnp.int32, (100, 128), 0)
    at = lax.broadcasted_iota(jnp.int32, (100, 128), 1)
    odd = at - 96
    for h in range(2):
        main = 25 * ((at >> 3) & 3) + 8 * (at >> 5) + (at & 7)
        other = jnp.where((odd < 8) & ((odd & 1) == h), 25 * (odd >> 1) + 24, -1)
        pick = jnp.where(rank == jnp.where(at < 96, main, other), 1.0, 0.0).astype(jnp.bfloat16)
        coefs[h] = jnp.dot(ordered, pick, preferred_element_type=jnp.float32).astype(jnp.bfloat16)


MESH = pl.DeviceIdType.MESH
PIECE = 2048
CHUNK = 4 * PIECE
HALF = PIECE // 2
ORDER = (0, 7, 1, 2, 3, 4, 5, 6)
AHEAD = 3
LIMIT = 50_331_648


def whole_kernel(
    count, basis, coefficients_in, lower_in, upper_in, mass_in, damping_in, stiffness_in, eigen_in,
    eig_ref, res_ref, norm_ref, coefficients, lower, upper, mass, damping, stiffness, eigen_row, lists,
    odd_rows, extra, coefs, ea, eb, above_a, above_b, below_a, below_b, down_lists, ra, rb, sa, sb,
    first_a, first_b, last_a, last_b, square_a, residual_a, square_b, residual_b, squares,
    input_sem, own_sem, odd_sem, sent_sem, chunk_sem, plane_sem, square_recv_sem,
):
    me, sub = lax.axis_index("vecs"), lax.axis_index("rows")
    subs = lax.axis_size("rows")
    following, previous = lax.rem(sub + 1, subs), lax.rem(sub + subs - 1, subs)
    ahead = [lax.rem(me + d, 4) for d in (1, 2, 3)]
    behind = [lax.rem(me + 4 - d, 4) for d in (1, 2, 3)]
    order = (0, 2, 1)

    basis_sem, extra_sem, vec_a_sem, vec_b_sem = ((sent_sem.at[k], chunk_sem.at[k]) for k in range(4))
    square_sem = (sent_sem.at[4], square_recv_sem)

    barrier = pltpu.get_barrier_semaphore()
    for peer in ahead:
        pl.semaphore_signal(barrier, inc=1, device_id={"vecs": peer}, device_id_type=MESH)

    @pl.loop(1, subs)
    def _(d):
        pl.semaphore_signal(barrier, inc=1, device_id={"rows": lax.rem(sub + d, subs)}, device_id_type=MESH)

    def remote(source, target, sems, at, peer):
        return pltpu.make_async_remote_copy(
            src_ref=source, dst_ref=target, send_sem=sems[0], recv_sem=sems[1].at[at],
            device_id=peer, device_id_type=MESH,
        )

    def all_of(block, sems, at=0):
        return remote(block, block, sems, at, {"vecs": ahead[0]})

    def columns(c, q):
        return pl.ds(pl.multiple_of(c * CHUNK + q * PIECE, PIECE), PIECE)

    def send_basis(c):
        for d in order:
            peer = ahead[d]
            for g in range(3):
                remote(
                    basis.at[pl.ds(8 * g, 8), columns(c, peer)], ra.at[c, g, me], basis_sem, c, {"vecs": peer}
                ).start()

    def send_extra(c):
        for d in order:
            peer = ahead[d]
            remote(extra.at[c, peer], rb.at[c, me], extra_sem, c, {"vecs": peer}).start()

    def own_copies(c):
        for g in range(3):
            yield pltpu.make_async_copy(
                basis.at[pl.ds(8 * g, 8), columns(c, me)], ra.at[c, g, me], own_sem.at[c]
            )

    def basis_arrived(c):
        pltpu.make_async_copy(ra.at[c, :, me], ra.at[c, :, me], own_sem.at[c]).wait()
        all_of(ra.at[c, :, pl.ds(0, 3)], basis_sem, c).wait_recv()
        all_of(rb.at[c, pl.ds(0, 3)], extra_sem, c).wait_recv()

    def send_vecs(c):
        for d in order:
            peer = ahead[d]
            remote(sa.at[c, peer], ea.at[:, columns(c, me)], vec_a_sem, c, {"vecs": peer}).start()
            remote(sb.at[c, peer], eb.at[:, columns(c, me)], vec_b_sem, c, {"vecs": peer}).start()

    def vecs_arrived(c):
        all_of(sa.at[c, pl.ds(0, 3)], vec_a_sem, c).wait_recv()
        all_of(sb.at[c, pl.ds(0, 3)], vec_b_sem, c).wait_recv()

    rows_local = basis.shape[1]
    plane_copies = {
        ORDER[0]: (
            remote(ea.at[:, pl.ds(0, PLANE)], above_a, (plane_sem.at[0, 0], plane_sem.at[1]), 0, {"rows": previous}),
            remote(eb.at[:, pl.ds(0, PLANE)], above_b, (plane_sem.at[0, 1], plane_sem.at[1]), 1, {"rows": previous}),
        ),
        ORDER[1]: (
            remote(ea.at[:, pl.ds(rows_local - PLANE, PLANE)], below_a, (plane_sem.at[0, 2], plane_sem.at[1]), 2, {"rows": following}),
            remote(eb.at[:, pl.ds(rows_local - PLANE, PLANE)], below_b, (plane_sem.at[0, 3], plane_sem.at[1]), 3, {"rows": following}),
        ),
    }
    list_copy = remote(lists, down_lists, (plane_sem.at[0, 4], plane_sem.at[1]), 4, {"rows": following})

    inputs = [
        pltpu.make_async_copy(source, target, input_sem.at[i])
        for i, (source, target) in enumerate((
            (coefficients_in, coefficients), (lower_in, lower), (upper_in, upper), (eigen_in, eigen_row),
            (mass_in, mass), (damping_in, damping), (stiffness_in, stiffness),
        ))
    ]
    inputs[0].start()
    odd_copy = pltpu.make_async_copy(basis.at[pl.ds(24, 1), :], odd_rows, odd_sem)
    odd_copy.start()
    for c in ORDER:
        for copy in own_copies(c):
            copy.start()
    for copy in inputs[1:]:
        copy.start()
    for copy in inputs[:4]:
        copy.wait()
    spread_coefficients(coefficients, coefs)
    used = lax.broadcasted_iota(jnp.int32, (1, PLANE), 1) < count[0]
    lists[0:1, :] = jnp.where(used, lower[...], -1)
    lists[1:2, :] = jnp.where(used, upper[...], -1)
    pl.semaphore_wait(barrier, subs + 2)
    for c in ORDER[:AHEAD]:
        send_basis(c)
    odd_copy.wait()
    for c in ORDER:
        for q in range(4):
            at = c * CHUNK + q * PIECE
            pair = [odd_rows[0:1, at + h * HALF : at + (h + 1) * HALF].astype(jnp.float32) for h in range(2)]
            extra[c, q] = jnp.concatenate(pair, axis=0).astype(jnp.bfloat16)
    for c in ORDER:
        rb[c, me] = extra[c, me]
    for c in ORDER[:AHEAD]:
        send_extra(c)
    list_copy.start()
    sums = (square_a, residual_a, square_b, residual_b)
    for ref in sums:
        ref[...] = jnp.zeros_like(ref)
    eigen = column_of(eigen_row[...])
    diag_refs = (mass, damping, stiffness)
    for copy in inputs[4:]:
        copy.wait()

    def planes_done(first, planes, links=None):
        residual_spans((ea, eb), (eig_ref, res_ref), diag_refs, eigen, first, planes, links, sums)

    def product(c):
        for h in range(2):
            at = pl.ds(h * HALF, HALF)
            parts = [ra[c, g, :, :, at].reshape(32, HALF) for g in range(3)]
            odd = jnp.concatenate(
                [rb[c, q].astype(jnp.float32) for q in range(4)] + [jnp.zeros((24, HALF), jnp.float32)], axis=0
            )
            whole = jnp.concatenate([*parts, odd.astype(jnp.bfloat16)], axis=0)
            out = jnp.dot(coefs[h], whole, preferred_element_type=jnp.float32)
            for p in range(4):
                sa[c, p, :, at] = out[8 * p : 8 * p + 8].astype(jnp.bfloat16)
                sb[c, p, :, at] = out[32 + 2 * p : 34 + 2 * p].astype(jnp.bfloat16)
        ea[:, columns(c, me)] = sa[c, me]
        eb[:, columns(c, me)] = sb[c, me]

    def arrived(c):
        vecs_arrived(c)
        for copy in plane_copies.get(c, ()):
            copy.start()

    def first_links():
        for copy in plane_copies[ORDER[1]]:
            copy.wait_recv()
        list_copy.wait_recv()
        link_plane(below_a, below_b, down_lists, 0, 1, first_a, first_b)

    def last_links():
        for copy in plane_copies[ORDER[0]]:
            copy.wait_recv()
        link_plane(above_a, above_b, lists, 1, 0, last_a, last_b)

    def outer_planes():
        planes_done(0, 1, (first_a, first_b))
        planes_done(rows_local // PLANE - 1, 1, (last_a, last_b))

    later = {5: first_links, 6: last_links, 7: outer_planes}
    for i, c in enumerate(ORDER):
        basis_arrived(c)
        product(c)
        send_vecs(c)
        if i + AHEAD < len(ORDER):
            send_basis(ORDER[i + AHEAD])
            send_extra(ORDER[i + AHEAD])
        if i >= 2:
            arrived(ORDER[i - 2])
            if i >= 4:
                planes_done(2 * ORDER[i - 2] - 1, 2)
        if i in later:
            later[i]()
    arrived(ORDER[-2])
    planes_done(2 * ORDER[-2] - 1, 2)
    arrived(ORDER[-1])
    planes_done(2 * ORDER[-1] - 1, 4)

    lane = lax.broadcasted_iota(jnp.int32, (1, 128), 1)
    message = jnp.zeros((1, 128), jnp.float32)
    for ref, start in ((square_a, 0), (square_b, 8), (residual_a, 16), (residual_b, 24)):
        column = jnp.sum(ref[...], axis=1, keepdims=True)
        row = lax.broadcasted_iota(jnp.int32, (ref.shape[0], 128), 0) + start
        message = message + jnp.sum(jnp.where(row == lane, column, 0.0), axis=0, keepdims=True)
    squares[sub] = message

    @pl.loop(1, subs)
    def _(d):
        remote(squares.at[sub], squares.at[sub], square_sem, 0, {"rows": lax.rem(sub + d, subs)}).start()

    for copies in plane_copies.values():
        for copy in copies:
            copy.wait_send()
    list_copy.wait_send()
    all_of(ra.at[:, :, pl.ds(0, 3)], basis_sem).wait_send()
    all_of(rb.at[:, pl.ds(0, 3)], extra_sem).wait_send()
    all_of(sa.at[:, pl.ds(0, 3)], vec_a_sem).wait_send()
    all_of(sb.at[:, pl.ds(0, 3)], vec_b_sem).wait_send()

    every = squares.at[pl.ds(0, subs - 1)]
    all_of(every, square_sem).wait_recv()
    all_of(every, square_sem).wait_send()
    total = jnp.sum(squares[...], axis=0)
    norms = jnp.sqrt(pltpu.roll(total, 112, 1)) / jnp.sqrt(total + 1.0)
    norm_ref[...] = norms[:, :10]


def whole(count, *arrays):
    basis = arrays[0]
    rows = basis.shape[1]
    chunks = rows // CHUNK
    subs = lax.axis_size("rows")
    vmem = pl.BlockSpec(memory_space=pltpu.VMEM)
    f32 = lambda *shape: pltpu.VMEM(shape, jnp.float32)
    bf16 = lambda *shape: pltpu.VMEM(shape, jnp.bfloat16)
    dma = pltpu.SemaphoreType.DMA
    return pl.pallas_call(
        whole_kernel,
        out_shape=(
            jax.ShapeDtypeStruct((10, rows), jnp.bfloat16),
            jax.ShapeDtypeStruct((10, rows), jnp.bfloat16),
            jax.ShapeDtypeStruct((1, 10), jnp.float32),
        ),
        in_specs=[pl.BlockSpec(memory_space=pltpu.SMEM)] + [pl.BlockSpec(memory_space=pltpu.HBM)] * 8,
        out_specs=(vmem,) * 3,
        scratch_shapes=[
            *[pltpu.VMEM(a.shape, a.dtype) for a in arrays[1:]], pltpu.VMEM((2, PLANE), jnp.int32),
            bf16(1, rows), bf16(chunks, 4, 2, HALF), bf16(2, 40, 128), bf16(8, rows), bf16(2, rows),
            bf16(8, PLANE), bf16(2, PLANE), bf16(8, PLANE), bf16(2, PLANE), pltpu.VMEM((2, PLANE), jnp.int32),
            bf16(chunks, 3, 4, 8, PIECE), bf16(chunks, 4, 2, HALF), bf16(chunks, 4, 8, PIECE), bf16(chunks, 4, 2, PIECE),
            f32(8, PLANE), f32(2, PLANE), f32(8, PLANE), f32(2, PLANE),
            f32(8, 128), f32(8, 128), f32(2, 128), f32(2, 128), f32(subs, 1, 128),
            dma((7,)), dma((chunks,)), dma(()), dma((5,)), dma((4, chunks)), dma((2, 5)), dma((1,)),
        ],
        compiler_params=pltpu.CompilerParams(
            collective_id=0, has_side_effects=True, vmem_limit_bytes=LIMIT
        ),
        name="whole",
    )(count, *[pltpu.with_memory_space_constraint(a, pltpu.HBM) for a in arrays])


def on_device(basis, coefficients, eigen_values, stiffness, damping, mass, link_count, lower_cells, upper_cells):
    rows_local = basis.shape[1]
    wide = lambda a: a.reshape(1, rows_local)
    eig, res, norms = whole(
        link_count, basis, coefficients.T, lower_cells, upper_cells, wide(mass), wide(damping), wide(stiffness), eigen_values[None, :]
    )
    return eig, res, norms.reshape(10)


def solution(mesh):
    placed = (
        P("vecs", "rows"), P(), P("vecs"), P("rows"), P("rows"), P("rows"), P("rows"), P("rows", None), P("rows", None),
    )
    return jax.shard_map(
        on_device,
        mesh=mesh,
        in_specs=placed,
        out_specs=(P("vecs", "rows"), P("vecs", "rows"), P("vecs")),
        check_vma=False,
    )
```

```python
import functools

import jax
import jax.numpy as jnp
from jax import lax
from jax.experimental import pallas as pl
from jax.experimental.pallas import tpu as pltpu
from jax.sharding import PartitionSpec as P

WID = 64
PLANE = WID * WID
SPAN = 1024
SLOTS = 512
LOW = 256


def link_plane(part_a, part_b, lists, gather, scatter, link_a, link_b):
    high = PLANE // LOW
    whole = jnp.concatenate(
        [part_a[...].astype(jnp.float32), part_b[...].astype(jnp.float32), jnp.zeros((6, PLANE), jnp.float32)], axis=0
    ).astype(jnp.bfloat16)
    table = jnp.concatenate([whole[:, LOW * h : LOW * (h + 1)] for h in range(high)], axis=0)
    cell = lax.broadcasted_iota(jnp.int32, (LOW, SLOTS), 0)

    def step(t, total):
        at = pl.multiple_of(t * SLOTS, SLOTS)
        source = lists[gather : gather + 1, pl.ds(at, SLOTS)]
        target = lists[scatter : scatter + 1, pl.ds(at, SLOTS)]
        pick = jnp.where(cell == (source & (LOW - 1)), 1.0, 0.0).astype(jnp.bfloat16)
        rows = jnp.dot(table, pick, preferred_element_type=jnp.float32)
        source_high = source >> 8
        value = jnp.zeros((16, SLOTS), jnp.float32)
        for h in range(high):
            value = value + jnp.where(source_high == h, rows[16 * h : 16 * h + 16], 0.0)
        target_high = target >> 8
        spread = jnp.concatenate(
            [jnp.where(target_high == h, value, 0.0).astype(jnp.bfloat16) for h in range(high)], axis=0
        )
        place = jnp.where(cell == (target & (LOW - 1)), 1.0, 0.0).astype(jnp.bfloat16)
        return total + lax.dot_general(
            spread, place, (((1,), (1,)), ((), ())), preferred_element_type=jnp.float32
        )

    total = lax.fori_loop(0, PLANE // SLOTS, step, jnp.zeros((16 * high, LOW), jnp.float32))
    for h in range(high):
        link_a[:, LOW * h : LOW * (h + 1)] = total[16 * h : 16 * h + 8]
        link_b[:, LOW * h : LOW * (h + 1)] = total[16 * h + 8 : 16 * h + 10]


def residual_spans(vecs, outs, diag_refs, eigen, first, planes, links, sums):
    eig_ref, res_ref = outs
    depth = eig_ref.shape[1] // PLANE
    spans = PLANE // SPAN
    column = lax.broadcasted_iota(jnp.int32, (1, SPAN), 1) & (WID - 1)
    groups = ((vecs[0], slice(0, 8)), (vecs[1], slice(8, 10)))
    factors = []
    for _, part in groups:
        lam = eigen[part]
        factors.append((lam, lam * lam, lam * lam * 0.1 + lam * 0.3 + 1.0))

    def step(i, totals):
        c = i % spans
        base = pl.multiple_of(first * PLANE + i * SPAN, SPAN)
        here = pl.ds(base, SPAN)
        before = pl.ds(pl.multiple_of(jnp.where(c > 0, base - 128, base), 128), 128)
        after = pl.ds(pl.multiple_of(jnp.where(c < spans - 1, base + SPAN, base), 128), 128)
        mass, damping, stiffness = (r[:, here] for r in diag_refs)
        done = []
        for k, (ref, part) in enumerate(groups):
            lam, square, coupling = factors[k]
            raw = ref[:, here]
            value = raw.astype(jnp.float32)
            left = jnp.where(c > 0, ref[:, before].astype(jnp.float32), 0.0)
            right = jnp.where(c < spans - 1, ref[:, after].astype(jnp.float32), 0.0)
            wide = jnp.concatenate([left, value, right], axis=1)
            span = SPAN + 256
            total = pltpu.roll(wide, WID, 1)[:, 128 : 128 + SPAN] + pltpu.roll(wide, span - WID, 1)[:, 128 : 128 + SPAN]
            total = total + jnp.where(column > 0, pltpu.roll(value, 1, 1), 0.0)
            total = total + jnp.where(column < WID - 1, pltpu.roll(value, SPAN - 1, 1), 0.0)
            if not (links is not None and first == 0):
                total = total + ref[:, pl.ds(pl.multiple_of(base - PLANE, SPAN), SPAN)].astype(jnp.float32)
            if not (links is not None and first == depth - 1):
                total = total + ref[:, pl.ds(pl.multiple_of(base + PLANE, SPAN), SPAN)].astype(jnp.float32)
            if links is not None:
                total = total + links[k][:, pl.ds(pl.multiple_of(i * SPAN, SPAN), SPAN)]
            residual = (square * mass + lam * damping + stiffness) * value - coupling * total
            eig_ref[part, here] = raw
            res_ref[part, here] = residual.astype(jnp.bfloat16)
            vector_sq, residual_sq = totals[2 * k], totals[2 * k + 1]
            for t in range(SPAN // 128):
                lanes = slice(128 * t, 128 * (t + 1))
                vector_sq = vector_sq + value[:, lanes] * value[:, lanes]
                residual_sq = residual_sq + residual[:, lanes] * residual[:, lanes]
            done += [vector_sq, residual_sq]
        return tuple(done)

    totals = lax.fori_loop(0, planes * spans, step, tuple(ref[...] for ref in sums))
    for ref, total in zip(sums, totals):
        ref[...] = total


def column_of(row):
    n = row.shape[1]
    same = lax.broadcasted_iota(jnp.int32, (n, n), 0) == lax.broadcasted_iota(jnp.int32, (n, n), 1)
    return jnp.sum(jnp.where(same, row, 0.0), axis=1, keepdims=True)


def spread_coefficients(coefficients, coefs, devices, which):
    out = lax.broadcasted_iota(jnp.int32, (40, 40), 0)
    vec = lax.broadcasted_iota(jnp.int32, (40, 40), 1)
    rest = out - 32
    group = jnp.where(out < 32, out >> 3, rest >> 1)
    place = jnp.where(out < 32, out & 7, 8 + (rest & 1))
    owner = devices[3]
    for k in range(3):
        owner = jnp.where(group == k, devices[k], owner)
    rows = jnp.where(vec == 10 * owner + place, 1.0, 0.0).astype(jnp.bfloat16)
    ordered = jnp.dot(rows, coefficients[...], preferred_element_type=jnp.float32).astype(jnp.bfloat16)
    rank = lax.broadcasted_iota(jnp.int32, (100, 64), 0)
    at = lax.broadcasted_iota(jnp.int32, (100, 64), 1)
    odd = at - 48
    for h in range(2):
        main = 25 * jnp.where(((at >> 3) & 1) == 0, devices[0], devices[1]) + 8 * (at >> 4) + (at & 7)
        other = 25 * jnp.where((odd >> 1) == 0, devices[0], devices[1]) + 24
        other = jnp.where((odd < 4) & ((odd & 1) == h), other, -1)
        pick = jnp.where(rank == jnp.where(at < 48, main, other), 1.0, 0.0).astype(jnp.bfloat16)
        coefs[which, h] = jnp.dot(ordered, pick, preferred_element_type=jnp.float32).astype(jnp.bfloat16)


STEPS = 32760.0


def send_scaled(parts, target):
    top = jnp.max(jnp.concatenate([jnp.abs(part) for part in parts], axis=1), axis=1, keepdims=True)
    power = jnp.ceil(jnp.log2(jnp.maximum(top, 1e-30)))
    factor = jnp.exp2(-power) * STEPS
    for h, part in enumerate(parts):
        target[:, h * HALF : (h + 1) * HALF] = jnp.round(part * factor).astype(jnp.int32).astype(jnp.int16)
    wide = jnp.broadcast_to(power, (power.shape[0], 128))
    target[:, PIECE : PIECE + 128] = wide.astype(jnp.int32).astype(jnp.int16)


def scaled_back(source, h):
    power = source[:, PIECE : PIECE + 128].astype(jnp.int32).astype(jnp.float32)[:, :1]
    return source[:, h * HALF : (h + 1) * HALF].astype(jnp.int32).astype(jnp.float32) * (jnp.exp2(power) * (1.0 / STEPS))


MESH = pl.DeviceIdType.MESH
PIECE = 2048
CHUNK = 4 * PIECE
HALF = PIECE // 2
ORDER = (0, 7, 1, 2, 3, 4, 5, 6)
AHEAD = 2
LIMIT = 50_331_648


def whole_kernel(
    count, basis, coefficients_in, lower_in, upper_in, mass_in, damping_in, stiffness_in, eigen_in,
    eig_ref, res_ref, norm_ref, coefficients, lower, upper, mass, damping, stiffness, eigen_row, lists,
    odd_rows, extra, coefs, ea, eb, above_a, above_b, below_a, below_b, down_lists, ra, rb,
    part_a, part_b, to_a, to_b, from_a, from_b, mate_a, mate_b,
    first_a, first_b, last_a, last_b, square_a, residual_a, square_b, residual_b, squares,
    input_sem, own_sem, odd_sem, sent_sem, chunk_sem, plane_sem, square_recv_sem,
):
    me, sub = lax.axis_index("vecs"), lax.axis_index("rows")
    subs = lax.axis_size("rows")
    following, previous = lax.rem(sub + 1, subs), lax.rem(sub + subs - 1, subs)
    one, two = me + 1 - 2 * lax.rem(me, 2), 3 - me
    mates, crosses = (one, two), (two, one)
    halves = (lax.rem(lax.div(me + 1, 2), 2), lax.div(me, 2))
    basis_sem, extra_sem, sum_a_sem, sum_b_sem, vec_a_sem, vec_b_sem = (
        (sent_sem.at[k], chunk_sem.at[k]) for k in range(6)
    )
    square_sem = (sent_sem.at[6], square_recv_sem)

    barrier = pltpu.get_barrier_semaphore()
    for peer in mates:
        pl.semaphore_signal(barrier, inc=1, device_id={"vecs": peer}, device_id_type=MESH)

    @pl.loop(1, subs)
    def _(d):
        pl.semaphore_signal(barrier, inc=1, device_id={"rows": lax.rem(sub + d, subs)}, device_id_type=MESH)

    def remote(source, target, sems, at, peer):
        return pltpu.make_async_remote_copy(
            src_ref=source, dst_ref=target, send_sem=sems[0], recv_sem=sems[1].at[at],
            device_id=peer, device_id_type=MESH,
        )

    def all_of(block, sems, at=0):
        return remote(block, block, sems, at, {"vecs": one})

    def columns(c, x, half):
        return pl.ds(pl.multiple_of(c * CHUNK + x * PLANE + half * PIECE, PIECE), PIECE)

    def send_basis(c):
        for x, (mate, half) in enumerate(zip(mates, halves)):
            for g in range(3):
                remote(
                    basis.at[pl.ds(8 * g, 8), columns(c, x, 1 - half)], ra.at[c, x, g, 1], basis_sem, c, {"vecs": mate}
                ).start()

    def send_extra(c):
        for x, (mate, half) in enumerate(zip(mates, halves)):
            remote(extra.at[c, 2 * x + 1 - half], rb.at[c, x, 1], extra_sem, c, {"vecs": mate}).start()

    def own_copies(c):
        for x, half in enumerate(halves):
            for g in range(3):
                yield pltpu.make_async_copy(
                    basis.at[pl.ds(8 * g, 8), columns(c, x, half)], ra.at[c, x, g, 0], own_sem.at[c]
                )

    def basis_arrived(c):
        pltpu.make_async_copy(ra.at[c, :, :, 0], ra.at[c, :, :, 0], own_sem.at[c]).wait()
        all_of(ra.at[c, :, :, 1], basis_sem, c).wait_recv()
        all_of(rb.at[c, :, 1], extra_sem, c).wait_recv()

    def send_sums(c):
        for x, cross in enumerate(crosses):
            remote(to_a.at[c, x], from_a.at[c, x], sum_a_sem, c, {"vecs": cross}).start()
            remote(to_b.at[c, x], from_b.at[c, x], sum_b_sem, c, {"vecs": cross}).start()

    def send_vecs(c):
        for x, (mate, half) in enumerate(zip(mates, halves)):
            remote(mate_a.at[c, x], ea.at[:, columns(c, x, half)], vec_a_sem, c, {"vecs": mate}).start()
            remote(mate_b.at[c, x], eb.at[:, columns(c, x, half)], vec_b_sem, c, {"vecs": mate}).start()

    def vecs_arrived(c):
        all_of(mate_a.at[c], vec_a_sem, c).wait_recv()
        all_of(mate_b.at[c], vec_b_sem, c).wait_recv()

    rows_local = basis.shape[1]
    plane_copies = {
        ORDER[0]: (
            remote(ea.at[:, pl.ds(0, PLANE)], above_a, (plane_sem.at[0, 0], plane_sem.at[1]), 0, {"rows": previous}),
            remote(eb.at[:, pl.ds(0, PLANE)], above_b, (plane_sem.at[0, 1], plane_sem.at[1]), 1, {"rows": previous}),
        ),
        ORDER[1]: (
            remote(ea.at[:, pl.ds(rows_local - PLANE, PLANE)], below_a, (plane_sem.at[0, 2], plane_sem.at[1]), 2, {"rows": following}),
            remote(eb.at[:, pl.ds(rows_local - PLANE, PLANE)], below_b, (plane_sem.at[0, 3], plane_sem.at[1]), 3, {"rows": following}),
        ),
    }
    list_copy = remote(lists, down_lists, (plane_sem.at[0, 4], plane_sem.at[1]), 4, {"rows": following})

    inputs = [
        pltpu.make_async_copy(source, target, input_sem.at[i])
        for i, (source, target) in enumerate((
            (coefficients_in, coefficients), (lower_in, lower), (upper_in, upper), (eigen_in, eigen_row),
            (mass_in, mass), (damping_in, damping), (stiffness_in, stiffness),
        ))
    ]
    inputs[0].start()
    odd_copy = pltpu.make_async_copy(basis.at[pl.ds(24, 1), :], odd_rows, odd_sem)
    odd_copy.start()
    for c in ORDER:
        for copy in own_copies(c):
            copy.start()
    for copy in inputs[1:]:
        copy.start()
    for copy in inputs[:4]:
        copy.wait()
    for x in range(2):
        devices = (me, mates[x], crosses[x], 6 - me - one - two)
        spread_coefficients(coefficients, coefs, devices, x)
    used = lax.broadcasted_iota(jnp.int32, (1, PLANE), 1) < count[0]
    lists[0:1, :] = jnp.where(used, lower[...], -1)
    lists[1:2, :] = jnp.where(used, upper[...], -1)
    pl.semaphore_wait(barrier, subs + 1)
    for c in ORDER[:AHEAD]:
        send_basis(c)
    odd_copy.wait()
    for c in ORDER:
        for q in range(4):
            at = c * CHUNK + q * PIECE
            pair = [odd_rows[0:1, at + h * HALF : at + (h + 1) * HALF].astype(jnp.float32) for h in range(2)]
            extra[c, q] = jnp.concatenate(pair, axis=0).astype(jnp.bfloat16)
    for c in ORDER:
        for x, half in enumerate(halves):
            rb[c, x, 0] = extra[c, 2 * x + half]
    for c in ORDER[:AHEAD]:
        send_extra(c)
    list_copy.start()
    sums = (square_a, residual_a, square_b, residual_b)
    for ref in sums:
        ref[...] = jnp.zeros_like(ref)
    eigen = column_of(eigen_row[...])
    diag_refs = (mass, damping, stiffness)
    for copy in inputs[4:]:
        copy.wait()

    def planes_done(first, planes, links=None):
        residual_spans((ea, eb), (eig_ref, res_ref), diag_refs, eigen, first, planes, links, sums)

    def product(c):
        for x in range(2):
            outs = []
            for h in range(2):
                at = pl.ds(h * HALF, HALF)
                parts = [ra[c, x, g, :, :, at].reshape(16, HALF) for g in range(3)]
                odd = jnp.concatenate(
                    [rb[c, x, q].astype(jnp.float32) for q in range(2)] + [jnp.zeros((12, HALF), jnp.float32)], axis=0
                )
                stack = jnp.concatenate([*parts, odd.astype(jnp.bfloat16)], axis=0)
                out = jnp.dot(coefs[x, h], stack, preferred_element_type=jnp.float32)
                part_a[c, x, :, at] = out[0:16]
                part_b[c, x, :, at] = out[32:36]
                outs.append(out)
            send_scaled([out[16:32] for out in outs], to_a.at[c, x])
            send_scaled([out[36:40] for out in outs], to_b.at[c, x])

    def combine(c):
        all_of(from_a.at[c], sum_a_sem, c).wait_recv()
        all_of(from_b.at[c], sum_b_sem, c).wait_recv()
        for x, half in enumerate(halves):
            for h in range(2):
                at = pl.ds(h * HALF, HALF)
                here = pl.ds(pl.multiple_of(c * CHUNK + x * PLANE + half * PIECE + h * HALF, HALF), HALF)
                vecs = (part_a[c, x, :, at] + scaled_back(from_a.at[c, x], h)).astype(jnp.bfloat16)
                ea[:, here] = vecs[:8]
                mate_a[c, x, :, at] = vecs[8:]
                vecs = (part_b[c, x, :, at] + scaled_back(from_b.at[c, x], h)).astype(jnp.bfloat16)
                eb[:, here] = vecs[:2]
                mate_b[c, x, :, at] = vecs[2:]
        send_vecs(c)

    def arrived(c):
        vecs_arrived(c)
        for copy in plane_copies.get(c, ()):
            copy.start()

    def first_links():
        for copy in plane_copies[ORDER[1]]:
            copy.wait_recv()
        list_copy.wait_recv()
        link_plane(below_a, below_b, down_lists, 0, 1, first_a, first_b)

    def last_links():
        for copy in plane_copies[ORDER[0]]:
            copy.wait_recv()
        link_plane(above_a, above_b, lists, 1, 0, last_a, last_b)

    def outer_planes():
        planes_done(0, 1, (first_a, first_b))
        planes_done(rows_local // PLANE - 1, 1, (last_a, last_b))

    later = {6: first_links, 7: last_links}
    for i, c in enumerate(ORDER):
        basis_arrived(c)
        product(c)
        send_sums(c)
        if i + AHEAD < len(ORDER):
            send_basis(ORDER[i + AHEAD])
            send_extra(ORDER[i + AHEAD])
        if i >= 1:
            combine(ORDER[i - 1])
        if i >= 3:
            arrived(ORDER[i - 3])
            if i >= 5:
                planes_done(2 * ORDER[i - 3] - 1, 2)
        if i in later:
            later[i]()
    combine(ORDER[-1])
    outer_planes()
    arrived(ORDER[-3])
    planes_done(2 * ORDER[-3] - 1, 2)
    arrived(ORDER[-2])
    planes_done(2 * ORDER[-2] - 1, 2)
    arrived(ORDER[-1])
    planes_done(2 * ORDER[-1] - 1, 4)

    lane = lax.broadcasted_iota(jnp.int32, (1, 128), 1)
    message = jnp.zeros((1, 128), jnp.float32)
    for ref, start in ((square_a, 0), (square_b, 8), (residual_a, 16), (residual_b, 24)):
        column = jnp.sum(ref[...], axis=1, keepdims=True)
        row = lax.broadcasted_iota(jnp.int32, (ref.shape[0], 128), 0) + start
        message = message + jnp.sum(jnp.where(row == lane, column, 0.0), axis=0, keepdims=True)
    squares[sub] = message

    @pl.loop(1, subs)
    def _(d):
        remote(squares.at[sub], squares.at[sub], square_sem, 0, {"rows": lax.rem(sub + d, subs)}).start()

    for copies in plane_copies.values():
        for copy in copies:
            copy.wait_send()
    list_copy.wait_send()
    all_of(ra.at[:, :, :, 1], basis_sem).wait_send()
    all_of(rb.at[:, :, 1], extra_sem).wait_send()
    all_of(from_a, sum_a_sem).wait_send()
    all_of(from_b, sum_b_sem).wait_send()
    all_of(mate_a, vec_a_sem).wait_send()
    all_of(mate_b, vec_b_sem).wait_send()
    every = squares.at[pl.ds(0, subs - 1)]
    all_of(every, square_sem).wait_recv()
    all_of(every, square_sem).wait_send()
    total = jnp.sum(squares[...], axis=0)
    norms = jnp.sqrt(pltpu.roll(total, 112, 1)) / jnp.sqrt(total + 1.0)
    norm_ref[...] = norms[:, :10]


def whole(count, *arrays):
    basis = arrays[0]
    rows = basis.shape[1]
    chunks = rows // CHUNK
    subs = lax.axis_size("rows")
    vmem = pl.BlockSpec(memory_space=pltpu.VMEM)
    f32 = lambda *shape: pltpu.VMEM(shape, jnp.float32)
    bf16 = lambda *shape: pltpu.VMEM(shape, jnp.bfloat16)
    dma = pltpu.SemaphoreType.DMA
    return pl.pallas_call(
        whole_kernel,
        out_shape=(
            jax.ShapeDtypeStruct((10, rows), jnp.bfloat16),
            jax.ShapeDtypeStruct((10, rows), jnp.bfloat16),
            jax.ShapeDtypeStruct((1, 10), jnp.float32),
        ),
        in_specs=[pl.BlockSpec(memory_space=pltpu.SMEM)] + [pl.BlockSpec(memory_space=pltpu.HBM)] * 8,
        out_specs=(vmem,) * 3,
        scratch_shapes=[
            *[pltpu.VMEM(a.shape, a.dtype) for a in arrays[1:]], pltpu.VMEM((2, PLANE), jnp.int32),
            bf16(1, rows), bf16(chunks, 4, 2, HALF), bf16(2, 2, 40, 64), bf16(8, rows), bf16(2, rows),
            bf16(8, PLANE), bf16(2, PLANE), bf16(8, PLANE), bf16(2, PLANE), pltpu.VMEM((2, PLANE), jnp.int32),
            bf16(chunks, 2, 3, 2, 8, PIECE), bf16(chunks, 2, 2, 2, HALF),
            f32(chunks, 2, 16, PIECE), f32(chunks, 2, 4, PIECE),
            *[pltpu.VMEM((chunks, 2, r, PIECE + 128), jnp.int16) for r in (16, 4, 16, 4)],
            bf16(chunks, 2, 8, PIECE), bf16(chunks, 2, 2, PIECE),
            f32(8, PLANE), f32(2, PLANE), f32(8, PLANE), f32(2, PLANE),
            f32(8, 128), f32(8, 128), f32(2, 128), f32(2, 128), f32(subs, 1, 128),
            dma((7,)), dma((chunks,)), dma(()), dma((7,)), dma((6, chunks)), dma((2, 5)), dma((1,)),
        ],
        compiler_params=pltpu.CompilerParams(
            collective_id=0, has_side_effects=True, vmem_limit_bytes=LIMIT
        ),
        name="whole",
    )(count, *[pltpu.with_memory_space_constraint(a, pltpu.HBM) for a in arrays])


def on_device(basis, coefficients, eigen_values, stiffness, damping, mass, link_count, lower_cells, upper_cells):
    rows_local = basis.shape[1]
    wide = lambda a: a.reshape(1, rows_local)
    eig, res, norms = whole(
        link_count, basis, coefficients.T, lower_cells, upper_cells, wide(mass), wide(damping), wide(stiffness), eigen_values[None, :]
    )
    return eig, res, norms.reshape(10)


def solution(mesh):
    placed = (
        P("vecs", "rows"), P(), P("vecs"), P("rows"), P("rows"), P("rows"), P("rows"), P("rows", None), P("rows", None),
    )
    return jax.shard_map(
        on_device,
        mesh=mesh,
        in_specs=placed,
        out_specs=(P("vecs", "rows"), P("vecs", "rows"), P("vecs")),
        check_vma=False,
    )
```

```python
import functools

import jax
import jax.numpy as jnp
from jax import lax
from jax.experimental import pallas as pl
from jax.experimental.pallas import tpu as pltpu
from jax.sharding import PartitionSpec as P

WID = 64
PLANE = WID * WID
SPAN = 1024
SLOTS = 512
LOW = 256


def link_plane(part_a, part_b, lists, gather, scatter, link_a, link_b):
    high = PLANE // LOW
    whole = jnp.concatenate(
        [part_a[...].astype(jnp.float32), part_b[...].astype(jnp.float32), jnp.zeros((6, PLANE), jnp.float32)], axis=0
    ).astype(jnp.bfloat16)
    table = jnp.concatenate([whole[:, LOW * h : LOW * (h + 1)] for h in range(high)], axis=0)
    cell = lax.broadcasted_iota(jnp.int32, (LOW, SLOTS), 0)

    def step(t, total):
        at = pl.multiple_of(t * SLOTS, SLOTS)
        source = lists[gather : gather + 1, pl.ds(at, SLOTS)]
        target = lists[scatter : scatter + 1, pl.ds(at, SLOTS)]
        pick = jnp.where(cell == (source & (LOW - 1)), 1.0, 0.0).astype(jnp.bfloat16)
        rows = jnp.dot(table, pick, preferred_element_type=jnp.float32)
        source_high = source >> 8
        value = jnp.zeros((16, SLOTS), jnp.float32)
        for h in range(high):
            value = value + jnp.where(source_high == h, rows[16 * h : 16 * h + 16], 0.0)
        target_high = target >> 8
        spread = jnp.concatenate(
            [jnp.where(target_high == h, value, 0.0).astype(jnp.bfloat16) for h in range(high)], axis=0
        )
        place = jnp.where(cell == (target & (LOW - 1)), 1.0, 0.0).astype(jnp.bfloat16)
        return total + lax.dot_general(
            spread, place, (((1,), (1,)), ((), ())), preferred_element_type=jnp.float32
        )

    total = lax.fori_loop(0, PLANE // SLOTS, step, jnp.zeros((16 * high, LOW), jnp.float32))
    for h in range(high):
        link_a[:, LOW * h : LOW * (h + 1)] = total[16 * h : 16 * h + 8]
        link_b[:, LOW * h : LOW * (h + 1)] = total[16 * h + 8 : 16 * h + 10]


def residual_spans(vecs, outs, diag_refs, eigen, first, planes, links, sums):
    eig_ref, res_ref = outs
    depth = eig_ref.shape[1] // PLANE
    spans = PLANE // SPAN
    column = lax.broadcasted_iota(jnp.int32, (1, SPAN), 1) & (WID - 1)
    groups = ((vecs[0], slice(0, 8)), (vecs[1], slice(8, 10)))
    factors = []
    for _, part in groups:
        lam = eigen[part]
        factors.append((lam, lam * lam, lam * lam * 0.1 + lam * 0.3 + 1.0))

    def step(i, totals):
        c = i % spans
        base = pl.multiple_of(first * PLANE + i * SPAN, SPAN)
        here = pl.ds(base, SPAN)
        before = pl.ds(pl.multiple_of(jnp.where(c > 0, base - 128, base), 128), 128)
        after = pl.ds(pl.multiple_of(jnp.where(c < spans - 1, base + SPAN, base), 128), 128)
        mass, damping, stiffness = (r[:, here] for r in diag_refs)
        done = []
        for k, (ref, part) in enumerate(groups):
            lam, square, coupling = factors[k]
            raw = ref[:, here]
            value = raw.astype(jnp.float32)
            left = jnp.where(c > 0, ref[:, before].astype(jnp.float32), 0.0)
            right = jnp.where(c < spans - 1, ref[:, after].astype(jnp.float32), 0.0)
            wide = jnp.concatenate([left, value, right], axis=1)
            span = SPAN + 256
            total = pltpu.roll(wide, WID, 1)[:, 128 : 128 + SPAN] + pltpu.roll(wide, span - WID, 1)[:, 128 : 128 + SPAN]
            total = total + jnp.where(column > 0, pltpu.roll(value, 1, 1), 0.0)
            total = total + jnp.where(column < WID - 1, pltpu.roll(value, SPAN - 1, 1), 0.0)
            if not (links is not None and first == 0):
                total = total + ref[:, pl.ds(pl.multiple_of(base - PLANE, SPAN), SPAN)].astype(jnp.float32)
            if not (links is not None and first == depth - 1):
                total = total + ref[:, pl.ds(pl.multiple_of(base + PLANE, SPAN), SPAN)].astype(jnp.float32)
            if links is not None:
                total = total + links[k][:, pl.ds(pl.multiple_of(i * SPAN, SPAN), SPAN)]
            residual = (square * mass + lam * damping + stiffness) * value - coupling * total
            eig_ref[part, here] = raw
            res_ref[part, here] = residual.astype(jnp.bfloat16)
            vector_sq, residual_sq = totals[2 * k], totals[2 * k + 1]
            for t in range(SPAN // 128):
                lanes = slice(128 * t, 128 * (t + 1))
                vector_sq = vector_sq + value[:, lanes] * value[:, lanes]
                residual_sq = residual_sq + residual[:, lanes] * residual[:, lanes]
            done += [vector_sq, residual_sq]
        return tuple(done)

    totals = lax.fori_loop(0, planes * spans, step, tuple(ref[...] for ref in sums))
    for ref, total in zip(sums, totals):
        ref[...] = total


def column_of(row):
    n = row.shape[1]
    same = lax.broadcasted_iota(jnp.int32, (n, n), 0) == lax.broadcasted_iota(jnp.int32, (n, n), 1)
    return jnp.sum(jnp.where(same, row, 0.0), axis=1, keepdims=True)


def spread_coefficients(coefficients, coefs, devices, which):
    out = lax.broadcasted_iota(jnp.int32, (40, 40), 0)
    vec = lax.broadcasted_iota(jnp.int32, (40, 40), 1)
    rest = out - 32
    group = jnp.where(out < 32, out >> 3, rest >> 1)
    place = jnp.where(out < 32, out & 7, 8 + (rest & 1))
    owner = devices[3]
    for k in range(3):
        owner = jnp.where(group == k, devices[k], owner)
    rows = jnp.where(vec == 10 * owner + place, 1.0, 0.0).astype(jnp.bfloat16)
    ordered = jnp.dot(rows, coefficients[...], preferred_element_type=jnp.float32).astype(jnp.bfloat16)
    rank = lax.broadcasted_iota(jnp.int32, (100, 64), 0)
    at = lax.broadcasted_iota(jnp.int32, (100, 64), 1)
    odd = at - 48
    for h in range(2):
        main = jnp.where(at < 24, 25 * devices[0] + at, 25 * devices[1] + at - 24)
        other = 25 * jnp.where((odd >> 1) == 0, devices[0], devices[1]) + 24
        other = jnp.where((odd < 4) & ((odd & 1) == h), other, -1)
        pick = jnp.where(rank == jnp.where(at < 48, main, other), 1.0, 0.0).astype(jnp.bfloat16)
        coefs[which, h] = jnp.dot(ordered, pick, preferred_element_type=jnp.float32).astype(jnp.bfloat16)


STEPS = 32760.0


def send_scaled(blocks, target):
    lane = lax.broadcasted_iota(jnp.int32, (8, 128), 1)
    powers, at = jnp.zeros((8, 128), jnp.float32), 0
    for k, parts in enumerate(blocks):
        top = jnp.max(jnp.abs(parts[0]), axis=1, keepdims=True)
        for part in parts[1:]:
            top = jnp.maximum(top, jnp.max(jnp.abs(part), axis=1, keepdims=True))
        power = jnp.ceil(jnp.log2(jnp.maximum(top, 1e-30)))
        powers = jnp.where(lane == k, power, powers)
        factor = jnp.exp2(-power) * STEPS
        for part in parts:
            target[:, at : at + HALF] = jnp.round(part * factor).astype(jnp.int32).astype(jnp.int16)
            at += HALF
    target[:, at : at + 128] = powers.astype(jnp.int32).astype(jnp.int16)


MESH = pl.DeviceIdType.MESH
PIECE = 2048
CHUNK = 4 * PIECE
HALF = PIECE // 2
ORDER = (0, 7, 1, 2, 3, 4, 5, 6)
AHEAD = 2
SUMS_LAG, VECS_LAG = 1, 2
OUTER = 7
LIMIT = 50_331_648


def whole_kernel(
    count, basis, coefficients_in, lower_in, upper_in, mass_in, damping_in, stiffness_in, eigen_in,
    eig_ref, res_ref, norm_ref, coefficients, lower, upper, mass, damping, stiffness, eigen_row, lists,
    odd_rows, extra, coefs, ea, eb, above_a, above_b, below_a, below_b, down_lists, ra, rb,
    part_a, part_b, to_sums, from_sums, mate_a, mate_b,
    first_a, first_b, last_a, last_b, square_a, residual_a, square_b, residual_b, squares,
    input_sem, own_sem, odd_sem, sent_sem, chunk_sem, plane_sem, square_recv_sem,
):
    me, sub = lax.axis_index("vecs"), lax.axis_index("rows")
    subs = lax.axis_size("rows")
    following, previous = lax.rem(sub + 1, subs), lax.rem(sub + subs - 1, subs)
    one, two = me + 1 - 2 * lax.rem(me, 2), 3 - me
    mates, crosses = (one, two), (two, one)
    halves = (lax.rem(lax.div(me + 1, 2), 2), lax.div(me, 2))
    basis_sem, extra_sem, sum_sem, vec_a_sem, vec_b_sem = (
        (sent_sem.at[k], chunk_sem.at[k]) for k in range(5)
    )
    square_sem = (sent_sem.at[5], square_recv_sem)

    barrier = pltpu.get_barrier_semaphore()
    for peer in mates:
        pl.semaphore_signal(barrier, inc=1, device_id={"vecs": peer}, device_id_type=MESH)

    @pl.loop(1, subs)
    def _(d):
        pl.semaphore_signal(barrier, inc=1, device_id={"rows": lax.rem(sub + d, subs)}, device_id_type=MESH)

    def remote(source, target, sems, at, peer):
        return pltpu.make_async_remote_copy(
            src_ref=source, dst_ref=target, send_sem=sems[0], recv_sem=sems[1].at[at],
            device_id=peer, device_id_type=MESH,
        )

    def all_of(block, sems, at=0):
        return remote(block, block, sems, at, {"vecs": one})

    def columns(c, x, half):
        return pl.ds(pl.multiple_of(c * CHUNK + x * CHUNK // 2 + half * PIECE, PIECE), PIECE)

    def send_basis(c):
        for x, (mate, half) in enumerate(zip(mates, halves)):
            remote(
                basis.at[pl.ds(0, 24), columns(c, x, 1 - half)], ra.at[c, x, 1], basis_sem, c, {"vecs": mate}
            ).start()

    def send_extra():
        for x, (mate, half) in enumerate(zip(mates, halves)):
            remote(extra.at[x, 1 - half], rb.at[x, 1], extra_sem, 0, {"vecs": mate}).start()

    def own_copies(c):
        for x, half in enumerate(halves):
            yield pltpu.make_async_copy(basis.at[pl.ds(0, 24), columns(c, x, half)], ra.at[c, x, 0], own_sem.at[c])

    def basis_arrived(c):
        pltpu.make_async_copy(ra.at[c, :, 0], ra.at[c, :, 0], own_sem.at[c]).wait()
        all_of(ra.at[c, :, 1], basis_sem, c).wait_recv()

    def send_sums(c):
        for x, cross in enumerate(crosses):
            remote(to_sums.at[c, x], from_sums.at[c, x], sum_sem, c, {"vecs": cross}).start()

    def send_vecs(c):
        for x, (mate, half) in enumerate(zip(mates, halves)):
            remote(mate_a.at[c, x], ea.at[:, columns(c, x, half)], vec_a_sem, c, {"vecs": mate}).start()
            remote(mate_b.at[c, x], eb.at[:, columns(c, x, half)], vec_b_sem, c, {"vecs": mate}).start()

    def vecs_arrived(c):
        all_of(mate_a.at[c], vec_a_sem, c).wait_recv()
        all_of(mate_b.at[c], vec_b_sem, c).wait_recv()

    rows_local = basis.shape[1]
    plane_copies = {
        ORDER[0]: (
            remote(ea.at[:, pl.ds(0, PLANE)], above_a, (plane_sem.at[0, 0], plane_sem.at[1]), 0, {"rows": previous}),
            remote(eb.at[:, pl.ds(0, PLANE)], above_b, (plane_sem.at[0, 1], plane_sem.at[1]), 1, {"rows": previous}),
        ),
        ORDER[1]: (
            remote(ea.at[:, pl.ds(rows_local - PLANE, PLANE)], below_a, (plane_sem.at[0, 2], plane_sem.at[1]), 2, {"rows": following}),
            remote(eb.at[:, pl.ds(rows_local - PLANE, PLANE)], below_b, (plane_sem.at[0, 3], plane_sem.at[1]), 3, {"rows": following}),
        ),
    }
    list_copy = remote(lists, down_lists, (plane_sem.at[0, 4], plane_sem.at[1]), 4, {"rows": following})

    inputs = [
        pltpu.make_async_copy(source, target, input_sem.at[i])
        for i, (source, target) in enumerate((
            (coefficients_in, coefficients), (lower_in, lower), (upper_in, upper), (eigen_in, eigen_row),
            (mass_in, mass), (damping_in, damping), (stiffness_in, stiffness),
        ))
    ]
    inputs[0].start()
    odd_copy = pltpu.make_async_copy(basis.at[pl.ds(24, 1), :], odd_rows, odd_sem)
    odd_copy.start()
    for c in ORDER:
        for copy in own_copies(c):
            copy.start()
    for copy in inputs[1:]:
        copy.start()
    pl.semaphore_wait(barrier, subs + 1)
    for c in ORDER[:AHEAD]:
        send_basis(c)
    odd_copy.wait()
    for c in ORDER:
        for q in range(4):
            at = c * CHUNK + q * PIECE
            pair = [odd_rows[0:1, at + h * HALF : at + (h + 1) * HALF].astype(jnp.float32) for h in range(2)]
            extra[q // 2, q % 2, c] = jnp.concatenate(pair, axis=0).astype(jnp.bfloat16)
    for x, half in enumerate(halves):
        rb[x, 0] = extra[x, half]
    send_extra()
    for copy in inputs[:4]:
        copy.wait()
    for x in range(2):
        devices = (me, mates[x], crosses[x], 6 - me - one - two)
        spread_coefficients(coefficients, coefs, devices, x)
    used = lax.broadcasted_iota(jnp.int32, (1, PLANE), 1) < count[0]
    lists[0:1, :] = jnp.where(used, lower[...], -1)
    lists[1:2, :] = jnp.where(used, upper[...], -1)
    list_copy.start()
    sums = (square_a, residual_a, square_b, residual_b)
    for ref in sums:
        ref[...] = jnp.zeros_like(ref)
    eigen = column_of(eigen_row[...])
    diag_refs = (mass, damping, stiffness)
    for copy in inputs[4:]:
        copy.wait()

    def planes_done(first, planes, links=None):
        residual_spans((ea, eb), (eig_ref, res_ref), diag_refs, eigen, first, planes, links, sums)

    def product(c):
        for x in range(2):
            outs = []
            for h in range(2):
                at = pl.ds(h * HALF, HALF)
                odd = jnp.concatenate(
                    [rb[x, q, c].astype(jnp.float32) for q in range(2)] + [jnp.zeros((12, HALF), jnp.float32)], axis=0
                )
                stack = jnp.concatenate([ra[c, x, 0, :, at], ra[c, x, 1, :, at], odd.astype(jnp.bfloat16)], axis=0)
                out = jnp.dot(coefs[x, h], stack, preferred_element_type=jnp.float32)
                part_a[c, x, :, at] = out[0:16]
                part_b[c, x, 4 * h : 4 * h + 4, :] = out[32:36]
                outs.append(out)
            ends = jnp.concatenate([out[36:40] for out in outs], axis=0)
            blocks = ([out[16:24] for out in outs], [out[24:32] for out in outs], [ends])
            send_scaled(blocks, to_sums.at[c, x])

    def combine(c):
        all_of(from_sums.at[c], sum_sem, c).wait_recv()
        for x, half in enumerate(halves):
            got = from_sums.at[c, x]
            whole = lambda k: got[:, k * HALF : (k + 1) * HALF].astype(jnp.int32).astype(jnp.float32)
            scale = jnp.exp2(got[:, 5 * HALF : 5 * HALF + 128].astype(jnp.int32).astype(jnp.float32)) * (1.0 / STEPS)
            ends = (part_b[c, x] + whole(4) * scale[:, 2:3]).astype(jnp.bfloat16)
            for h in range(2):
                at = pl.ds(h * HALF, HALF)
                here = pl.ds(pl.multiple_of(c * CHUNK + x * CHUNK // 2 + half * PIECE + h * HALF, HALF), HALF)
                ea[:, here] = (part_a[c, x, :8, at] + whole(h) * scale[:, 0:1]).astype(jnp.bfloat16)
                mate_a[c, x, :, at] = (part_a[c, x, 8:, at] + whole(2 + h) * scale[:, 1:2]).astype(jnp.bfloat16)
                eb[:, here] = ends[4 * h : 4 * h + 2]
                mate_b[c, x, :, at] = ends[4 * h + 2 : 4 * h + 4]
        send_vecs(c)

    def arrived(c):
        vecs_arrived(c)
        for copy in plane_copies.get(c, ()):
            copy.start()

    def first_links():
        for copy in plane_copies[ORDER[1]]:
            copy.wait_recv()
        list_copy.wait_recv()
        link_plane(below_a, below_b, down_lists, 0, 1, first_a, first_b)

    def last_links():
        for copy in plane_copies[ORDER[0]]:
            copy.wait_recv()
        link_plane(above_a, above_b, lists, 1, 0, last_a, last_b)

    def outer_planes():
        planes_done(0, 1, (first_a, first_b))
        planes_done(rows_local // PLANE - 1, 1, (last_a, last_b))

    later = {4: first_links, 5: last_links}
    depth = rows_local // PLANE
    present, waiting = set(), list(range(1, depth - 1))

    def settle(i):
        c = ORDER[i]
        arrived(c)
        present.update(range(c * CHUNK // PLANE, (c + 1) * CHUNK // PLANE))
        ready = [z for z in waiting if {z - 1, z, z + 1} <= present]
        while ready:
            n = 1
            while n < len(ready) and ready[n] == ready[0] + n:
                n += 1
            planes_done(ready[0], n)
            for z in ready[:n]:
                waiting.remove(z)
            ready = ready[n:]

    last = len(ORDER)
    all_of(rb.at[:, 1], extra_sem).wait_recv()
    for i in range(last + VECS_LAG):
        if i < last:
            basis_arrived(ORDER[i])
            product(ORDER[i])
            send_sums(ORDER[i])
            if i + AHEAD < last:
                send_basis(ORDER[i + AHEAD])
        if 0 <= i - SUMS_LAG < last:
            combine(ORDER[i - SUMS_LAG])
        if i in later:
            later[i]()
        if i == OUTER:
            outer_planes()
        if i >= VECS_LAG:
            settle(i - VECS_LAG)

    lane = lax.broadcasted_iota(jnp.int32, (1, 128), 1)
    message = jnp.zeros((1, 128), jnp.float32)
    for ref, start in ((square_a, 0), (square_b, 8), (residual_a, 16), (residual_b, 24)):
        column = jnp.sum(ref[...], axis=1, keepdims=True)
        row = lax.broadcasted_iota(jnp.int32, (ref.shape[0], 128), 0) + start
        message = message + jnp.sum(jnp.where(row == lane, column, 0.0), axis=0, keepdims=True)
    squares[sub] = message

    @pl.loop(1, subs)
    def _(d):
        remote(squares.at[sub], squares.at[sub], square_sem, 0, {"rows": lax.rem(sub + d, subs)}).start()

    for copies in plane_copies.values():
        for copy in copies:
            copy.wait_send()
    list_copy.wait_send()
    all_of(ra.at[:, :, 1], basis_sem).wait_send()
    all_of(rb.at[:, 1], extra_sem).wait_send()
    all_of(from_sums, sum_sem).wait_send()
    all_of(mate_a, vec_a_sem).wait_send()
    all_of(mate_b, vec_b_sem).wait_send()
    every = squares.at[pl.ds(0, subs - 1)]
    all_of(every, square_sem).wait_recv()
    all_of(every, square_sem).wait_send()
    total = jnp.sum(squares[...], axis=0)
    norms = jnp.sqrt(pltpu.roll(total, 112, 1)) / jnp.sqrt(total + 1.0)
    norm_ref[...] = norms[:, :10]


def whole(count, *arrays):
    basis = arrays[0]
    rows = basis.shape[1]
    chunks = rows // CHUNK
    subs = lax.axis_size("rows")
    vmem = pl.BlockSpec(memory_space=pltpu.VMEM)
    f32 = lambda *shape: pltpu.VMEM(shape, jnp.float32)
    bf16 = lambda *shape: pltpu.VMEM(shape, jnp.bfloat16)
    dma = pltpu.SemaphoreType.DMA
    return pl.pallas_call(
        whole_kernel,
        out_shape=(
            jax.ShapeDtypeStruct((10, rows), jnp.bfloat16),
            jax.ShapeDtypeStruct((10, rows), jnp.bfloat16),
            jax.ShapeDtypeStruct((1, 10), jnp.float32),
        ),
        in_specs=[pl.BlockSpec(memory_space=pltpu.SMEM)] + [pl.BlockSpec(memory_space=pltpu.HBM)] * 8,
        out_specs=(vmem,) * 3,
        scratch_shapes=[
            *[pltpu.VMEM(a.shape, a.dtype) for a in arrays[1:]], pltpu.VMEM((2, PLANE), jnp.int32),
            bf16(1, rows), bf16(2, 2, chunks, 2, HALF), bf16(2, 2, 40, 64), bf16(8, rows), bf16(2, rows),
            bf16(8, PLANE), bf16(2, PLANE), bf16(8, PLANE), bf16(2, PLANE), pltpu.VMEM((2, PLANE), jnp.int32),
            bf16(chunks, 2, 2, 24, PIECE), bf16(2, 2, chunks, 2, HALF),
            f32(chunks, 2, 16, PIECE), f32(chunks, 2, 8, HALF),
            *[pltpu.VMEM((chunks, 2, 8, 5 * HALF + 128), jnp.int16) for _ in range(2)],
            bf16(chunks, 2, 8, PIECE), bf16(chunks, 2, 2, PIECE),
            f32(8, PLANE), f32(2, PLANE), f32(8, PLANE), f32(2, PLANE),
            f32(8, 128), f32(8, 128), f32(2, 128), f32(2, 128), f32(subs, 1, 128),
            dma((7,)), dma((chunks,)), dma(()), dma((6,)), dma((5, chunks)), dma((2, 5)), dma((1,)),
        ],
        compiler_params=pltpu.CompilerParams(
            collective_id=0, has_side_effects=True, vmem_limit_bytes=LIMIT
        ),
        name="whole",
    )(count, *[pltpu.with_memory_space_constraint(a, pltpu.HBM) for a in arrays])


def on_device(basis, coefficients, eigen_values, stiffness, damping, mass, link_count, lower_cells, upper_cells):
    rows_local = basis.shape[1]
    wide = lambda a: a.reshape(1, rows_local)
    eig, res, norms = whole(
        link_count, basis, coefficients.T, lower_cells, upper_cells, wide(mass), wide(damping), wide(stiffness), eigen_values[None, :]
    )
    return eig, res, norms.reshape(10)


def solution(mesh):
    placed = (
        P("vecs", "rows"), P(), P("vecs"), P("rows"), P("rows"), P("rows"), P("rows"), P("rows", None), P("rows", None),
    )
    return jax.shard_map(
        on_device,
        mesh=mesh,
        in_specs=placed,
        out_specs=(P("vecs", "rows"), P("vecs", "rows"), P("vecs")),
        check_vma=False,
    )
```

```python
import functools

import jax
import jax.numpy as jnp
from jax import lax
from jax.experimental import pallas as pl
from jax.experimental.pallas import tpu as pltpu
from jax.sharding import PartitionSpec as P

WID = 64
PLANE = WID * WID
SPAN = 1024
SLOTS = 512
LOW = 256


def link_plane(part_a, part_b, lists, gather, scatter, link_a, link_b):
    high = PLANE // LOW
    whole = jnp.concatenate(
        [part_a[...].astype(jnp.float32), part_b[...].astype(jnp.float32), jnp.zeros((6, PLANE), jnp.float32)], axis=0
    ).astype(jnp.bfloat16)
    table = jnp.concatenate([whole[:, LOW * h : LOW * (h + 1)] for h in range(high)], axis=0)
    cell = lax.broadcasted_iota(jnp.int32, (LOW, SLOTS), 0)

    def step(t, total):
        at = pl.multiple_of(t * SLOTS, SLOTS)
        source = lists[gather : gather + 1, pl.ds(at, SLOTS)]
        target = lists[scatter : scatter + 1, pl.ds(at, SLOTS)]
        pick = jnp.where(cell == (source & (LOW - 1)), 1.0, 0.0).astype(jnp.bfloat16)
        rows = jnp.dot(table, pick, preferred_element_type=jnp.float32)
        source_high = source >> 8
        value = jnp.zeros((16, SLOTS), jnp.float32)
        for h in range(high):
            value = value + jnp.where(source_high == h, rows[16 * h : 16 * h + 16], 0.0)
        target_high = target >> 8
        spread = jnp.concatenate(
            [jnp.where(target_high == h, value, 0.0).astype(jnp.bfloat16) for h in range(high)], axis=0
        )
        place = jnp.where(cell == (target & (LOW - 1)), 1.0, 0.0).astype(jnp.bfloat16)
        return total + lax.dot_general(
            spread, place, (((1,), (1,)), ((), ())), preferred_element_type=jnp.float32
        )

    total = lax.fori_loop(0, PLANE // SLOTS, step, jnp.zeros((16 * high, LOW), jnp.float32))
    for h in range(high):
        link_a[:, LOW * h : LOW * (h + 1)] = total[16 * h : 16 * h + 8]
        link_b[:, LOW * h : LOW * (h + 1)] = total[16 * h + 8 : 16 * h + 10]


def residual_spans(vecs, outs, diag_refs, eigen, first, planes, links, sums):
    eig_ref, res_ref = outs
    depth = eig_ref.shape[1] // PLANE
    spans = PLANE // SPAN
    column = lax.broadcasted_iota(jnp.int32, (1, SPAN), 1) & (WID - 1)
    groups = ((vecs[0], slice(0, 8)), (vecs[1], slice(8, 10)))
    factors = []
    for _, part in groups:
        lam = eigen[part]
        factors.append((lam, lam * lam, lam * lam * 0.1 + lam * 0.3 + 1.0))

    def step(i, totals):
        c = i % spans
        base = pl.multiple_of(first * PLANE + i * SPAN, SPAN)
        here = pl.ds(base, SPAN)
        before = pl.ds(pl.multiple_of(jnp.where(c > 0, base - 128, base), 128), 128)
        after = pl.ds(pl.multiple_of(jnp.where(c < spans - 1, base + SPAN, base), 128), 128)
        mass, damping, stiffness = (r[:, here] for r in diag_refs)
        done = []
        for k, (ref, part) in enumerate(groups):
            lam, square, coupling = factors[k]
            raw = ref[:, here]
            value = raw.astype(jnp.float32)
            left = jnp.where(c > 0, ref[:, before].astype(jnp.float32), 0.0)
            right = jnp.where(c < spans - 1, ref[:, after].astype(jnp.float32), 0.0)
            wide = jnp.concatenate([left, value, right], axis=1)
            span = SPAN + 256
            total = pltpu.roll(wide, WID, 1)[:, 128 : 128 + SPAN] + pltpu.roll(wide, span - WID, 1)[:, 128 : 128 + SPAN]
            total = total + jnp.where(column > 0, pltpu.roll(value, 1, 1), 0.0)
            total = total + jnp.where(column < WID - 1, pltpu.roll(value, SPAN - 1, 1), 0.0)
            if not (links is not None and first == 0):
                total = total + ref[:, pl.ds(pl.multiple_of(base - PLANE, SPAN), SPAN)].astype(jnp.float32)
            if not (links is not None and first == depth - 1):
                total = total + ref[:, pl.ds(pl.multiple_of(base + PLANE, SPAN), SPAN)].astype(jnp.float32)
            if links is not None:
                total = total + links[k][:, pl.ds(pl.multiple_of(i * SPAN, SPAN), SPAN)]
            residual = (square * mass + lam * damping + stiffness) * value - coupling * total
            eig_ref[part, here] = raw
            res_ref[part, here] = residual.astype(jnp.bfloat16)
            vector_sq, residual_sq = totals[2 * k], totals[2 * k + 1]
            for t in range(SPAN // 128):
                lanes = slice(128 * t, 128 * (t + 1))
                vector_sq = vector_sq + value[:, lanes] * value[:, lanes]
                residual_sq = residual_sq + residual[:, lanes] * residual[:, lanes]
            done += [vector_sq, residual_sq]
        return tuple(done)

    totals = lax.fori_loop(0, planes * spans, step, tuple(ref[...] for ref in sums))
    for ref, total in zip(sums, totals):
        ref[...] = total


def column_of(row):
    n = row.shape[1]
    same = lax.broadcasted_iota(jnp.int32, (n, n), 0) == lax.broadcasted_iota(jnp.int32, (n, n), 1)
    return jnp.sum(jnp.where(same, row, 0.0), axis=1, keepdims=True)


def spread_coefficients(coefficients, coefs, devices, which):
    out = lax.broadcasted_iota(jnp.int32, (40, 40), 0)
    vec = lax.broadcasted_iota(jnp.int32, (40, 40), 1)
    rest = out - 32
    group = jnp.where(out < 32, out >> 3, rest >> 1)
    place = jnp.where(out < 32, out & 7, 8 + (rest & 1))
    owner = devices[3]
    for k in range(3):
        owner = jnp.where(group == k, devices[k], owner)
    rows = jnp.where(vec == 10 * owner + place, 1.0, 0.0).astype(jnp.bfloat16)
    ordered = jnp.dot(rows, coefficients[...], preferred_element_type=jnp.float32).astype(jnp.bfloat16)
    rank = lax.broadcasted_iota(jnp.int32, (100, 64), 0)
    at = lax.broadcasted_iota(jnp.int32, (100, 64), 1)
    odd = at - 48
    for h in range(2):
        main = jnp.where(at < 24, 25 * devices[0] + at, 25 * devices[1] + at - 24)
        other = 25 * jnp.where((odd >> 1) == 0, devices[0], devices[1]) + 24
        other = jnp.where((odd < 4) & ((odd & 1) == h), other, -1)
        pick = jnp.where(rank == jnp.where(at < 48, main, other), 1.0, 0.0).astype(jnp.bfloat16)
        coefs[which, h] = jnp.dot(ordered, pick, preferred_element_type=jnp.float32).astype(jnp.bfloat16)


STEPS = 32760.0


def send_scaled(blocks, target):
    lane = lax.broadcasted_iota(jnp.int32, (8, 128), 1)
    powers, at = jnp.zeros((8, 128), jnp.float32), 0
    for k, parts in enumerate(blocks):
        top = jnp.max(jnp.abs(parts[0]), axis=1, keepdims=True)
        for part in parts[1:]:
            top = jnp.maximum(top, jnp.max(jnp.abs(part), axis=1, keepdims=True))
        power = jnp.ceil(jnp.log2(jnp.maximum(top, 1e-30)))
        powers = jnp.where(lane == k, power, powers)
        factor = jnp.exp2(-power) * STEPS
        for part in parts:
            target[:, at : at + HALF] = jnp.round(part * factor).astype(jnp.int32).astype(jnp.int16)
            at += HALF
    target[:, at : at + 128] = powers.astype(jnp.int32).astype(jnp.int16)


MESH = pl.DeviceIdType.MESH
PIECE = 2048
CHUNK = 4 * PIECE
HALF = PIECE // 2
ORDER = (0, 7, 1, 2, 3, 4, 5, 6)
AHEAD = 2
SUMS_LAG, VECS_LAG = 1, 2
OUTER = 7
LIMIT = 50_331_648


def whole_kernel(
    count, basis, coefficients_in, lower_in, upper_in, mass_in, damping_in, stiffness_in, eigen_in,
    eig_ref, res_ref, norm_ref, coefficients, lower, upper, mass, damping, stiffness, eigen_row, lists,
    odd_rows, extra, coefs, ea, eb, above_a, above_b, below_a, below_b, down_lists, ra, rb,
    part_a, part_b, to_sums, from_sums, mate_a, mate_b,
    first_a, first_b, last_a, last_b, square_a, residual_a, square_b, residual_b, squares,
    input_sem, own_sem, odd_sem, sent_sem, chunk_sem, plane_sem, square_recv_sem,
):
    me, sub = lax.axis_index("vecs"), lax.axis_index("rows")
    subs = lax.axis_size("rows")
    following, previous = lax.rem(sub + 1, subs), lax.rem(sub + subs - 1, subs)
    one, two = me + 1 - 2 * lax.rem(me, 2), 3 - me
    mates, crosses = (one, two), (two, one)
    halves = (lax.rem(lax.div(me + 1, 2), 2), lax.div(me, 2))
    basis_sem, extra_sem, sum_sem, vec_a_sem, vec_b_sem = (
        (sent_sem.at[k], chunk_sem.at[k]) for k in range(5)
    )
    square_sem = (sent_sem.at[5], square_recv_sem)

    barrier = pltpu.get_barrier_semaphore()
    for peer in mates:
        pl.semaphore_signal(barrier, inc=1, device_id={"vecs": peer}, device_id_type=MESH)

    @pl.loop(1, subs)
    def _(d):
        pl.semaphore_signal(barrier, inc=1, device_id={"rows": lax.rem(sub + d, subs)}, device_id_type=MESH)

    def remote(source, target, sems, at, peer):
        return pltpu.make_async_remote_copy(
            src_ref=source, dst_ref=target, send_sem=sems[0], recv_sem=sems[1].at[at],
            device_id=peer, device_id_type=MESH,
        )

    def all_of(block, sems, at=0):
        return remote(block, block, sems, at, {"vecs": one})

    def columns(c, x, half):
        return pl.ds(pl.multiple_of(c * CHUNK + x * CHUNK // 2 + half * PIECE, PIECE), PIECE)

    def send_basis(c):
        for x, (mate, half) in enumerate(zip(mates, halves)):
            remote(
                basis.at[pl.ds(0, 24), columns(c, x, 1 - half)], ra.at[c, x, 1], basis_sem, c, {"vecs": mate}
            ).start()

    def send_extra():
        for x, (mate, half) in enumerate(zip(mates, halves)):
            remote(extra.at[x, 1 - half], rb.at[x, 1], extra_sem, 0, {"vecs": mate}).start()

    def own_copies(c):
        for x, half in enumerate(halves):
            yield pltpu.make_async_copy(basis.at[pl.ds(0, 24), columns(c, x, half)], ra.at[c, x, 0], own_sem.at[c])

    def basis_arrived(c):
        pltpu.make_async_copy(ra.at[c, :, 0], ra.at[c, :, 0], own_sem.at[c]).wait()
        all_of(ra.at[c, :, 1], basis_sem, c).wait_recv()

    def send_sums(c):
        for x, cross in enumerate(crosses):
            remote(to_sums.at[c, x], from_sums.at[c, x], sum_sem, c, {"vecs": cross}).start()

    def send_vecs(c):
        for x, (mate, half) in enumerate(zip(mates, halves)):
            remote(mate_a.at[c, x], ea.at[:, columns(c, x, half)], vec_a_sem, c, {"vecs": mate}).start()
            remote(mate_b.at[c, x], eb.at[:, columns(c, x, half)], vec_b_sem, c, {"vecs": mate}).start()

    def vecs_arrived(c):
        all_of(mate_a.at[c], vec_a_sem, c).wait_recv()
        all_of(mate_b.at[c], vec_b_sem, c).wait_recv()

    rows_local = basis.shape[1]
    plane_copies = {
        ORDER[0]: (
            remote(ea.at[:, pl.ds(0, PLANE)], above_a, (plane_sem.at[0, 0], plane_sem.at[1]), 0, {"rows": previous}),
            remote(eb.at[:, pl.ds(0, PLANE)], above_b, (plane_sem.at[0, 1], plane_sem.at[1]), 1, {"rows": previous}),
        ),
        ORDER[1]: (
            remote(ea.at[:, pl.ds(rows_local - PLANE, PLANE)], below_a, (plane_sem.at[0, 2], plane_sem.at[1]), 2, {"rows": following}),
            remote(eb.at[:, pl.ds(rows_local - PLANE, PLANE)], below_b, (plane_sem.at[0, 3], plane_sem.at[1]), 3, {"rows": following}),
        ),
    }
    list_copy = remote(lists, down_lists, (plane_sem.at[0, 4], plane_sem.at[1]), 4, {"rows": following})

    inputs = [
        pltpu.make_async_copy(source, target, input_sem.at[i])
        for i, (source, target) in enumerate((
            (coefficients_in, coefficients), (lower_in, lower), (upper_in, upper), (eigen_in, eigen_row),
            (mass_in, mass), (damping_in, damping), (stiffness_in, stiffness),
        ))
    ]
    inputs[0].start()
    odd_copy = pltpu.make_async_copy(basis.at[pl.ds(24, 1), :], odd_rows, odd_sem)
    odd_copy.start()
    for c in ORDER:
        for copy in own_copies(c):
            copy.start()
    for copy in inputs[1:]:
        copy.start()
    pl.semaphore_wait(barrier, subs + 1)
    for c in ORDER[:AHEAD]:
        send_basis(c)
    odd_copy.wait()
    for c in ORDER:
        for q in range(4):
            at = c * CHUNK + q * PIECE
            pair = [odd_rows[0:1, at + h * HALF : at + (h + 1) * HALF].astype(jnp.float32) for h in range(2)]
            extra[q // 2, q % 2, c] = jnp.concatenate(pair, axis=0).astype(jnp.bfloat16)
    for x, half in enumerate(halves):
        rb[x, 0] = extra[x, half]
    send_extra()
    for copy in inputs[:4]:
        copy.wait()
    for x in range(2):
        devices = (me, mates[x], crosses[x], 6 - me - one - two)
        spread_coefficients(coefficients, coefs, devices, x)
    used = lax.broadcasted_iota(jnp.int32, (1, PLANE), 1) < count[0]
    lists[0:1, :] = jnp.where(used, lower[...], -1)
    lists[1:2, :] = jnp.where(used, upper[...], -1)
    list_copy.start()
    sums = (square_a, residual_a, square_b, residual_b)
    for ref in sums:
        ref[...] = jnp.zeros_like(ref)
    eigen = column_of(eigen_row[...])
    diag_refs = (mass, damping, stiffness)
    for copy in inputs[4:]:
        copy.wait()

    def planes_done(first, planes, links=None):
        residual_spans((ea, eb), (eig_ref, res_ref), diag_refs, eigen, first, planes, links, sums)

    def product(c):
        for x in range(2):
            outs = []
            for h in range(2):
                at = pl.ds(h * HALF, HALF)
                odd = jnp.concatenate(
                    [rb[x, q, c].astype(jnp.float32) for q in range(2)] + [jnp.zeros((12, HALF), jnp.float32)], axis=0
                )
                stack = jnp.concatenate([ra[c, x, 0, :, at], ra[c, x, 1, :, at], odd.astype(jnp.bfloat16)], axis=0)
                out = jnp.dot(coefs[x, h], stack, preferred_element_type=jnp.float32)
                part_a[c, x, :, at] = out[0:16]
                part_b[c, x, 4 * h : 4 * h + 4, :] = out[32:36]
                outs.append(out)
            ends = jnp.concatenate([out[36:40] for out in outs], axis=0)
            blocks = ([out[16:24] for out in outs], [out[24:32] for out in outs], [ends])
            send_scaled(blocks, to_sums.at[c, x])

    def combine(c):
        all_of(from_sums.at[c], sum_sem, c).wait_recv()
        for x, half in enumerate(halves):
            got = from_sums.at[c, x]
            whole = lambda k: got[:, k * HALF : (k + 1) * HALF].astype(jnp.int32).astype(jnp.float32)
            scale = jnp.exp2(got[:, 5 * HALF : 5 * HALF + 128].astype(jnp.int32).astype(jnp.float32)) * (1.0 / STEPS)
            ends = (part_b[c, x] + whole(4) * scale[:, 2:3]).astype(jnp.bfloat16)
            for h in range(2):
                at = pl.ds(h * HALF, HALF)
                here = pl.ds(pl.multiple_of(c * CHUNK + x * CHUNK // 2 + half * PIECE + h * HALF, HALF), HALF)
                ea[:, here] = (part_a[c, x, :8, at] + whole(h) * scale[:, 0:1]).astype(jnp.bfloat16)
                mate_a[c, x, :, at] = (part_a[c, x, 8:, at] + whole(2 + h) * scale[:, 1:2]).astype(jnp.bfloat16)
                eb[:, here] = ends[4 * h : 4 * h + 2]
                mate_b[c, x, :, at] = ends[4 * h + 2 : 4 * h + 4]
        send_vecs(c)

    def arrived(c):
        vecs_arrived(c)
        for copy in plane_copies.get(c, ()):
            copy.start()

    def first_links():
        for copy in plane_copies[ORDER[1]]:
            copy.wait_recv()
        list_copy.wait_recv()
        link_plane(below_a, below_b, down_lists, 0, 1, first_a, first_b)

    def last_links():
        for copy in plane_copies[ORDER[0]]:
            copy.wait_recv()
        link_plane(above_a, above_b, lists, 1, 0, last_a, last_b)

    def outer_planes():
        planes_done(0, 1, (first_a, first_b))
        planes_done(rows_local // PLANE - 1, 1, (last_a, last_b))

    later = {4: first_links, 5: last_links}
    depth = rows_local // PLANE
    present, waiting = set(), list(range(1, depth - 1))

    def settle(i):
        c = ORDER[i]
        arrived(c)
        present.update(range(c * CHUNK // PLANE, (c + 1) * CHUNK // PLANE))
        ready = [z for z in waiting if {z - 1, z, z + 1} <= present]
        while ready:
            n = 1
            while n < len(ready) and ready[n] == ready[0] + n:
                n += 1
            planes_done(ready[0], n)
            for z in ready[:n]:
                waiting.remove(z)
            ready = ready[n:]

    last = len(ORDER)
    all_of(rb.at[:, 1], extra_sem).wait_recv()
    for i in range(last + VECS_LAG):
        if i < last:
            basis_arrived(ORDER[i])
            product(ORDER[i])
            send_sums(ORDER[i])
        if 0 <= i - SUMS_LAG < last:
            combine(ORDER[i - SUMS_LAG])
        if i + AHEAD < last:
            send_basis(ORDER[i + AHEAD])
        if i in later:
            later[i]()
        if i == OUTER:
            outer_planes()
        if i >= VECS_LAG:
            settle(i - VECS_LAG)

    lane = lax.broadcasted_iota(jnp.int32, (1, 128), 1)
    message = jnp.zeros((1, 128), jnp.float32)
    for ref, start in ((square_a, 0), (square_b, 8), (residual_a, 16), (residual_b, 24)):
        column = jnp.sum(ref[...], axis=1, keepdims=True)
        row = lax.broadcasted_iota(jnp.int32, (ref.shape[0], 128), 0) + start
        message = message + jnp.sum(jnp.where(row == lane, column, 0.0), axis=0, keepdims=True)
    squares[sub] = message

    @pl.loop(1, subs)
    def _(d):
        remote(squares.at[sub], squares.at[sub], square_sem, 0, {"rows": lax.rem(sub + d, subs)}).start()

    for copies in plane_copies.values():
        for copy in copies:
            copy.wait_send()
    list_copy.wait_send()
    all_of(ra.at[:, :, 1], basis_sem).wait_send()
    all_of(rb.at[:, 1], extra_sem).wait_send()
    all_of(from_sums, sum_sem).wait_send()
    all_of(mate_a, vec_a_sem).wait_send()
    all_of(mate_b, vec_b_sem).wait_send()
    every = squares.at[pl.ds(0, subs - 1)]
    all_of(every, square_sem).wait_recv()
    all_of(every, square_sem).wait_send()
    total = jnp.sum(squares[...], axis=0)
    norms = jnp.sqrt(pltpu.roll(total, 112, 1)) / jnp.sqrt(total + 1.0)
    norm_ref[...] = norms[:, :10]


def whole(count, *arrays):
    basis = arrays[0]
    rows = basis.shape[1]
    chunks = rows // CHUNK
    subs = lax.axis_size("rows")
    vmem = pl.BlockSpec(memory_space=pltpu.VMEM)
    f32 = lambda *shape: pltpu.VMEM(shape, jnp.float32)
    bf16 = lambda *shape: pltpu.VMEM(shape, jnp.bfloat16)
    dma = pltpu.SemaphoreType.DMA
    return pl.pallas_call(
        whole_kernel,
        out_shape=(
            jax.ShapeDtypeStruct((10, rows), jnp.bfloat16),
            jax.ShapeDtypeStruct((10, rows), jnp.bfloat16),
            jax.ShapeDtypeStruct((1, 10), jnp.float32),
        ),
        in_specs=[pl.BlockSpec(memory_space=pltpu.SMEM)] + [pl.BlockSpec(memory_space=pltpu.HBM)] * 8,
        out_specs=(vmem,) * 3,
        scratch_shapes=[
            *[pltpu.VMEM(a.shape, a.dtype) for a in arrays[1:]], pltpu.VMEM((2, PLANE), jnp.int32),
            bf16(1, rows), bf16(2, 2, chunks, 2, HALF), bf16(2, 2, 40, 64), bf16(8, rows), bf16(2, rows),
            bf16(8, PLANE), bf16(2, PLANE), bf16(8, PLANE), bf16(2, PLANE), pltpu.VMEM((2, PLANE), jnp.int32),
            bf16(chunks, 2, 2, 24, PIECE), bf16(2, 2, chunks, 2, HALF),
            f32(chunks, 2, 16, PIECE), f32(chunks, 2, 8, HALF),
            *[pltpu.VMEM((chunks, 2, 8, 5 * HALF + 128), jnp.int16) for _ in range(2)],
            bf16(chunks, 2, 8, PIECE), bf16(chunks, 2, 2, PIECE),
            f32(8, PLANE), f32(2, PLANE), f32(8, PLANE), f32(2, PLANE),
            f32(8, 128), f32(8, 128), f32(2, 128), f32(2, 128), f32(subs, 1, 128),
            dma((7,)), dma((chunks,)), dma(()), dma((6,)), dma((5, chunks)), dma((2, 5)), dma((1,)),
        ],
        compiler_params=pltpu.CompilerParams(
            collective_id=0, has_side_effects=True, vmem_limit_bytes=LIMIT
        ),
        name="whole",
    )(count, *[pltpu.with_memory_space_constraint(a, pltpu.HBM) for a in arrays])


def store_kernel(*refs):
    sources, targets, sems = refs[:3], refs[3:6], refs[6]
    copies = [
        pltpu.make_async_copy(source, target, sems.at[k]) for k, (source, target) in enumerate(zip(sources, targets))
    ]
    for copy in copies:
        copy.start()
    for copy in copies:
        copy.wait()


def store(*arrays):
    return pl.pallas_call(
        store_kernel,
        out_shape=tuple(jax.ShapeDtypeStruct(a.shape, a.dtype) for a in arrays),
        in_specs=[pl.BlockSpec(memory_space=pltpu.VMEM)] * 3,
        out_specs=(pl.BlockSpec(memory_space=pltpu.HBM),) * 3,
        scratch_shapes=[pltpu.SemaphoreType.DMA((3,))],
        compiler_params=pltpu.CompilerParams(vmem_limit_bytes=16 * 2**20),
        name="store",
    )(*arrays)


def on_device(basis, coefficients, eigen_values, stiffness, damping, mass, link_count, lower_cells, upper_cells):
    rows_local = basis.shape[1]
    wide = lambda a: a.reshape(1, rows_local)
    eig, res, norms = whole(
        link_count, basis, coefficients.T, lower_cells, upper_cells, wide(mass), wide(damping), wide(stiffness), eigen_values[None, :]
    )
    eig, res, norms = store(eig, res, norms)
    return eig, res, norms.reshape(10)


def solution(mesh):
    placed = (
        P("vecs", "rows"), P(), P("vecs"), P("rows"), P("rows"), P("rows"), P("rows"), P("rows", None), P("rows", None),
    )
    return jax.shard_map(
        on_device,
        mesh=mesh,
        in_specs=placed,
        out_specs=(P("vecs", "rows"), P("vecs", "rows"), P("vecs")),
        check_vma=False,
    )
```

```python
import functools

import jax
import jax.numpy as jnp
from jax import lax
from jax.experimental import pallas as pl
from jax.experimental.pallas import tpu as pltpu
from jax.sharding import PartitionSpec as P

WID = 64
PLANE = WID * WID
SPAN = 2048
SLOTS = 1024
LOW = 256


def link_plane(part_a, part_b, lists, gather, scatter, link_a, link_b):
    high = PLANE // LOW
    whole = jnp.concatenate(
        [part_a[...].astype(jnp.float32), part_b[...].astype(jnp.float32), jnp.zeros((6, PLANE), jnp.float32)], axis=0
    ).astype(jnp.bfloat16)
    table = jnp.concatenate([whole[:, LOW * h : LOW * (h + 1)] for h in range(high)], axis=0)
    cell = lax.broadcasted_iota(jnp.int32, (LOW, SLOTS), 0)

    def step(t, total):
        at = pl.multiple_of(t * SLOTS, SLOTS)
        source = lists[gather : gather + 1, pl.ds(at, SLOTS)]
        target = lists[scatter : scatter + 1, pl.ds(at, SLOTS)]
        pick = jnp.where(cell == (source & (LOW - 1)), 1.0, 0.0).astype(jnp.bfloat16)
        rows = jnp.dot(table, pick, preferred_element_type=jnp.float32)
        source_high = source >> 8
        value = jnp.zeros((16, SLOTS), jnp.float32)
        for h in range(high):
            value = value + jnp.where(source_high == h, rows[16 * h : 16 * h + 16], 0.0)
        target_high = target >> 8
        spread = jnp.concatenate(
            [jnp.where(target_high == h, value, 0.0).astype(jnp.bfloat16) for h in range(high)], axis=0
        )
        place = jnp.where(cell == (target & (LOW - 1)), 1.0, 0.0).astype(jnp.bfloat16)
        return total + lax.dot_general(
            spread, place, (((1,), (1,)), ((), ())), preferred_element_type=jnp.float32
        )

    total = lax.fori_loop(0, PLANE // SLOTS, step, jnp.zeros((16 * high, LOW), jnp.float32))
    for h in range(high):
        link_a[:, LOW * h : LOW * (h + 1)] = total[16 * h : 16 * h + 8]
        link_b[:, LOW * h : LOW * (h + 1)] = total[16 * h + 8 : 16 * h + 10]


def residual_spans(vecs, outs, diag_refs, eigen, first, planes, links, sums):
    eig_ref, res_ref = outs
    depth = eig_ref.shape[1] // PLANE
    spans = PLANE // SPAN
    column = lax.broadcasted_iota(jnp.int32, (1, SPAN), 1) & (WID - 1)
    groups = ((vecs[0], slice(0, 8)), (vecs[1], slice(8, 10)))
    factors = []
    for _, part in groups:
        lam = eigen[part]
        factors.append((lam, lam * lam, lam * lam * 0.1 + lam * 0.3 + 1.0))

    def step(i, totals):
        c = i % spans
        base = pl.multiple_of(first * PLANE + i * SPAN, SPAN)
        here = pl.ds(base, SPAN)
        before = pl.ds(pl.multiple_of(jnp.where(c > 0, base - 128, base), 128), 128)
        after = pl.ds(pl.multiple_of(jnp.where(c < spans - 1, base + SPAN, base), 128), 128)
        mass, damping, stiffness = (r[:, here] for r in diag_refs)
        done = []
        for k, (ref, part) in enumerate(groups):
            lam, square, coupling = factors[k]
            raw = ref[:, here]
            value = raw.astype(jnp.float32)
            left = jnp.where(c > 0, ref[:, before].astype(jnp.float32), 0.0)
            right = jnp.where(c < spans - 1, ref[:, after].astype(jnp.float32), 0.0)
            wide = jnp.concatenate([left, value, right], axis=1)
            span = SPAN + 256
            total = pltpu.roll(wide, WID, 1)[:, 128 : 128 + SPAN] + pltpu.roll(wide, span - WID, 1)[:, 128 : 128 + SPAN]
            total = total + jnp.where(column > 0, pltpu.roll(value, 1, 1), 0.0)
            total = total + jnp.where(column < WID - 1, pltpu.roll(value, SPAN - 1, 1), 0.0)
            if not (links is not None and first == 0):
                total = total + ref[:, pl.ds(pl.multiple_of(base - PLANE, SPAN), SPAN)].astype(jnp.float32)
            if not (links is not None and first == depth - 1):
                total = total + ref[:, pl.ds(pl.multiple_of(base + PLANE, SPAN), SPAN)].astype(jnp.float32)
            if links is not None:
                total = total + links[k][:, pl.ds(pl.multiple_of(i * SPAN, SPAN), SPAN)]
            residual = (square * mass + lam * damping + stiffness) * value - coupling * total
            eig_ref[part, here] = raw
            res_ref[part, here] = residual.astype(jnp.bfloat16)
            vector_sq, residual_sq = totals[2 * k], totals[2 * k + 1]
            for t in range(SPAN // 128):
                lanes = slice(128 * t, 128 * (t + 1))
                vector_sq = vector_sq + value[:, lanes] * value[:, lanes]
                residual_sq = residual_sq + residual[:, lanes] * residual[:, lanes]
            done += [vector_sq, residual_sq]
        return tuple(done)

    totals = lax.fori_loop(0, planes * spans, step, tuple(ref[...] for ref in sums), unroll=2)
    for ref, total in zip(sums, totals):
        ref[...] = total


def column_of(row):
    n = row.shape[1]
    same = lax.broadcasted_iota(jnp.int32, (n, n), 0) == lax.broadcasted_iota(jnp.int32, (n, n), 1)
    return jnp.sum(jnp.where(same, row, 0.0), axis=1, keepdims=True)


def spread_coefficients(coefficients, coefs, devices, which):
    out = lax.broadcasted_iota(jnp.int32, (40, 40), 0)
    vec = lax.broadcasted_iota(jnp.int32, (40, 40), 1)
    rest = out - 32
    group = jnp.where(out < 32, out >> 3, rest >> 1)
    place = jnp.where(out < 32, out & 7, 8 + (rest & 1))
    owner = devices[3]
    for k in range(3):
        owner = jnp.where(group == k, devices[k], owner)
    rows = jnp.where(vec == 10 * owner + place, 1.0, 0.0).astype(jnp.bfloat16)
    ordered = jnp.dot(rows, coefficients[...], preferred_element_type=jnp.float32).astype(jnp.bfloat16)
    rank = lax.broadcasted_iota(jnp.int32, (100, 64), 0)
    at = lax.broadcasted_iota(jnp.int32, (100, 64), 1)
    odd = at - 48
    for h in range(2):
        main = jnp.where(at < 24, 25 * devices[0] + at, 25 * devices[1] + at - 24)
        other = 25 * jnp.where((odd >> 1) == 0, devices[0], devices[1]) + 24
        other = jnp.where((odd < 4) & ((odd & 1) == h), other, -1)
        pick = jnp.where(rank == jnp.where(at < 48, main, other), 1.0, 0.0).astype(jnp.bfloat16)
        coefs[which, h] = jnp.dot(ordered, pick, preferred_element_type=jnp.float32).astype(jnp.bfloat16)


STEPS = 32760.0


def send_scaled(blocks, target):
    lane = lax.broadcasted_iota(jnp.int32, (8, 128), 1)
    powers, at = jnp.zeros((8, 128), jnp.float32), 0
    for k, parts in enumerate(blocks):
        top = jnp.max(jnp.abs(parts[0]), axis=1, keepdims=True)
        for part in parts[1:]:
            top = jnp.maximum(top, jnp.max(jnp.abs(part), axis=1, keepdims=True))
        power = jnp.ceil(jnp.log2(jnp.maximum(top, 1e-30)))
        powers = jnp.where(lane == k, power, powers)
        factor = jnp.exp2(-power) * STEPS
        for part in parts:
            target[:, at : at + HALF] = jnp.round(part * factor).astype(jnp.int32).astype(jnp.int16)
            at += HALF
    target[:, at : at + 128] = powers.astype(jnp.int32).astype(jnp.int16)


MESH = pl.DeviceIdType.MESH
PIECE = 2048
CHUNK = 4 * PIECE
HALF = PIECE // 2
ORDER = (0, 7, 1, 2, 3, 4, 5, 6)
AHEAD = 2
SUMS_LAG, VECS_LAG = 1, 2
OUTER = 7
LIMIT = 50_331_648


def whole_kernel(
    count, basis, coefficients_in, lower_in, upper_in, mass_in, damping_in, stiffness_in, eigen_in,
    eig_ref, res_ref, norm_ref, coefficients, lower, upper, mass, damping, stiffness, eigen_row, lists,
    odd_rows, extra, coefs, ea, eb, above_a, above_b, below_a, below_b, down_lists, ra, rb,
    part_a, part_b, to_sums, from_sums, mate_a, mate_b,
    first_a, first_b, last_a, last_b, square_a, residual_a, square_b, residual_b, squares,
    input_sem, own_sem, odd_sem, sent_sem, chunk_sem, plane_sem, square_recv_sem,
):
    me, sub = lax.axis_index("vecs"), lax.axis_index("rows")
    subs = lax.axis_size("rows")
    following, previous = lax.rem(sub + 1, subs), lax.rem(sub + subs - 1, subs)
    one, two = me + 1 - 2 * lax.rem(me, 2), 3 - me
    mates, crosses = (one, two), (two, one)
    halves = (lax.rem(lax.div(me + 1, 2), 2), lax.div(me, 2))
    basis_sem, extra_sem, sum_sem, vec_a_sem, vec_b_sem = (
        (sent_sem.at[k], chunk_sem.at[k]) for k in range(5)
    )
    square_sem = (sent_sem.at[5], square_recv_sem)

    barrier = pltpu.get_barrier_semaphore()
    for peer in mates:
        pl.semaphore_signal(barrier, inc=1, device_id={"vecs": peer}, device_id_type=MESH)

    @pl.loop(1, subs)
    def _(d):
        pl.semaphore_signal(barrier, inc=1, device_id={"rows": lax.rem(sub + d, subs)}, device_id_type=MESH)

    def remote(source, target, sems, at, peer):
        return pltpu.make_async_remote_copy(
            src_ref=source, dst_ref=target, send_sem=sems[0], recv_sem=sems[1].at[at],
            device_id=peer, device_id_type=MESH,
        )

    def all_of(block, sems, at=0):
        return remote(block, block, sems, at, {"vecs": one})

    def columns(c, x, half):
        return pl.ds(pl.multiple_of(c * CHUNK + x * CHUNK // 2 + half * PIECE, PIECE), PIECE)

    def send_basis(c):
        for x, (mate, half) in enumerate(zip(mates, halves)):
            remote(
                basis.at[pl.ds(0, 24), columns(c, x, 1 - half)], ra.at[c, x, 1], basis_sem, c, {"vecs": mate}
            ).start()

    def send_extra():
        for x, (mate, half) in enumerate(zip(mates, halves)):
            remote(extra.at[x, 1 - half], rb.at[x, 1], extra_sem, 0, {"vecs": mate}).start()

    def own_copies(c):
        for x, half in enumerate(halves):
            yield pltpu.make_async_copy(basis.at[pl.ds(0, 24), columns(c, x, half)], ra.at[c, x, 0], own_sem.at[c])

    def basis_arrived(c):
        pltpu.make_async_copy(ra.at[c, :, 0], ra.at[c, :, 0], own_sem.at[c]).wait()
        all_of(ra.at[c, :, 1], basis_sem, c).wait_recv()

    def send_sums(c):
        for x, cross in enumerate(crosses):
            remote(to_sums.at[c, x], from_sums.at[c, x], sum_sem, c, {"vecs": cross}).start()

    def send_vecs(c):
        for x, (mate, half) in enumerate(zip(mates, halves)):
            remote(mate_a.at[c, x], ea.at[:, columns(c, x, half)], vec_a_sem, c, {"vecs": mate}).start()
            remote(mate_b.at[c, x], eb.at[:, columns(c, x, half)], vec_b_sem, c, {"vecs": mate}).start()

    def vecs_arrived(c):
        all_of(mate_a.at[c], vec_a_sem, c).wait_recv()
        all_of(mate_b.at[c], vec_b_sem, c).wait_recv()

    rows_local = basis.shape[1]
    plane_copies = {
        ORDER[0]: (
            remote(ea.at[:, pl.ds(0, PLANE)], above_a, (plane_sem.at[0, 0], plane_sem.at[1]), 0, {"rows": previous}),
            remote(eb.at[:, pl.ds(0, PLANE)], above_b, (plane_sem.at[0, 1], plane_sem.at[1]), 1, {"rows": previous}),
        ),
        ORDER[1]: (
            remote(ea.at[:, pl.ds(rows_local - PLANE, PLANE)], below_a, (plane_sem.at[0, 2], plane_sem.at[1]), 2, {"rows": following}),
            remote(eb.at[:, pl.ds(rows_local - PLANE, PLANE)], below_b, (plane_sem.at[0, 3], plane_sem.at[1]), 3, {"rows": following}),
        ),
    }
    list_copy = remote(lists, down_lists, (plane_sem.at[0, 4], plane_sem.at[1]), 4, {"rows": following})

    inputs = [
        pltpu.make_async_copy(source, target, input_sem.at[i])
        for i, (source, target) in enumerate((
            (coefficients_in, coefficients), (lower_in, lower), (upper_in, upper), (eigen_in, eigen_row),
            (mass_in, mass), (damping_in, damping), (stiffness_in, stiffness),
        ))
    ]
    inputs[0].start()
    odd_copy = pltpu.make_async_copy(basis.at[pl.ds(24, 1), :], odd_rows, odd_sem)
    odd_copy.start()
    for c in ORDER:
        for copy in own_copies(c):
            copy.start()
    for copy in inputs[1:]:
        copy.start()
    pl.semaphore_wait(barrier, subs + 1)
    for c in ORDER[:AHEAD]:
        send_basis(c)
    odd_copy.wait()
    for c in ORDER:
        for q in range(4):
            at = c * CHUNK + q * PIECE
            pair = [odd_rows[0:1, at + h * HALF : at + (h + 1) * HALF].astype(jnp.float32) for h in range(2)]
            extra[q // 2, q % 2, c] = jnp.concatenate(pair, axis=0).astype(jnp.bfloat16)
    for x, half in enumerate(halves):
        rb[x, 0] = extra[x, half]
    send_extra()
    for copy in inputs[:4]:
        copy.wait()
    for x in range(2):
        devices = (me, mates[x], crosses[x], 6 - me - one - two)
        spread_coefficients(coefficients, coefs, devices, x)
    used = lax.broadcasted_iota(jnp.int32, (1, PLANE), 1) < count[0]
    lists[0:1, :] = jnp.where(used, lower[...], -1)
    lists[1:2, :] = jnp.where(used, upper[...], -1)
    list_copy.start()
    sums = (square_a, residual_a, square_b, residual_b)
    for ref in sums:
        ref[...] = jnp.zeros_like(ref)
    eigen = column_of(eigen_row[...])
    diag_refs = (mass, damping, stiffness)
    for copy in inputs[4:]:
        copy.wait()

    def planes_done(first, planes, links=None):
        residual_spans((ea, eb), (eig_ref, res_ref), diag_refs, eigen, first, planes, links, sums)

    def product(c):
        for x in range(2):
            outs = []
            for h in range(2):
                at = pl.ds(h * HALF, HALF)
                odd = jnp.concatenate(
                    [rb[x, q, c].astype(jnp.float32) for q in range(2)] + [jnp.zeros((12, HALF), jnp.float32)], axis=0
                )
                stack = jnp.concatenate([ra[c, x, 0, :, at], ra[c, x, 1, :, at], odd.astype(jnp.bfloat16)], axis=0)
                out = jnp.dot(coefs[x, h], stack, preferred_element_type=jnp.float32)
                part_a[c, x, :, at] = out[0:16]
                part_b[c, x, 4 * h : 4 * h + 4, :] = out[32:36]
                outs.append(out)
            ends = jnp.concatenate([out[36:40] for out in outs], axis=0)
            blocks = ([out[16:24] for out in outs], [out[24:32] for out in outs], [ends])
            send_scaled(blocks, to_sums.at[c, x])

    def combine(c):
        all_of(from_sums.at[c], sum_sem, c).wait_recv()
        for x, half in enumerate(halves):
            got = from_sums.at[c, x]
            whole = lambda k: got[:, k * HALF : (k + 1) * HALF].astype(jnp.int32).astype(jnp.float32)
            scale = jnp.exp2(got[:, 5 * HALF : 5 * HALF + 128].astype(jnp.int32).astype(jnp.float32)) * (1.0 / STEPS)
            ends = (part_b[c, x] + whole(4) * scale[:, 2:3]).astype(jnp.bfloat16)
            for h in range(2):
                at = pl.ds(h * HALF, HALF)
                here = pl.ds(pl.multiple_of(c * CHUNK + x * CHUNK // 2 + half * PIECE + h * HALF, HALF), HALF)
                ea[:, here] = (part_a[c, x, :8, at] + whole(h) * scale[:, 0:1]).astype(jnp.bfloat16)
                mate_a[c, x, :, at] = (part_a[c, x, 8:, at] + whole(2 + h) * scale[:, 1:2]).astype(jnp.bfloat16)
                eb[:, here] = ends[4 * h : 4 * h + 2]
                mate_b[c, x, :, at] = ends[4 * h + 2 : 4 * h + 4]
        send_vecs(c)

    def arrived(c):
        vecs_arrived(c)
        for copy in plane_copies.get(c, ()):
            copy.start()

    def first_links():
        for copy in plane_copies[ORDER[1]]:
            copy.wait_recv()
        list_copy.wait_recv()
        link_plane(below_a, below_b, down_lists, 0, 1, first_a, first_b)

    def last_links():
        for copy in plane_copies[ORDER[0]]:
            copy.wait_recv()
        link_plane(above_a, above_b, lists, 1, 0, last_a, last_b)

    def outer_planes():
        planes_done(0, 1, (first_a, first_b))
        planes_done(rows_local // PLANE - 1, 1, (last_a, last_b))

    later = {4: first_links, 5: last_links}
    depth = rows_local // PLANE
    present, waiting = set(), list(range(1, depth - 1))

    def settle(i):
        c = ORDER[i]
        arrived(c)
        present.update(range(c * CHUNK // PLANE, (c + 1) * CHUNK // PLANE))
        ready = [z for z in waiting if {z - 1, z, z + 1} <= present]
        while ready:
            n = 1
            while n < len(ready) and ready[n] == ready[0] + n:
                n += 1
            planes_done(ready[0], n)
            for z in ready[:n]:
                waiting.remove(z)
            ready = ready[n:]

    last = len(ORDER)
    all_of(rb.at[:, 1], extra_sem).wait_recv()
    for i in range(last + VECS_LAG):
        if i < last:
            basis_arrived(ORDER[i])
            product(ORDER[i])
            send_sums(ORDER[i])
        if 0 <= i - SUMS_LAG < last:
            combine(ORDER[i - SUMS_LAG])
        if i + AHEAD < last:
            send_basis(ORDER[i + AHEAD])
        if i in later:
            later[i]()
        if i == OUTER:
            outer_planes()
        if i >= VECS_LAG:
            settle(i - VECS_LAG)

    lane = lax.broadcasted_iota(jnp.int32, (1, 128), 1)
    message = jnp.zeros((1, 128), jnp.float32)
    for ref, start in ((square_a, 0), (square_b, 8), (residual_a, 16), (residual_b, 24)):
        column = jnp.sum(ref[...], axis=1, keepdims=True)
        row = lax.broadcasted_iota(jnp.int32, (ref.shape[0], 128), 0) + start
        message = message + jnp.sum(jnp.where(row == lane, column, 0.0), axis=0, keepdims=True)
    squares[sub] = message

    @pl.loop(1, subs)
    def _(d):
        remote(squares.at[sub], squares.at[sub], square_sem, 0, {"rows": lax.rem(sub + d, subs)}).start()

    for copies in plane_copies.values():
        for copy in copies:
            copy.wait_send()
    list_copy.wait_send()
    all_of(ra.at[:, :, 1], basis_sem).wait_send()
    all_of(rb.at[:, 1], extra_sem).wait_send()
    all_of(from_sums, sum_sem).wait_send()
    all_of(mate_a, vec_a_sem).wait_send()
    all_of(mate_b, vec_b_sem).wait_send()
    every = squares.at[pl.ds(0, subs - 1)]
    all_of(every, square_sem).wait_recv()
    all_of(every, square_sem).wait_send()
    total = jnp.sum(squares[...], axis=0)
    norms = jnp.sqrt(pltpu.roll(total, 112, 1)) / jnp.sqrt(total + 1.0)
    norm_ref[...] = norms[:, :10]


def whole(count, *arrays):
    basis = arrays[0]
    rows = basis.shape[1]
    chunks = rows // CHUNK
    subs = lax.axis_size("rows")
    vmem = pl.BlockSpec(memory_space=pltpu.VMEM)
    f32 = lambda *shape: pltpu.VMEM(shape, jnp.float32)
    bf16 = lambda *shape: pltpu.VMEM(shape, jnp.bfloat16)
    dma = pltpu.SemaphoreType.DMA
    return pl.pallas_call(
        whole_kernel,
        out_shape=(
            jax.ShapeDtypeStruct((10, rows), jnp.bfloat16),
            jax.ShapeDtypeStruct((10, rows), jnp.bfloat16),
            jax.ShapeDtypeStruct((1, 10), jnp.float32),
        ),
        in_specs=[pl.BlockSpec(memory_space=pltpu.SMEM)] + [pl.BlockSpec(memory_space=pltpu.HBM)] * 8,
        out_specs=(vmem,) * 3,
        scratch_shapes=[
            *[pltpu.VMEM(a.shape, a.dtype) for a in arrays[1:]], pltpu.VMEM((2, PLANE), jnp.int32),
            bf16(1, rows), bf16(2, 2, chunks, 2, HALF), bf16(2, 2, 40, 64), bf16(8, rows), bf16(2, rows),
            bf16(8, PLANE), bf16(2, PLANE), bf16(8, PLANE), bf16(2, PLANE), pltpu.VMEM((2, PLANE), jnp.int32),
            bf16(chunks, 2, 2, 24, PIECE), bf16(2, 2, chunks, 2, HALF),
            f32(chunks, 2, 16, PIECE), f32(chunks, 2, 8, HALF),
            *[pltpu.VMEM((chunks, 2, 8, 5 * HALF + 128), jnp.int16) for _ in range(2)],
            bf16(chunks, 2, 8, PIECE), bf16(chunks, 2, 2, PIECE),
            f32(8, PLANE), f32(2, PLANE), f32(8, PLANE), f32(2, PLANE),
            f32(8, 128), f32(8, 128), f32(2, 128), f32(2, 128), f32(subs, 1, 128),
            dma((7,)), dma((chunks,)), dma(()), dma((6,)), dma((5, chunks)), dma((2, 5)), dma((1,)),
        ],
        compiler_params=pltpu.CompilerParams(
            collective_id=0, has_side_effects=True, vmem_limit_bytes=LIMIT
        ),
        name="whole",
    )(count, *[pltpu.with_memory_space_constraint(a, pltpu.HBM) for a in arrays])


def store_kernel(*refs):
    sources, targets, sems = refs[:3], refs[3:6], refs[6]
    copies = [
        pltpu.make_async_copy(source, target, sems.at[k]) for k, (source, target) in enumerate(zip(sources, targets))
    ]
    for copy in copies:
        copy.start()
    for copy in copies:
        copy.wait()


def store(*arrays):
    return pl.pallas_call(
        store_kernel,
        out_shape=tuple(jax.ShapeDtypeStruct(a.shape, a.dtype) for a in arrays),
        in_specs=[pl.BlockSpec(memory_space=pltpu.VMEM)] * 3,
        out_specs=(pl.BlockSpec(memory_space=pltpu.HBM),) * 3,
        scratch_shapes=[pltpu.SemaphoreType.DMA((3,))],
        compiler_params=pltpu.CompilerParams(vmem_limit_bytes=16 * 2**20),
        name="store",
    )(*arrays)


def on_device(basis, coefficients, eigen_values, stiffness, damping, mass, link_count, lower_cells, upper_cells):
    rows_local = basis.shape[1]
    wide = lambda a: a.reshape(1, rows_local)
    eig, res, norms = whole(
        link_count, basis, coefficients.T, lower_cells, upper_cells, wide(mass), wide(damping), wide(stiffness), eigen_values[None, :]
    )
    eig, res, norms = store(eig, res, norms)
    return eig, res, norms.reshape(10)


def solution(mesh):
    placed = (
        P("vecs", "rows"), P(), P("vecs"), P("rows"), P("rows"), P("rows"), P("rows"), P("rows", None), P("rows", None),
    )
    return jax.shard_map(
        on_device,
        mesh=mesh,
        in_specs=placed,
        out_specs=(P("vecs", "rows"), P("vecs", "rows"), P("vecs")),
        check_vma=False,
    )
```

```python
import functools

import jax
import jax.numpy as jnp
from jax import lax
from jax.experimental import pallas as pl
from jax.experimental.pallas import tpu as pltpu
from jax.sharding import PartitionSpec as P

WID = 64
PLANE = WID * WID
SPAN = 2048
SLOTS = 1024
LOW = 256


def link_plane(part_a, part_b, lists, gather, scatter, link_a, link_b):
    high = PLANE // LOW
    whole = jnp.concatenate(
        [part_a[...].astype(jnp.float32), part_b[...].astype(jnp.float32), jnp.zeros((6, PLANE), jnp.float32)], axis=0
    ).astype(jnp.bfloat16)
    table = jnp.concatenate([whole[:, LOW * h : LOW * (h + 1)] for h in range(high)], axis=0)
    cell = lax.broadcasted_iota(jnp.int32, (LOW, SLOTS), 0)

    def step(t, total):
        at = pl.multiple_of(t * SLOTS, SLOTS)
        source = lists[gather : gather + 1, pl.ds(at, SLOTS)]
        target = lists[scatter : scatter + 1, pl.ds(at, SLOTS)]
        pick = jnp.where(cell == (source & (LOW - 1)), 1.0, 0.0).astype(jnp.bfloat16)
        rows = jnp.dot(table, pick, preferred_element_type=jnp.float32)
        source_high = source >> 8
        value = jnp.zeros((16, SLOTS), jnp.float32)
        for h in range(high):
            value = value + jnp.where(source_high == h, rows[16 * h : 16 * h + 16], 0.0)
        target_high = target >> 8
        spread = jnp.concatenate(
            [jnp.where(target_high == h, value, 0.0).astype(jnp.bfloat16) for h in range(high)], axis=0
        )
        place = jnp.where(cell == (target & (LOW - 1)), 1.0, 0.0).astype(jnp.bfloat16)
        return total + lax.dot_general(
            spread, place, (((1,), (1,)), ((), ())), preferred_element_type=jnp.float32
        )

    total = lax.fori_loop(0, PLANE // SLOTS, step, jnp.zeros((16 * high, LOW), jnp.float32))
    for h in range(high):
        link_a[:, LOW * h : LOW * (h + 1)] = total[16 * h : 16 * h + 8]
        link_b[:, LOW * h : LOW * (h + 1)] = total[16 * h + 8 : 16 * h + 10]


def residual_spans(vecs, outs, diag_refs, eigen, first, planes, links, sums):
    eig_ref, res_ref = outs
    depth = eig_ref.shape[1] // PLANE
    spans = PLANE // SPAN
    column = lax.broadcasted_iota(jnp.int32, (1, SPAN), 1) & (WID - 1)
    groups = ((vecs[0], slice(0, 8)), (vecs[1], slice(8, 10)))
    factors = []
    for _, part in groups:
        lam = eigen[part]
        factors.append((lam, lam * lam, lam * lam * 0.1 + lam * 0.3 + 1.0))

    def step(i, totals):
        c = i % spans
        base = pl.multiple_of(first * PLANE + i * SPAN, SPAN)
        here = pl.ds(base, SPAN)
        before = pl.ds(pl.multiple_of(jnp.where(c > 0, base - 128, base), 128), 128)
        after = pl.ds(pl.multiple_of(jnp.where(c < spans - 1, base + SPAN, base), 128), 128)
        mass, damping, stiffness = (r[:, here] for r in diag_refs)
        done = []
        for k, (ref, part) in enumerate(groups):
            lam, square, coupling = factors[k]
            raw = ref[:, here]
            value = raw.astype(jnp.float32)
            left = jnp.where(c > 0, ref[:, before].astype(jnp.float32), 0.0)
            right = jnp.where(c < spans - 1, ref[:, after].astype(jnp.float32), 0.0)
            wide = jnp.concatenate([left, value, right], axis=1)
            span = SPAN + 256
            total = pltpu.roll(wide, WID, 1)[:, 128 : 128 + SPAN] + pltpu.roll(wide, span - WID, 1)[:, 128 : 128 + SPAN]
            total = total + jnp.where(column > 0, pltpu.roll(value, 1, 1), 0.0)
            total = total + jnp.where(column < WID - 1, pltpu.roll(value, SPAN - 1, 1), 0.0)
            if not (links is not None and first == 0):
                total = total + ref[:, pl.ds(pl.multiple_of(base - PLANE, SPAN), SPAN)].astype(jnp.float32)
            if not (links is not None and first == depth - 1):
                total = total + ref[:, pl.ds(pl.multiple_of(base + PLANE, SPAN), SPAN)].astype(jnp.float32)
            if links is not None:
                total = total + links[k][:, pl.ds(pl.multiple_of(i * SPAN, SPAN), SPAN)]
            residual = (square * mass + lam * damping + stiffness) * value - coupling * total
            eig_ref[part, here] = raw
            res_ref[part, here] = residual.astype(jnp.bfloat16)
            vector_sq, residual_sq = totals[2 * k], totals[2 * k + 1]
            for t in range(SPAN // 128):
                lanes = slice(128 * t, 128 * (t + 1))
                vector_sq = vector_sq + value[:, lanes] * value[:, lanes]
                residual_sq = residual_sq + residual[:, lanes] * residual[:, lanes]
            done += [vector_sq, residual_sq]
        return tuple(done)

    totals = lax.fori_loop(0, planes * spans, step, tuple(ref[...] for ref in sums), unroll=2)
    for ref, total in zip(sums, totals):
        ref[...] = total


def column_of(row):
    n = row.shape[1]
    same = lax.broadcasted_iota(jnp.int32, (n, n), 0) == lax.broadcasted_iota(jnp.int32, (n, n), 1)
    return jnp.sum(jnp.where(same, row, 0.0), axis=1, keepdims=True)


def spread_coefficients(coefficients, coefs, devices, which):
    out = lax.broadcasted_iota(jnp.int32, (40, 40), 0)
    vec = lax.broadcasted_iota(jnp.int32, (40, 40), 1)
    rest = out - 32
    group = jnp.where(out < 32, out >> 3, rest >> 1)
    place = jnp.where(out < 32, out & 7, 8 + (rest & 1))
    owner = devices[3]
    for k in range(3):
        owner = jnp.where(group == k, devices[k], owner)
    rows = jnp.where(vec == 10 * owner + place, 1.0, 0.0).astype(jnp.bfloat16)
    ordered = jnp.dot(rows, coefficients[...], preferred_element_type=jnp.float32).astype(jnp.bfloat16)
    rank = lax.broadcasted_iota(jnp.int32, (100, 64), 0)
    at = lax.broadcasted_iota(jnp.int32, (100, 64), 1)
    odd = at - 48
    for h in range(2):
        main = jnp.where(at < 24, 25 * devices[0] + at, 25 * devices[1] + at - 24)
        other = 25 * jnp.where((odd >> 1) == 0, devices[0], devices[1]) + 24
        other = jnp.where((odd < 4) & ((odd & 1) == h), other, -1)
        pick = jnp.where(rank == jnp.where(at < 48, main, other), 1.0, 0.0).astype(jnp.bfloat16)
        coefs[which, h] = jnp.dot(ordered, pick, preferred_element_type=jnp.float32).astype(jnp.bfloat16)


STEPS = 32760.0


def send_scaled(blocks, target):
    lane = lax.broadcasted_iota(jnp.int32, (8, 128), 1)
    powers, at = jnp.zeros((8, 128), jnp.float32), 0
    for k, parts in enumerate(blocks):
        top = jnp.max(jnp.abs(parts[0]), axis=1, keepdims=True)
        for part in parts[1:]:
            top = jnp.maximum(top, jnp.max(jnp.abs(part), axis=1, keepdims=True))
        power = jnp.ceil(jnp.log2(jnp.maximum(top, 1e-30)))
        powers = jnp.where(lane == k, power, powers)
        factor = jnp.exp2(-power) * STEPS
        for part in parts:
            target[:, at : at + HALF] = jnp.round(part * factor).astype(jnp.int32).astype(jnp.int16)
            at += HALF
    target[:, at : at + 128] = powers.astype(jnp.int32).astype(jnp.int16)


MESH = pl.DeviceIdType.MESH
PIECE = 2048
CHUNK = 4 * PIECE
HALF = PIECE // 2
ORDER = (0, 7, 1, 2, 3, 4, 5, 6)
AHEAD = 2
SUMS_LAG, VECS_LAG = 1, 2
OUTER = 7
LIMIT = 50_331_648


def whole_kernel(
    count, basis, coefficients_in, lower_in, upper_in, mass_in, damping_in, stiffness_in, eigen_in,
    eig_ref, res_ref, norm_ref, coefficients, lower, upper, mass, damping, stiffness, eigen_row, lists,
    odd_rows, extra, coefs, ea, eb, above_a, above_b, below_a, below_b, down_lists, ra, rb,
    part_a, part_b, to_sums, from_sums, mate_a, mate_b,
    first_a, first_b, last_a, last_b, square_a, residual_a, square_b, residual_b, squares,
    input_sem, own_sem, odd_sem, sent_sem, chunk_sem, extra_recv_sem, plane_sem, square_recv_sem,
):
    me, sub = lax.axis_index("vecs"), lax.axis_index("rows")
    subs = lax.axis_size("rows")
    following, previous = lax.rem(sub + 1, subs), lax.rem(sub + subs - 1, subs)
    one, two = me + 1 - 2 * lax.rem(me, 2), 3 - me
    mates, crosses = (one, two), (two, one)
    halves = (lax.rem(lax.div(me + 1, 2), 2), lax.div(me, 2))
    basis_sem, extra_sem, sum_sem, vec_a_sem, vec_b_sem = (
        (sent_sem.at[k], extra_recv_sem if k == 1 else chunk_sem.at[k - (k > 1)]) for k in range(5)
    )
    square_sem = (sent_sem.at[5], square_recv_sem)

    barrier = pltpu.get_barrier_semaphore()
    for peer in mates:
        pl.semaphore_signal(barrier, inc=1, device_id={"vecs": peer}, device_id_type=MESH)

    @pl.loop(1, subs)
    def _(d):
        pl.semaphore_signal(barrier, inc=1, device_id={"rows": lax.rem(sub + d, subs)}, device_id_type=MESH)

    def remote(source, target, sems, at, peer):
        return pltpu.make_async_remote_copy(
            src_ref=source, dst_ref=target, send_sem=sems[0], recv_sem=sems[1].at[at],
            device_id=peer, device_id_type=MESH,
        )

    def all_of(block, sems, at=0):
        return remote(block, block, sems, at, {"vecs": one})

    def columns(c, x, half):
        return pl.ds(pl.multiple_of(c * CHUNK + x * CHUNK // 2 + half * PIECE, PIECE), PIECE)

    def send_basis(c):
        for x, (mate, half) in enumerate(zip(mates, halves)):
            remote(
                basis.at[pl.ds(0, 24), columns(c, x, 1 - half)], ra.at[c, x, 1], basis_sem, c, {"vecs": mate}
            ).start()

    def send_extra():
        for x, (mate, half) in enumerate(zip(mates, halves)):
            remote(extra.at[x, 1 - half], rb.at[x, 1], extra_sem, 0, {"vecs": mate}).start()

    def own_copies(c):
        for x, half in enumerate(halves):
            yield pltpu.make_async_copy(basis.at[pl.ds(0, 24), columns(c, x, half)], ra.at[c, x, 0], own_sem.at[c])

    def basis_arrived(c):
        pltpu.make_async_copy(ra.at[c, :, 0], ra.at[c, :, 0], own_sem.at[c]).wait()
        all_of(ra.at[c, :, 1], basis_sem, c).wait_recv()

    def send_sums(c):
        for x, cross in enumerate(crosses):
            remote(to_sums.at[c, x], from_sums.at[c, x], sum_sem, c, {"vecs": cross}).start()

    def send_vecs(c):
        for x, (mate, half) in enumerate(zip(mates, halves)):
            remote(mate_a.at[c, x], ea.at[:, columns(c, x, half)], vec_a_sem, c, {"vecs": mate}).start()
            remote(mate_b.at[c, x], eb.at[:, columns(c, x, half)], vec_b_sem, c, {"vecs": mate}).start()

    def vecs_arrived(c):
        all_of(mate_a.at[c], vec_a_sem, c).wait_recv()
        all_of(mate_b.at[c], vec_b_sem, c).wait_recv()

    rows_local = basis.shape[1]
    plane_copies = {
        ORDER[0]: (
            remote(ea.at[:, pl.ds(0, PLANE)], above_a, (plane_sem.at[0, 0], plane_sem.at[1]), 0, {"rows": previous}),
            remote(eb.at[:, pl.ds(0, PLANE)], above_b, (plane_sem.at[0, 1], plane_sem.at[1]), 1, {"rows": previous}),
        ),
        ORDER[1]: (
            remote(ea.at[:, pl.ds(rows_local - PLANE, PLANE)], below_a, (plane_sem.at[0, 2], plane_sem.at[1]), 2, {"rows": following}),
            remote(eb.at[:, pl.ds(rows_local - PLANE, PLANE)], below_b, (plane_sem.at[0, 3], plane_sem.at[1]), 3, {"rows": following}),
        ),
    }
    list_copy = remote(lists, down_lists, (plane_sem.at[0, 4], plane_sem.at[1]), 4, {"rows": following})

    inputs = [
        pltpu.make_async_copy(source, target, input_sem.at[i])
        for i, (source, target) in enumerate((
            (coefficients_in, coefficients), (lower_in, lower), (upper_in, upper), (eigen_in, eigen_row),
            (mass_in, mass), (damping_in, damping), (stiffness_in, stiffness),
        ))
    ]
    inputs[0].start()
    odd_copy = pltpu.make_async_copy(basis.at[pl.ds(24, 1), :], odd_rows, odd_sem)
    odd_copy.start()
    for c in ORDER:
        for copy in own_copies(c):
            copy.start()
    for copy in inputs[1:]:
        copy.start()
    pl.semaphore_wait(barrier, subs + 1)
    for c in ORDER[:AHEAD]:
        send_basis(c)
    odd_copy.wait()
    for c in ORDER:
        for q in range(4):
            at = c * CHUNK + q * PIECE
            pair = [odd_rows[0:1, at + h * HALF : at + (h + 1) * HALF].astype(jnp.float32) for h in range(2)]
            extra[q // 2, q % 2, c] = jnp.concatenate(pair, axis=0).astype(jnp.bfloat16)
    for x, half in enumerate(halves):
        rb[x, 0] = extra[x, half]
    send_extra()
    for copy in inputs[:4]:
        copy.wait()
    for x in range(2):
        devices = (me, mates[x], crosses[x], 6 - me - one - two)
        spread_coefficients(coefficients, coefs, devices, x)
    used = lax.broadcasted_iota(jnp.int32, (1, PLANE), 1) < count[0]
    lists[0:1, :] = jnp.where(used, lower[...], -1)
    lists[1:2, :] = jnp.where(used, upper[...], -1)
    list_copy.start()
    sums = (square_a, residual_a, square_b, residual_b)
    for ref in sums:
        ref[...] = jnp.zeros_like(ref)
    eigen = column_of(eigen_row[...])
    diag_refs = (mass, damping, stiffness)
    for copy in inputs[4:]:
        copy.wait()

    def planes_done(first, planes, links=None):
        residual_spans((ea, eb), (eig_ref, res_ref), diag_refs, eigen, first, planes, links, sums)

    def product(c):
        for x in range(2):
            outs = []
            for h in range(2):
                at = pl.ds(h * HALF, HALF)
                odd = jnp.concatenate(
                    [rb[x, q, c].astype(jnp.float32) for q in range(2)] + [jnp.zeros((12, HALF), jnp.float32)], axis=0
                )
                stack = jnp.concatenate([ra[c, x, 0, :, at], ra[c, x, 1, :, at], odd.astype(jnp.bfloat16)], axis=0)
                out = jnp.dot(coefs[x, h], stack, preferred_element_type=jnp.float32)
                part_a[c, x, :, at] = out[0:16]
                part_b[c, x, 4 * h : 4 * h + 4, :] = out[32:36]
                outs.append(out)
            ends = jnp.concatenate([out[36:40] for out in outs], axis=0)
            blocks = ([out[16:24] for out in outs], [out[24:32] for out in outs], [ends])
            send_scaled(blocks, to_sums.at[c, x])

    def combine(c):
        all_of(from_sums.at[c], sum_sem, c).wait_recv()
        for x, half in enumerate(halves):
            got = from_sums.at[c, x]
            whole = lambda k: got[:, k * HALF : (k + 1) * HALF].astype(jnp.int32).astype(jnp.float32)
            scale = jnp.exp2(got[:, 5 * HALF : 5 * HALF + 128].astype(jnp.int32).astype(jnp.float32)) * (1.0 / STEPS)
            ends = (part_b[c, x] + whole(4) * scale[:, 2:3]).astype(jnp.bfloat16)
            for h in range(2):
                at = pl.ds(h * HALF, HALF)
                here = pl.ds(pl.multiple_of(c * CHUNK + x * CHUNK // 2 + half * PIECE + h * HALF, HALF), HALF)
                ea[:, here] = (part_a[c, x, :8, at] + whole(h) * scale[:, 0:1]).astype(jnp.bfloat16)
                mate_a[c, x, :, at] = (part_a[c, x, 8:, at] + whole(2 + h) * scale[:, 1:2]).astype(jnp.bfloat16)
                eb[:, here] = ends[4 * h : 4 * h + 2]
                mate_b[c, x, :, at] = ends[4 * h + 2 : 4 * h + 4]
        send_vecs(c)

    def arrived(c):
        vecs_arrived(c)
        for copy in plane_copies.get(c, ()):
            copy.start()

    def first_links():
        for copy in plane_copies[ORDER[1]]:
            copy.wait_recv()
        list_copy.wait_recv()
        link_plane(below_a, below_b, down_lists, 0, 1, first_a, first_b)

    def last_links():
        for copy in plane_copies[ORDER[0]]:
            copy.wait_recv()
        link_plane(above_a, above_b, lists, 1, 0, last_a, last_b)

    def outer_planes():
        planes_done(0, 1, (first_a, first_b))
        planes_done(rows_local // PLANE - 1, 1, (last_a, last_b))

    later = {4: first_links, 5: last_links}
    depth = rows_local // PLANE
    present, waiting = set(), list(range(1, depth - 1))

    def settle(i):
        c = ORDER[i]
        arrived(c)
        present.update(range(c * CHUNK // PLANE, (c + 1) * CHUNK // PLANE))
        ready = [z for z in waiting if {z - 1, z, z + 1} <= present]
        while ready:
            n = 1
            while n < len(ready) and ready[n] == ready[0] + n:
                n += 1
            planes_done(ready[0], n)
            for z in ready[:n]:
                waiting.remove(z)
            ready = ready[n:]

    last = len(ORDER)
    all_of(rb.at[:, 1], extra_sem).wait_recv()
    for i in range(last + VECS_LAG):
        if i < last:
            basis_arrived(ORDER[i])
            product(ORDER[i])
            send_sums(ORDER[i])
        if 0 <= i - SUMS_LAG < last:
            combine(ORDER[i - SUMS_LAG])
        if i + AHEAD < last:
            send_basis(ORDER[i + AHEAD])
        if i in later:
            later[i]()
        if i == OUTER:
            outer_planes()
        if i >= VECS_LAG:
            settle(i - VECS_LAG)

    lane = lax.broadcasted_iota(jnp.int32, (1, 128), 1)
    message = jnp.zeros((1, 128), jnp.float32)
    for ref, start in ((square_a, 0), (square_b, 8), (residual_a, 16), (residual_b, 24)):
        column = jnp.sum(ref[...], axis=1, keepdims=True)
        row = lax.broadcasted_iota(jnp.int32, (ref.shape[0], 128), 0) + start
        message = message + jnp.sum(jnp.where(row == lane, column, 0.0), axis=0, keepdims=True)
    squares[sub] = message

    @pl.loop(1, subs)
    def _(d):
        remote(squares.at[sub], squares.at[sub], square_sem, 0, {"rows": lax.rem(sub + d, subs)}).start()

    for copies in plane_copies.values():
        for copy in copies:
            copy.wait_send()
    list_copy.wait_send()
    all_of(ra.at[:, :, 1], basis_sem).wait_send()
    all_of(rb.at[:, 1], extra_sem).wait_send()
    all_of(from_sums, sum_sem).wait_send()
    all_of(mate_a, vec_a_sem).wait_send()
    all_of(mate_b, vec_b_sem).wait_send()
    every = squares.at[pl.ds(0, subs - 1)]
    all_of(every, square_sem).wait_recv()
    all_of(every, square_sem).wait_send()
    total = jnp.sum(squares[...], axis=0)
    norms = jnp.sqrt(pltpu.roll(total, 112, 1)) / jnp.sqrt(total + 1.0)
    norm_ref[...] = norms[:, :10]


def whole(count, *arrays):
    basis = arrays[0]
    rows = basis.shape[1]
    chunks = rows // CHUNK
    subs = lax.axis_size("rows")
    vmem = pl.BlockSpec(memory_space=pltpu.VMEM)
    f32 = lambda *shape: pltpu.VMEM(shape, jnp.float32)
    bf16 = lambda *shape: pltpu.VMEM(shape, jnp.bfloat16)
    dma = pltpu.SemaphoreType.DMA
    return pl.pallas_call(
        whole_kernel,
        out_shape=(
            jax.ShapeDtypeStruct((10, rows), jnp.bfloat16),
            jax.ShapeDtypeStruct((10, rows), jnp.bfloat16),
            jax.ShapeDtypeStruct((1, 10), jnp.float32),
        ),
        in_specs=[pl.BlockSpec(memory_space=pltpu.SMEM)] + [pl.BlockSpec(memory_space=pltpu.HBM)] * 8,
        out_specs=(vmem,) * 3,
        scratch_shapes=[
            *[pltpu.VMEM(a.shape, a.dtype) for a in arrays[1:]], pltpu.VMEM((2, PLANE), jnp.int32),
            bf16(1, rows), bf16(2, 2, chunks, 2, HALF), bf16(2, 2, 40, 64), bf16(8, rows), bf16(2, rows),
            bf16(8, PLANE), bf16(2, PLANE), bf16(8, PLANE), bf16(2, PLANE), pltpu.VMEM((2, PLANE), jnp.int32),
            bf16(chunks, 2, 2, 24, PIECE), bf16(2, 2, chunks, 2, HALF),
            f32(chunks, 2, 16, PIECE), f32(chunks, 2, 8, HALF),
            *[pltpu.VMEM((chunks, 2, 8, 5 * HALF + 128), jnp.int16) for _ in range(2)],
            bf16(chunks, 2, 8, PIECE), bf16(chunks, 2, 2, PIECE),
            f32(8, PLANE), f32(2, PLANE), f32(8, PLANE), f32(2, PLANE),
            f32(8, 128), f32(8, 128), f32(2, 128), f32(2, 128), f32(subs, 1, 128),
            dma((7,)), dma((chunks,)), dma(()), dma((6,)), dma((4, chunks)), dma((1,)), dma((2, 5)), dma((1,)),
        ],
        compiler_params=pltpu.CompilerParams(
            collective_id=0, has_side_effects=True, vmem_limit_bytes=LIMIT
        ),
        name="whole",
    )(count, *[pltpu.with_memory_space_constraint(a, pltpu.HBM) for a in arrays])


def store_kernel(*refs):
    sources, targets, sems = refs[:3], refs[3:6], refs[6]
    copies = [
        pltpu.make_async_copy(source, target, sems.at[k]) for k, (source, target) in enumerate(zip(sources, targets))
    ]
    for copy in copies:
        copy.start()
    for copy in copies:
        copy.wait()


def store(*arrays):
    return pl.pallas_call(
        store_kernel,
        out_shape=tuple(jax.ShapeDtypeStruct(a.shape, a.dtype) for a in arrays),
        in_specs=[pl.BlockSpec(memory_space=pltpu.VMEM)] * 3,
        out_specs=(pl.BlockSpec(memory_space=pltpu.HBM),) * 3,
        scratch_shapes=[pltpu.SemaphoreType.DMA((3,))],
        compiler_params=pltpu.CompilerParams(vmem_limit_bytes=16 * 2**20),
        name="store",
    )(*arrays)


def on_device(basis, coefficients, eigen_values, stiffness, damping, mass, link_count, lower_cells, upper_cells):
    rows_local = basis.shape[1]
    wide = lambda a: a.reshape(1, rows_local)
    eig, res, norms = whole(
        link_count, basis, coefficients.T, lower_cells, upper_cells, wide(mass), wide(damping), wide(stiffness), eigen_values[None, :]
    )
    eig, res, norms = store(eig, res, norms)
    return eig, res, norms.reshape(10)


def solution(mesh):
    placed = (
        P("vecs", "rows"), P(), P("vecs"), P("rows"), P("rows"), P("rows"), P("rows"), P("rows", None), P("rows", None),
    )
    return jax.shard_map(
        on_device,
        mesh=mesh,
        in_specs=placed,
        out_specs=(P("vecs", "rows"), P("vecs", "rows"), P("vecs")),
        check_vma=False,
    )
```

```python
import functools

import jax
import jax.numpy as jnp
from jax import lax
from jax.experimental import pallas as pl
from jax.experimental.pallas import tpu as pltpu
from jax.sharding import PartitionSpec as P

WID = 64
PLANE = WID * WID
SPAN = 2048
SLOTS = 1024
LOW = 256


def link_plane(part_a, part_b, lists, gather, scatter, link_a, link_b):
    high = PLANE // LOW
    whole = jnp.concatenate(
        [part_a[...].astype(jnp.float32), part_b[...].astype(jnp.float32), jnp.zeros((6, PLANE), jnp.float32)], axis=0
    ).astype(jnp.bfloat16)
    table = jnp.concatenate([whole[:, LOW * h : LOW * (h + 1)] for h in range(high)], axis=0)
    cell = lax.broadcasted_iota(jnp.int32, (LOW, SLOTS), 0)

    def step(t, total):
        at = pl.multiple_of(t * SLOTS, SLOTS)
        source = lists[gather : gather + 1, pl.ds(at, SLOTS)]
        target = lists[scatter : scatter + 1, pl.ds(at, SLOTS)]
        pick = jnp.where(cell == (source & (LOW - 1)), 1.0, 0.0).astype(jnp.bfloat16)
        rows = jnp.dot(table, pick, preferred_element_type=jnp.float32)
        source_high = source >> 8
        value = jnp.zeros((16, SLOTS), jnp.float32)
        for h in range(high):
            value = value + jnp.where(source_high == h, rows[16 * h : 16 * h + 16], 0.0)
        target_high = target >> 8
        spread = jnp.concatenate(
            [jnp.where(target_high == h, value, 0.0).astype(jnp.bfloat16) for h in range(high)], axis=0
        )
        place = jnp.where(cell == (target & (LOW - 1)), 1.0, 0.0).astype(jnp.bfloat16)
        return total + lax.dot_general(
            spread, place, (((1,), (1,)), ((), ())), preferred_element_type=jnp.float32
        )

    total = lax.fori_loop(0, PLANE // SLOTS, step, jnp.zeros((16 * high, LOW), jnp.float32))
    for h in range(high):
        link_a[:, LOW * h : LOW * (h + 1)] = total[16 * h : 16 * h + 8]
        link_b[:, LOW * h : LOW * (h + 1)] = total[16 * h + 8 : 16 * h + 10]


def residual_spans(vecs, outs, diag_refs, eigen, first, planes, links, sums):
    eig_ref, res_ref = outs
    depth = eig_ref.shape[1] // PLANE
    spans = PLANE // SPAN
    column = lax.broadcasted_iota(jnp.int32, (1, SPAN), 1) & (WID - 1)
    groups = ((vecs[0], slice(0, 8)), (vecs[1], slice(8, 10)))
    factors = []
    for _, part in groups:
        lam = eigen[part]
        factors.append((lam, lam * lam, lam * lam * 0.1 + lam * 0.3 + 1.0))

    def step(i, totals):
        c = i % spans
        base = pl.multiple_of(first * PLANE + i * SPAN, SPAN)
        here = pl.ds(base, SPAN)
        before = pl.ds(pl.multiple_of(jnp.where(c > 0, base - 128, base), 128), 128)
        after = pl.ds(pl.multiple_of(jnp.where(c < spans - 1, base + SPAN, base), 128), 128)
        mass, damping, stiffness = (r[:, here] for r in diag_refs)
        done = []
        for k, (ref, part) in enumerate(groups):
            lam, square, coupling = factors[k]
            raw = ref[:, here]
            value = raw.astype(jnp.float32)
            left = jnp.where(c > 0, ref[:, before].astype(jnp.float32), 0.0)
            right = jnp.where(c < spans - 1, ref[:, after].astype(jnp.float32), 0.0)
            wide = jnp.concatenate([left, value, right], axis=1)
            span = SPAN + 256
            total = pltpu.roll(wide, WID, 1)[:, 128 : 128 + SPAN] + pltpu.roll(wide, span - WID, 1)[:, 128 : 128 + SPAN]
            total = total + jnp.where(column > 0, pltpu.roll(value, 1, 1), 0.0)
            total = total + jnp.where(column < WID - 1, pltpu.roll(value, SPAN - 1, 1), 0.0)
            if not (links is not None and first == 0):
                total = total + ref[:, pl.ds(pl.multiple_of(base - PLANE, SPAN), SPAN)].astype(jnp.float32)
            if not (links is not None and first == depth - 1):
                total = total + ref[:, pl.ds(pl.multiple_of(base + PLANE, SPAN), SPAN)].astype(jnp.float32)
            if links is not None:
                total = total + links[k][:, pl.ds(pl.multiple_of(i * SPAN, SPAN), SPAN)]
            residual = (square * mass + lam * damping + stiffness) * value - coupling * total
            eig_ref[part, here] = raw
            res_ref[part, here] = residual.astype(jnp.bfloat16)
            vector_sq, residual_sq = totals[2 * k], totals[2 * k + 1]
            for t in range(SPAN // 128):
                lanes = slice(128 * t, 128 * (t + 1))
                vector_sq = vector_sq + value[:, lanes] * value[:, lanes]
                residual_sq = residual_sq + residual[:, lanes] * residual[:, lanes]
            done += [vector_sq, residual_sq]
        return tuple(done)

    totals = lax.fori_loop(0, planes * spans, step, tuple(ref[...] for ref in sums), unroll=2)
    for ref, total in zip(sums, totals):
        ref[...] = total


def column_of(row):
    n = row.shape[1]
    same = lax.broadcasted_iota(jnp.int32, (n, n), 0) == lax.broadcasted_iota(jnp.int32, (n, n), 1)
    return jnp.sum(jnp.where(same, row, 0.0), axis=1, keepdims=True)


def spread_coefficients(coefficients, coefs, devices, which):
    out = lax.broadcasted_iota(jnp.int32, (40, 40), 0)
    vec = lax.broadcasted_iota(jnp.int32, (40, 40), 1)
    rest = out - 32
    group = jnp.where(out < 32, out >> 3, rest >> 1)
    place = jnp.where(out < 32, out & 7, 8 + (rest & 1))
    owner = devices[3]
    for k in range(3):
        owner = jnp.where(group == k, devices[k], owner)
    rows = jnp.where(vec == 10 * owner + place, 1.0, 0.0).astype(jnp.bfloat16)
    ordered = jnp.dot(rows, coefficients[...], preferred_element_type=jnp.float32).astype(jnp.bfloat16)
    rank = lax.broadcasted_iota(jnp.int32, (100, 64), 0)
    at = lax.broadcasted_iota(jnp.int32, (100, 64), 1)
    odd = at - 48
    for h in range(2):
        main = jnp.where(at < 24, 25 * devices[0] + at, 25 * devices[1] + at - 24)
        other = 25 * jnp.where((odd >> 1) == 0, devices[0], devices[1]) + 24
        other = jnp.where((odd < 4) & ((odd & 1) == h), other, -1)
        pick = jnp.where(rank == jnp.where(at < 48, main, other), 1.0, 0.0).astype(jnp.bfloat16)
        coefs[which, h] = jnp.dot(ordered, pick, preferred_element_type=jnp.float32).astype(jnp.bfloat16)


STEPS = 32760.0


def send_scaled(blocks, target):
    lane = lax.broadcasted_iota(jnp.int32, (8, 128), 1)
    powers, at = jnp.zeros((8, 128), jnp.float32), 0
    for k, parts in enumerate(blocks):
        top = jnp.max(jnp.abs(parts[0]), axis=1, keepdims=True)
        for part in parts[1:]:
            top = jnp.maximum(top, jnp.max(jnp.abs(part), axis=1, keepdims=True))
        power = jnp.ceil(jnp.log2(jnp.maximum(top, 1e-30)))
        powers = jnp.where(lane == k, power, powers)
        factor = jnp.exp2(-power) * STEPS
        for part in parts:
            target[:, at : at + HALF] = jnp.round(part * factor).astype(jnp.int32).astype(jnp.int16)
            at += HALF
    target[:, at : at + 128] = powers.astype(jnp.int32).astype(jnp.int16)


MESH = pl.DeviceIdType.MESH
PIECE = 2048
CHUNK = 4 * PIECE
HALF = PIECE // 2
ORDER = (0, 7, 1, 2, 3, 4, 5, 6)
AHEAD = 2
SUMS_LAG, VECS_LAG = 1, 2
OUTER = 7
LIMIT = 50_331_648


def whole_kernel(
    count, basis, coefficients_in, lower_in, upper_in, mass_in, damping_in, stiffness_in, eigen_in,
    eig_ref, res_ref, norm_ref, coefficients, lower, upper, mass, damping, stiffness, eigen_row, lists,
    odd_rows, extra, coefs, ea, eb, above_a, above_b, below_a, below_b, down_lists, ra, rb,
    part_a, part_b, to_sums, from_sums, mate_a, mate_b,
    first_a, first_b, last_a, last_b, square_a, residual_a, square_b, residual_b, squares,
    input_sem, own_sem, odd_sem, sent_sem, chunk_sem, extra_recv_sem, plane_sem, square_recv_sem,
):
    me, sub = lax.axis_index("vecs"), lax.axis_index("rows")
    subs = lax.axis_size("rows")
    following, previous = lax.rem(sub + 1, subs), lax.rem(sub + subs - 1, subs)
    one, two = me + 1 - 2 * lax.rem(me, 2), 3 - me
    mates, crosses = (one, two), (two, one)
    halves = (lax.rem(lax.div(me + 1, 2), 2), lax.div(me, 2))
    basis_sem, extra_sem, sum_sem, vec_a_sem, vec_b_sem = (
        (sent_sem.at[k], extra_recv_sem if k == 1 else chunk_sem.at[k - (k > 1)]) for k in range(5)
    )
    square_sem = (sent_sem.at[5], square_recv_sem)

    barrier = pltpu.get_barrier_semaphore()
    for peer in mates:
        pl.semaphore_signal(barrier, inc=1, device_id={"vecs": peer}, device_id_type=MESH)

    @pl.loop(1, subs)
    def _(d):
        pl.semaphore_signal(barrier, inc=1, device_id={"rows": lax.rem(sub + d, subs)}, device_id_type=MESH)

    def remote(source, target, sems, at, peer):
        return pltpu.make_async_remote_copy(
            src_ref=source, dst_ref=target, send_sem=sems[0], recv_sem=sems[1].at[at],
            device_id=peer, device_id_type=MESH,
        )

    def all_of(block, sems, at=0):
        return remote(block, block, sems, at, {"vecs": one})

    def columns(c, x, half):
        return pl.ds(pl.multiple_of(c * CHUNK + x * CHUNK // 2 + half * PIECE, PIECE), PIECE)

    def send_basis(c):
        for x, (mate, half) in enumerate(zip(mates, halves)):
            remote(
                basis.at[pl.ds(0, 24), columns(c, x, 1 - half)], ra.at[c, x, 1], basis_sem, c, {"vecs": mate}
            ).start()

    def send_extra():
        for x, (mate, half) in enumerate(zip(mates, halves)):
            remote(extra.at[x, 1 - half], rb.at[x, 1], extra_sem, 0, {"vecs": mate}).start()

    def own_copies(c):
        for x, half in enumerate(halves):
            yield pltpu.make_async_copy(basis.at[pl.ds(0, 24), columns(c, x, half)], ra.at[c, x, 0], own_sem)

    def basis_arrived(c):
        all_of(ra.at[c, :, 1], basis_sem, c).wait_recv()

    def send_sums(c):
        for x, cross in enumerate(crosses):
            remote(to_sums.at[c, x], from_sums.at[c, x], sum_sem, c, {"vecs": cross}).start()

    def send_vecs(c):
        for x, (mate, half) in enumerate(zip(mates, halves)):
            remote(mate_a.at[c, x], ea.at[:, columns(c, x, half)], vec_a_sem, c, {"vecs": mate}).start()
            remote(mate_b.at[c, x], eb.at[:, columns(c, x, half)], vec_b_sem, c, {"vecs": mate}).start()

    def vecs_arrived(c):
        all_of(mate_a.at[c], vec_a_sem, c).wait_recv()
        all_of(mate_b.at[c], vec_b_sem, c).wait_recv()

    rows_local = basis.shape[1]
    plane_copies = {
        ORDER[0]: (
            remote(ea.at[:, pl.ds(0, PLANE)], above_a, (plane_sem.at[0, 0], plane_sem.at[1]), 0, {"rows": previous}),
            remote(eb.at[:, pl.ds(0, PLANE)], above_b, (plane_sem.at[0, 1], plane_sem.at[1]), 1, {"rows": previous}),
        ),
        ORDER[1]: (
            remote(ea.at[:, pl.ds(rows_local - PLANE, PLANE)], below_a, (plane_sem.at[0, 2], plane_sem.at[1]), 2, {"rows": following}),
            remote(eb.at[:, pl.ds(rows_local - PLANE, PLANE)], below_b, (plane_sem.at[0, 3], plane_sem.at[1]), 3, {"rows": following}),
        ),
    }
    list_copy = remote(lists, down_lists, (plane_sem.at[0, 4], plane_sem.at[1]), 4, {"rows": following})

    inputs = [
        pltpu.make_async_copy(source, target, input_sem.at[i])
        for i, (source, target) in enumerate((
            (coefficients_in, coefficients), (lower_in, lower), (upper_in, upper), (eigen_in, eigen_row),
            (mass_in, mass), (damping_in, damping), (stiffness_in, stiffness),
        ))
    ]
    inputs[0].start()
    odd_copy = pltpu.make_async_copy(basis.at[pl.ds(24, 1), :], odd_rows, odd_sem)
    odd_copy.start()
    for c in ORDER:
        for copy in own_copies(c):
            copy.start()
    for copy in inputs[1:]:
        copy.start()
    pl.semaphore_wait(barrier, subs + 1)
    for c in ORDER[:AHEAD]:
        send_basis(c)
    odd_copy.wait()
    for c in ORDER:
        for q in range(4):
            at = c * CHUNK + q * PIECE
            pair = [odd_rows[0:1, at + h * HALF : at + (h + 1) * HALF].astype(jnp.float32) for h in range(2)]
            extra[q // 2, q % 2, c] = jnp.concatenate(pair, axis=0).astype(jnp.bfloat16)
    for x, half in enumerate(halves):
        rb[x, 0] = extra[x, half]
    send_extra()
    for copy in inputs[:4]:
        copy.wait()
    for x in range(2):
        devices = (me, mates[x], crosses[x], 6 - me - one - two)
        spread_coefficients(coefficients, coefs, devices, x)
    used = lax.broadcasted_iota(jnp.int32, (1, PLANE), 1) < count[0]
    lists[0:1, :] = jnp.where(used, lower[...], -1)
    lists[1:2, :] = jnp.where(used, upper[...], -1)
    list_copy.start()
    sums = (square_a, residual_a, square_b, residual_b)
    for ref in sums:
        ref[...] = jnp.zeros_like(ref)
    eigen = column_of(eigen_row[...])
    diag_refs = (mass, damping, stiffness)
    for copy in inputs[4:]:
        copy.wait()

    def planes_done(first, planes, links=None):
        residual_spans((ea, eb), (eig_ref, res_ref), diag_refs, eigen, first, planes, links, sums)

    def product(c):
        for x in range(2):
            outs = []
            for h in range(2):
                at = pl.ds(h * HALF, HALF)
                odd = jnp.concatenate(
                    [rb[x, q, c].astype(jnp.float32) for q in range(2)] + [jnp.zeros((12, HALF), jnp.float32)], axis=0
                )
                stack = jnp.concatenate([ra[c, x, 0, :, at], ra[c, x, 1, :, at], odd.astype(jnp.bfloat16)], axis=0)
                out = jnp.dot(coefs[x, h], stack, preferred_element_type=jnp.float32)
                part_a[c, x, :, at] = out[0:16]
                part_b[c, x, 4 * h : 4 * h + 4, :] = out[32:36]
                outs.append(out)
            ends = jnp.concatenate([out[36:40] for out in outs], axis=0)
            blocks = ([out[16:24] for out in outs], [out[24:32] for out in outs], [ends])
            send_scaled(blocks, to_sums.at[c, x])

    def combine(c):
        all_of(from_sums.at[c], sum_sem, c).wait_recv()
        for x, half in enumerate(halves):
            got = from_sums.at[c, x]
            whole = lambda k: got[:, k * HALF : (k + 1) * HALF].astype(jnp.int32).astype(jnp.float32)
            scale = jnp.exp2(got[:, 5 * HALF : 5 * HALF + 128].astype(jnp.int32).astype(jnp.float32)) * (1.0 / STEPS)
            ends = (part_b[c, x] + whole(4) * scale[:, 2:3]).astype(jnp.bfloat16)
            for h in range(2):
                at = pl.ds(h * HALF, HALF)
                here = pl.ds(pl.multiple_of(c * CHUNK + x * CHUNK // 2 + half * PIECE + h * HALF, HALF), HALF)
                ea[:, here] = (part_a[c, x, :8, at] + whole(h) * scale[:, 0:1]).astype(jnp.bfloat16)
                mate_a[c, x, :, at] = (part_a[c, x, 8:, at] + whole(2 + h) * scale[:, 1:2]).astype(jnp.bfloat16)
                eb[:, here] = ends[4 * h : 4 * h + 2]
                mate_b[c, x, :, at] = ends[4 * h + 2 : 4 * h + 4]
        send_vecs(c)

    def arrived(c):
        vecs_arrived(c)
        for copy in plane_copies.get(c, ()):
            copy.start()

    def first_links():
        for copy in plane_copies[ORDER[1]]:
            copy.wait_recv()
        list_copy.wait_recv()
        link_plane(below_a, below_b, down_lists, 0, 1, first_a, first_b)

    def last_links():
        for copy in plane_copies[ORDER[0]]:
            copy.wait_recv()
        link_plane(above_a, above_b, lists, 1, 0, last_a, last_b)

    def outer_planes():
        planes_done(0, 1, (first_a, first_b))
        planes_done(rows_local // PLANE - 1, 1, (last_a, last_b))

    later = {4: first_links, 5: last_links}
    depth = rows_local // PLANE
    present, waiting = set(), list(range(1, depth - 1))

    def settle(i):
        c = ORDER[i]
        arrived(c)
        present.update(range(c * CHUNK // PLANE, (c + 1) * CHUNK // PLANE))
        ready = [z for z in waiting if {z - 1, z, z + 1} <= present]
        while ready:
            n = 1
            while n < len(ready) and ready[n] == ready[0] + n:
                n += 1
            planes_done(ready[0], n)
            for z in ready[:n]:
                waiting.remove(z)
            ready = ready[n:]

    last = len(ORDER)
    pltpu.make_async_copy(ra.at[:, :, 0], ra.at[:, :, 0], own_sem).wait()
    all_of(rb.at[:, 1], extra_sem).wait_recv()
    for i in range(last + VECS_LAG):
        if i < last:
            basis_arrived(ORDER[i])
            product(ORDER[i])
            send_sums(ORDER[i])
        if 0 <= i - SUMS_LAG < last:
            combine(ORDER[i - SUMS_LAG])
        if i + AHEAD < last:
            send_basis(ORDER[i + AHEAD])
        if i in later:
            later[i]()
        if i == OUTER:
            outer_planes()
        if i >= VECS_LAG:
            settle(i - VECS_LAG)

    lane = lax.broadcasted_iota(jnp.int32, (1, 128), 1)
    message = jnp.zeros((1, 128), jnp.float32)
    for ref, start in ((square_a, 0), (square_b, 8), (residual_a, 16), (residual_b, 24)):
        column = jnp.sum(ref[...], axis=1, keepdims=True)
        row = lax.broadcasted_iota(jnp.int32, (ref.shape[0], 128), 0) + start
        message = message + jnp.sum(jnp.where(row == lane, column, 0.0), axis=0, keepdims=True)
    squares[sub] = message

    @pl.loop(1, subs)
    def _(d):
        remote(squares.at[sub], squares.at[sub], square_sem, 0, {"rows": lax.rem(sub + d, subs)}).start()

    for copies in plane_copies.values():
        for copy in copies:
            copy.wait_send()
    list_copy.wait_send()
    all_of(ra.at[:, :, 1], basis_sem).wait_send()
    all_of(rb.at[:, 1], extra_sem).wait_send()
    all_of(from_sums, sum_sem).wait_send()
    all_of(mate_a, vec_a_sem).wait_send()
    all_of(mate_b, vec_b_sem).wait_send()
    every = squares.at[pl.ds(0, subs - 1)]
    all_of(every, square_sem).wait_recv()
    all_of(every, square_sem).wait_send()
    total = jnp.sum(squares[...], axis=0)
    norms = jnp.sqrt(pltpu.roll(total, 112, 1)) / jnp.sqrt(total + 1.0)
    norm_ref[...] = norms[:, :10]


def whole(count, *arrays):
    basis = arrays[0]
    rows = basis.shape[1]
    chunks = rows // CHUNK
    subs = lax.axis_size("rows")
    vmem = pl.BlockSpec(memory_space=pltpu.VMEM)
    f32 = lambda *shape: pltpu.VMEM(shape, jnp.float32)
    bf16 = lambda *shape: pltpu.VMEM(shape, jnp.bfloat16)
    dma = pltpu.SemaphoreType.DMA
    return pl.pallas_call(
        whole_kernel,
        out_shape=(
            jax.ShapeDtypeStruct((10, rows), jnp.bfloat16),
            jax.ShapeDtypeStruct((10, rows), jnp.bfloat16),
            jax.ShapeDtypeStruct((1, 10), jnp.float32),
        ),
        in_specs=[pl.BlockSpec(memory_space=pltpu.SMEM)] + [pl.BlockSpec(memory_space=pltpu.HBM)] * 8,
        out_specs=(vmem,) * 3,
        scratch_shapes=[
            *[pltpu.VMEM(a.shape, a.dtype) for a in arrays[1:]], pltpu.VMEM((2, PLANE), jnp.int32),
            bf16(1, rows), bf16(2, 2, chunks, 2, HALF), bf16(2, 2, 40, 64), bf16(8, rows), bf16(2, rows),
            bf16(8, PLANE), bf16(2, PLANE), bf16(8, PLANE), bf16(2, PLANE), pltpu.VMEM((2, PLANE), jnp.int32),
            bf16(chunks, 2, 2, 24, PIECE), bf16(2, 2, chunks, 2, HALF),
            f32(chunks, 2, 16, PIECE), f32(chunks, 2, 8, HALF),
            *[pltpu.VMEM((chunks, 2, 8, 5 * HALF + 128), jnp.int16) for _ in range(2)],
            bf16(chunks, 2, 8, PIECE), bf16(chunks, 2, 2, PIECE),
            f32(8, PLANE), f32(2, PLANE), f32(8, PLANE), f32(2, PLANE),
            f32(8, 128), f32(8, 128), f32(2, 128), f32(2, 128), f32(subs, 1, 128),
            dma((7,)), dma(()), dma(()), dma((6,)), dma((4, chunks)), dma((1,)), dma((2, 5)), dma((1,)),
        ],
        compiler_params=pltpu.CompilerParams(
            collective_id=0, has_side_effects=True, vmem_limit_bytes=LIMIT
        ),
        name="whole",
    )(count, *[pltpu.with_memory_space_constraint(a, pltpu.HBM) for a in arrays])


def store_kernel(*refs):
    sources, targets, sems = refs[:3], refs[3:6], refs[6]
    copies = [
        pltpu.make_async_copy(source, target, sems.at[k]) for k, (source, target) in enumerate(zip(sources, targets))
    ]
    for copy in copies:
        copy.start()
    for copy in copies:
        copy.wait()


def store(*arrays):
    return pl.pallas_call(
        store_kernel,
        out_shape=tuple(jax.ShapeDtypeStruct(a.shape, a.dtype) for a in arrays),
        in_specs=[pl.BlockSpec(memory_space=pltpu.VMEM)] * 3,
        out_specs=(pl.BlockSpec(memory_space=pltpu.HBM),) * 3,
        scratch_shapes=[pltpu.SemaphoreType.DMA((3,))],
        compiler_params=pltpu.CompilerParams(vmem_limit_bytes=16 * 2**20),
        name="store",
    )(*arrays)


def on_device(basis, coefficients, eigen_values, stiffness, damping, mass, link_count, lower_cells, upper_cells):
    rows_local = basis.shape[1]
    wide = lambda a: a.reshape(1, rows_local)
    eig, res, norms = whole(
        link_count, basis, coefficients.T, lower_cells, upper_cells, wide(mass), wide(damping), wide(stiffness), eigen_values[None, :]
    )
    eig, res, norms = store(eig, res, norms)
    return eig, res, norms.reshape(10)


def solution(mesh):
    placed = (
        P("vecs", "rows"), P(), P("vecs"), P("rows"), P("rows"), P("rows"), P("rows"), P("rows", None), P("rows", None),
    )
    return jax.shard_map(
        on_device,
        mesh=mesh,
        in_specs=placed,
        out_specs=(P("vecs", "rows"), P("vecs", "rows"), P("vecs")),
        check_vma=False,
    )
```
